32 devices in a mesh: gx: 16 (over z, x, core), gy: 2 (over y).
Axes of the slice: x: 2, y: 2, z: 4, core: 2. Of those that a mesh axis runs over, the one named last changes fastest.
Arguments:
- temp_adjoint: float32 [8, 256, 2048], P(None, 'gy', 'gx'), may hold values from -6 to 6
- height_adjoint: float32 [256, 2048], P('gy', 'gx'), may hold values from -6 to 6
- east_velocity: float32 [8, 256, 2048], P(None, 'gy', 'gx'), may hold values from -0.8 to 0.8
- north_velocity: float32 [8, 256, 2048], P(None, 'gy', 'gx'), may hold values from -0.8 to 0.8
- temp_store: float32 [8, 256, 2048], P(None, 'gy', 'gx'), may hold values from -4 to 4
- salt_store: float32 [8, 256, 2048], P(None, 'gy', 'gx'), may hold values from -4 to 4
- slot_map: int32 [16, 2, 8], P('gx', 'gy'), may hold values from 0 to 7, each once within a row
- land_mask: int32 [8, 256, 2048], P(None, 'gy', 'gx'), may hold values 0 or 1
- ocean_depth: float32 [256, 2048], P('gy', 'gx'), may hold values from 0.1 to 1
Outputs:
- temp_back: float32 [8, 256, 2048], P(None, 'gy', 'gx')
- salt_back: float32 [8, 256, 2048], P(None, 'gy', 'gx')
- surface_adjoint: float32 [256, 2048], P('gy', 'gx')
The draws below stay inside these ranges and needn't reach their ends.
Inputs may be any that keep to these rules, and one draw needn't show every extreme that they name: `slot_map`: each tile's entries over the last dimension name every slot 0 to 7 once.
All inputs are finite; a program needn't handle non-finite values. No bound on the sum of `land_mask` on one device may be relied on, other than what follows from the above.
Results may differ from the reference program's by a relative error of at most 0.00013.
Values sent between devices are 32-bit elements; how exact they have to be, the bound alone decides.
No kernel may reach another device: no remote copies, remote signals or barrier semaphores. Data moves between devices by JAX's collectives and lax.ppermute only.
A program may use at most 64 MiB of HBM per device.

```python
import math
import jax
import jax.numpy as jnp
from jax import lax

LEV = 8
CY = 128
CX = 128
ITERS = 6
TILES_X = 16
TILES_Y = 2
NX = 2048
NY = 256


def plant(drawn, rng, least, top_value):
    index_at = [jax.random.randint(jax.random.fold_in(rng, axis), (), 0, length) for axis, length in enumerate(drawn.shape)]
    main_axis = drawn.shape.index(max(drawn.shape))
    beside = index_at[:main_axis] + [(index_at[main_axis] + 1) % drawn.shape[main_axis]] + index_at[main_axis + 1:]
    return drawn.at[tuple(index_at)].set(least).at[tuple(beside)].set(top_value)


def level_of(rng, extent, split, smallest, top_value):
    gain, own = 1.0, jax.random.fold_in(rng, 6)
    for dim, shards_of in split:
        draws = jnp.exp(jax.random.uniform(jax.random.fold_in(own, dim), (shards_of,), jnp.float32, smallest / len(split), top_value / len(split)))
        gain = gain * jnp.repeat(draws, extent[dim] // shards_of).reshape([-1 if axis == dim else 1 for axis in range(len(extent))])
    return gain


def bell_draw(key, shape, width, reach, shards=(), kind=jnp.bfloat16):
    array = width * jax.random.normal(key, shape, jnp.float32)
    if shards:
        array = array * level_of(key, shape, shards, -0.22, 0.18)
    return jnp.clip(array, -reach, reach).astype(kind)


def setup_inputs(seed: int = 0) -> dict:
    key_list = jax.random.split(jax.random.key(seed), 10)
    temp_adjoint = bell_draw(key_list[0], (LEV, NY, NX), 1.0, 6.0, ((1, 2), (2, 16)), jnp.float32)
    height_adjoint = bell_draw(key_list[1], (NY, NX), 1.0, 6.0, ((0, 2), (1, 16)), jnp.float32)
    east_velocity = bell_draw(key_list[2], (LEV, NY, NX), 0.2, 0.8, ((1, 2), (2, 16)), jnp.float32)
    north_velocity = bell_draw(key_list[3], (LEV, NY, NX), 0.2, 0.8, ((1, 2), (2, 16)), jnp.float32)
    temp_store = bell_draw(key_list[4], (LEV, NY, NX), 1.0, 4.0, ((1, 2), (2, 16)), jnp.float32)
    salt_store = bell_draw(key_list[5], (LEV, NY, NX), 1.0, 4.0, ((1, 2), (2, 16)), jnp.float32)
    slot_map = jax.vmap(lambda own: jax.random.permutation(own, LEV))(jax.random.split(key_list[6], TILES_X * TILES_Y)).reshape((TILES_X, TILES_Y, LEV)).astype(jnp.int32)
    land_mask = plant((jax.random.randint(key_list[7], (LEV, NY, NX), 0, 4) < 3).astype(jnp.int32), jax.random.fold_in(key_list[7], 1), 0, 1)
    ocean_depth = jnp.clip(jnp.exp(math.log(1.0) - 2.3025851 * jax.random.uniform(key_list[8], (NY, NX), jnp.float32) ** level_of(key_list[8], (NY, NX), ((0, 2), (1, 16)), -0.2, 0.2)), 0.1, 1.0)
    return dict(temp_adjoint=temp_adjoint, height_adjoint=height_adjoint, east_velocity=east_velocity, north_velocity=north_velocity, temp_store=temp_store, salt_store=salt_store, slot_map=slot_map, land_mask=land_mask, ocean_depth=ocean_depth)


DIFFUSE = 0.2
TIMESTEP = 1.0
STIFFNESS = 8.0
GRAVITY = 4.0
THERMAL = 0.5
NONLINEAR = 0.4
CABBELING = 0.3
HALINE = 0.8


def west_of(grid_field):
    return jnp.roll(grid_field, 1, axis=-1)


def east_of(grid_field):
    return jnp.roll(grid_field, -1, axis=-1)


def south_of(grid_field):
    zero_edge = jnp.zeros_like(grid_field[..., :1, :])
    return jnp.concatenate([zero_edge, grid_field[..., :-1, :]], axis=-2)


def north_of(grid_field):
    zero_edge = jnp.zeros_like(grid_field[..., :1, :])
    return jnp.concatenate([grid_field[..., 1:, :], zero_edge], axis=-2)


NEIGHBOURS = (west_of, east_of, south_of, north_of)


def surface_apply(grid_field, face_links, face_weights):
    applied = grid_field
    for neighbour, face_weight in zip(NEIGHBOURS, face_weights):
        applied = applied + face_weight * (grid_field - neighbour(grid_field))
    return applied


def reference(temp_adjoint, height_adjoint, east_velocity, north_velocity, temp_store, salt_store, slot_map, land_mask, ocean_depth):
    wet_cells = land_mask.astype(jnp.float32)
    masked = wet_cells * temp_adjoint
    east_coef = DIFFUSE - 0.5 * east_velocity
    west_coef = DIFFUSE + 0.5 * east_velocity
    north_coef = DIFFUSE - 0.5 * north_velocity
    south_coef = DIFFUSE + 0.5 * north_velocity
    inflow = west_of(east_coef * masked) + east_of(west_coef * masked)
    inflow = inflow + south_of(north_coef * masked) + north_of(south_coef * masked)
    tracer_back = masked + TIMESTEP * (inflow - (east_coef + west_coef + north_coef + south_coef) * masked)

    open_cells = wet_cells[0]
    face_links = [open_cells * neighbour(open_cells) for neighbour in NEIGHBOURS]
    face_weights = [STIFFNESS * 0.5 * (ocean_depth + neighbour(ocean_depth)) * link_open
                    for neighbour, link_open in zip(NEIGHBOURS, face_links)]
    target = open_cells * height_adjoint
    solution = jnp.zeros_like(target)
    residual = target
    direction = target
    norm_now = jnp.sum(residual * residual)
    for iteration in range(ITERS):
        image_field = surface_apply(direction, face_links, face_weights)
        step_size = norm_now / jnp.sum(direction * image_field)
        solution = solution + step_size * direction
        residual = residual - step_size * image_field
        norm_next = jnp.sum(residual * residual)
        direction = residual + (norm_next / norm_now) * direction
        norm_now = norm_next

    height_load = ocean_depth * solution
    pressure_pull = jnp.zeros_like(height_load)
    for neighbour, link_open in zip(NEIGHBOURS, face_links):
        pressure_pull = pressure_pull + link_open * (neighbour(height_load) - height_load)
    adj_pressure = -GRAVITY * pressure_pull
    thickness = 1.0 + jnp.arange(LEV, dtype=jnp.float32) / LEV
    adj_density = thickness[:, None, None] * adj_pressure[None] * wet_cells

    slot_onehot = (slot_map[:, :, :, None] == jnp.arange(LEV, dtype=jnp.int32)[None, None, None, :]).astype(jnp.float32)
    tiles_x = slot_map.shape[0]
    tiles_y = slot_map.shape[1]

    def reorder(store):
        blocks = store.reshape(LEV, tiles_y, CY, tiles_x, CX)
        ordered = jnp.einsum("ijks,sjyix->kjyix", slot_onehot, blocks, precision=lax.Precision.HIGHEST)
        return jnp.roll(ordered.reshape(LEV, NY, NX), -(NX // 2), axis=-1)

    ck_temp = reorder(temp_store)
    ck_salt = reorder(salt_store)
    temp_back = tracer_back + (THERMAL + 2.0 * NONLINEAR * ck_temp + CABBELING * ck_salt) * adj_density
    salt_back = (HALINE + CABBELING * ck_temp) * adj_density
    return temp_back, salt_back, solution
```

```python
import functools

import jax
import jax.numpy as jnp
from jax import lax
from jax.experimental import pallas as pl
from jax.experimental.pallas import tpu as pltpu
from jax.sharding import PartitionSpec as P

ITERS = 6
RING = 8
LANES = 128

DIFFUSE = 0.2
TIMESTEP = 1.0
STIFFNESS = 8.0
GRAVITY = 4.0
THERMAL = 0.5
NONLINEAR = 0.4
CABBELING = 0.3
HALINE = 0.8


VMEM = pl.BlockSpec(memory_space=pltpu.VMEM)
SMEM = pl.BlockSpec(memory_space=pltpu.SMEM)

OFF_AT, WEIGHT_AT = 16, 32
PAIRS = [(i, j) for i in range(ITERS + 1) for j in range(i, ITERS + 1)]


def call(kernel, outs, args, specs=None, flops=100000, name=None):
    shapes = [jax.ShapeDtypeStruct(shape, jnp.float32) for shape in outs]
    return pl.pallas_call(
        kernel,
        out_shape=shapes,
        in_specs=specs or [VMEM] * len(args),
        out_specs=[VMEM] * len(outs),
        cost_estimate=pl.CostEstimate(flops=flops, bytes_accessed=1000000, transcendentals=0),
        name=name,
    )(*args)


def total(value):
    return jnp.sum(jnp.sum(value, axis=0, keepdims=True), axis=1, keepdims=True)


def lane_index(shape):
    return lax.broadcasted_iota(jnp.int32, shape, 1)


def pack_x_kernel(levels, height, mask, depth, temp, east, to_east, to_west):
    wet = mask[0].astype(jnp.float32)
    fields = (wet * height[...], wet, depth[...])
    for at, field in enumerate(fields):
        flipped = jnp.transpose(field)
        to_west[at * RING : (at + 1) * RING, :] = flipped[:RING]
        to_east[at * RING : (at + 1) * RING, :] = flipped[-RING:]
    base = 3 * RING
    for level in range(levels):
        masked = mask[level].astype(jnp.float32) * temp[level]
        flux_east = (DIFFUSE - 0.5 * east[level]) * masked
        flux_west = (DIFFUSE + 0.5 * east[level]) * masked
        last = jnp.transpose(flux_east[:, -LANES:])
        first = jnp.transpose(flux_west[:, :LANES])
        to_east[base + level : base + level + 1, :] = last[-1:]
        to_west[base + level : base + level + 1, :] = first[:1]


def pack_y_kernel(
    levels, height, mask, depth, temp, north, from_west, from_east, sides, tracer_sides, to_north, to_south
):
    rows, columns = height.shape
    wet = mask[0].astype(jnp.float32)
    fields = (wet * height[...], wet, depth[...])
    for at, field in enumerate(fields):
        span = slice(at * RING, (at + 1) * RING)
        middle = jnp.zeros((LANES - 2 * RING, rows), jnp.float32)
        side = jnp.transpose(jnp.concatenate([from_east[span, :], middle, from_west[span, :]], axis=0))
        sides[at] = side
        to_north[span, :columns] = field[-RING:]
        to_north[span, columns:] = side[-RING:]
        to_south[span, :columns] = field[:RING]
        to_south[span, columns:] = side[:RING]
    base = 3 * RING
    span = slice(base, base + levels)
    middle = jnp.zeros((LANES - 2 * levels, rows), jnp.float32)
    tracer_sides[...] = jnp.transpose(
        jnp.concatenate([from_east[span, :], middle, from_west[span, :]], axis=0)
    )
    to_north[span, columns:] = jnp.zeros((levels, LANES), jnp.float32)
    to_south[span, columns:] = jnp.zeros((levels, LANES), jnp.float32)
    for level in range(levels):
        masked = mask[level].astype(jnp.float32) * temp[level]
        flux_north = (DIFFUSE - 0.5 * north[level]) * masked
        flux_south = (DIFFUSE + 0.5 * north[level]) * masked
        to_north[base + level : base + level + 1, :columns] = flux_north[-1:]
        to_south[base + level : base + level + 1, :columns] = flux_south[:1]


def tile_basis_kernel(height, mask, depth, row_out):
    rows, columns = height.shape
    wet = mask[0].astype(jnp.float32)
    deep = depth[...]
    row = lax.broadcasted_iota(jnp.int32, (rows, columns), 0)
    lane = lane_index((rows, columns))
    east_weight = (
        STIFFNESS * 0.5 * (deep + pltpu.roll(deep, columns - 1, 1)) * wet * pltpu.roll(wet, columns - 1, 1)
    )
    east_weight = jnp.where(lane == columns - 1, 0.0, east_weight)
    west_weight = pltpu.roll(east_weight, 1, 1)
    north_weight = STIFFNESS * 0.5 * (deep + pltpu.roll(deep, rows - 1, 0)) * wet * pltpu.roll(wet, rows - 1, 0)
    north_weight = jnp.where(row == rows - 1, 0.0, north_weight)
    south_weight = pltpu.roll(north_weight, 1, 0)

    def spread(field):
        out = west_weight * (field - pltpu.roll(field, 1, 1))
        out = out + east_weight * (field - pltpu.roll(field, columns - 1, 1))
        out = out + south_weight * (field - pltpu.roll(field, 1, 0))
        return out + north_weight * (field - pltpu.roll(field, rows - 1, 0))

    field = wet * height[...]
    square = total(field * field)
    weight = jnp.sqrt(square)
    vector = field * jnp.where(square > 0.0, lax.rsqrt(jnp.maximum(square, 1e-30)), 0.0)
    before, link = jnp.zeros_like(vector), jnp.zeros_like(square)
    at = lane_index((1, LANES))
    out = jnp.where(at == WEIGHT_AT, weight, 0.0)
    for step in range(ITERS):
        image = spread(vector) - link * before
        along, size = total(image * vector), total(image * image)
        out = jnp.where(at == step, along, out)
        if step + 1 < ITERS:
            left = size - along * along
            alive = left > 1e-6 * size
            scale = jnp.where(alive, lax.rsqrt(jnp.maximum(left, 1e-30)), 0.0)
            link = jnp.where(alive, jnp.sqrt(jnp.maximum(left, 0.0)), 0.0)
            before, vector = vector, (image - along * vector) * scale
            out = jnp.where(at == OFF_AT + step, link, out)
    row_out[...] = out


def merged_recurrence(tiles):
    at = lane_index(tiles.shape)
    diagonal = jnp.where(at < ITERS, tiles, 0.0)
    above = jnp.where(at < ITERS - 1, pltpu.roll(tiles, LANES - OFF_AT, 1), 0.0)
    below = pltpu.roll(above, 1, 1)
    vector = jnp.where(at == 0, pltpu.roll(tiles, LANES - WEIGHT_AT, 1), 0.0)
    square = total(vector * vector)
    vector = vector * jnp.where(square > 0.0, lax.rsqrt(jnp.maximum(square, 1e-30)), 0.0)
    before, link = jnp.zeros_like(vector), jnp.zeros_like(square)
    running = jnp.ones_like(square)
    steps = []
    for step in range(ITERS):
        image = diagonal * vector - link * before
        image = image + above * pltpu.roll(vector, LANES - 1, 1) + below * pltpu.roll(vector, 1, 1)
        along, size = total(image * vector), total(image * image)
        left = size - along * along
        alive = left > 1e-6 * size
        middle = jnp.where(running > 0.0, along, 4.0 * STIFFNESS)
        back = link
        scale = jnp.where(alive, lax.rsqrt(jnp.maximum(left, 1e-30)), 0.0)
        link = jnp.where(alive, jnp.sqrt(jnp.maximum(left, 0.0)), 0.0)
        steps.append((middle, jnp.where(alive, link, 2.0 * STIFFNESS), back))
        running = jnp.where(alive, running, 0.0)
        before, vector = vector, (image - along * vector) * scale
    return steps


def krylov_kernel(
    height, mask, depth, sides, from_south, from_north, tiles, basis, ground, products, steps_out
):
    rows, columns = height.shape
    full_rows, full_columns = rows + 2 * RING, columns + LANES
    wet = mask[0].astype(jnp.float32)
    own = (wet * height[...], wet, depth[...])

    def widened(at):
        span = slice(at * RING, (at + 1) * RING)
        tile = jnp.concatenate([own[at], sides[at]], axis=1)
        return jnp.concatenate([tile, from_north[span, :], from_south[span, :]], axis=0)

    field, opening, deep = widened(0), widened(1), widened(2)
    ground[0] = opening
    ground[1] = deep
    west_weight = STIFFNESS * 0.5 * (deep + pltpu.roll(deep, 1, 1)) * opening * pltpu.roll(opening, 1, 1)
    east_weight = pltpu.roll(west_weight, full_columns - 1, 1)
    south_weight = STIFFNESS * 0.5 * (deep + pltpu.roll(deep, 1, 0)) * opening * pltpu.roll(opening, 1, 0)
    north_weight = pltpu.roll(south_weight, full_rows - 1, 0)

    def spread(value):
        out = west_weight * (value - pltpu.roll(value, 1, 1))
        out = out + east_weight * (value - pltpu.roll(value, full_columns - 1, 1))
        out = out + south_weight * (value - pltpu.roll(value, 1, 0))
        return out + north_weight * (value - pltpu.roll(value, full_rows - 1, 0))

    steps = merged_recurrence(tiles[...])
    at = lane_index((1, LANES))
    row = jnp.zeros((1, LANES), jnp.float32)
    for step, entries in enumerate(steps):
        for kind, entry in enumerate(entries):
            row = jnp.where(at == kind * OFF_AT + step, entry, row)
    steps_out[...] = row
    vectors = [field]
    before, value = None, field
    basis[0] = field
    for step, (middle, link, back) in enumerate(steps):
        image = spread(value) - middle * value
        if step:
            image = image - back * before
        before, value = value, image * (1.0 / link)
        if step + 1 < ITERS:
            basis[step + 1] = value
        vectors.append(value)
    cut = [vector[:rows, :columns] for vector in vectors]
    partial = [jnp.sum(cut[i] * cut[j], axis=0, keepdims=True) for i, j in PAIRS]
    partial = [sum(part[:, k : k + LANES] for k in range(0, columns, LANES)) for part in partial]
    partial = partial + [jnp.zeros((LANES - len(partial), LANES), jnp.float32)]
    table = jnp.transpose(jnp.concatenate(partial, axis=0))
    products[...] = jnp.sum(table, axis=0, keepdims=True)


def solve_kernel(gathered, steps_in, basis, ground, surface, pressure):
    rows, columns = surface.shape
    count = ITERS + 1
    summed = jnp.sum(gathered[...], axis=0, keepdims=True)
    known = steps_in[...]
    at = lane_index((1, LANES))

    def entry(row, index):
        return jnp.sum(jnp.where(at == index, row, 0.0), axis=1, keepdims=True)

    gram = {}
    for index, (i, j) in enumerate(PAIRS):
        gram[i, j] = gram[j, i] = entry(summed, index)
    middle = [entry(known, step) for step in range(ITERS)]
    link = [entry(known, OFF_AT + step) for step in range(ITERS)]
    back = [entry(known, 2 * OFF_AT + step) for step in range(ITERS)]
    zero = jnp.zeros((1, 1), jnp.float32)

    def applied(vector):
        out = [zero] * (len(vector) + 1)
        for i, part in enumerate(vector):
            out[i] = out[i] + part + middle[i] * part
            out[i + 1] = out[i + 1] + link[i] * part
            if i:
                out[i - 1] = out[i - 1] + back[i] * part
        return out

    def inner(left, right):
        out = zero
        for i, a in enumerate(left):
            part = zero
            for j, b in enumerate(right):
                part = part + gram[i, j] * b
            out = out + a * part
        return out

    def scaled_add(left, scale, right):
        size = max(len(left), len(right))
        left = left + [zero] * (size - len(left))
        right = right + [zero] * (size - len(right))
        return [a + scale * b for a, b in zip(left, right)]

    residual = direction = [jnp.ones((1, 1), jnp.float32)]
    iterate = [zero]
    norm_now = gram[0, 0]
    for iteration in range(ITERS):
        image = applied(direction)
        product = inner(direction, image)
        step_size = jnp.where(product > 0.0, norm_now / product, 0.0)
        iterate = scaled_add(iterate, step_size, direction)
        if iteration + 1 < ITERS:
            residual = scaled_add(residual, -step_size, image)
            norm_next = inner(residual, residual)
            growth = jnp.where(norm_now > 0.0, norm_next / norm_now, 0.0)
            direction = scaled_add(residual, growth, direction)
            norm_now = norm_next
    value = iterate[0] * basis[0]
    for k in range(1, ITERS):
        value = value + iterate[k] * basis[k]
    surface[...] = value[:rows, :columns]
    opening = ground[0]
    load = ground[1] * value
    full_rows, full_columns = value.shape
    pull = jnp.zeros_like(load)
    for shift, axis in ((1, 1), (full_columns - 1, 1), (1, 0), (full_rows - 1, 0)):
        pull = pull + opening * pltpu.roll(opening, shift, axis) * (pltpu.roll(load, shift, axis) - load)
    pressure[...] = -GRAVITY * pull[:rows, :columns]


def tracer_kernel(levels, temp, east, north, mask, tracer_sides, from_south, from_north, tracer):
    rows, columns = temp.shape[1:]
    row = lax.broadcasted_iota(jnp.int32, (rows, columns), 0)
    lane = lane_index((rows, columns))
    base = 3 * RING
    for level in range(levels):
        masked = mask[level].astype(jnp.float32) * temp[level]
        east_coef = DIFFUSE - 0.5 * east[level]
        west_coef = DIFFUSE + 0.5 * east[level]
        north_coef = DIFFUSE - 0.5 * north[level]
        south_coef = DIFFUSE + 0.5 * north[level]
        side_west = tracer_sides[:, LANES - levels + level : LANES - levels + level + 1]
        side_east = tracer_sides[:, level : level + 1]
        side_south = from_south[base + level : base + level + 1, :columns]
        side_north = from_north[base + level : base + level + 1, :columns]
        inflow = jnp.where(lane == 0, side_west, pltpu.roll(east_coef * masked, 1, 1))
        inflow = inflow + jnp.where(
            lane == columns - 1, side_east, pltpu.roll(west_coef * masked, columns - 1, 1)
        )
        inflow = inflow + jnp.where(row == 0, side_south, pltpu.roll(north_coef * masked, 1, 0))
        inflow = inflow + jnp.where(
            row == rows - 1, side_north, pltpu.roll(south_coef * masked, rows - 1, 0)
        )
        tracer[level] = masked + TIMESTEP * (
            inflow - (east_coef + west_coef + north_coef + south_coef) * masked
        )


def level_of_slot(slots, slot, levels):
    level = jnp.int32(0)
    for k in range(1, levels):
        level = jnp.where(slots[k] == slot, jnp.int32(k), level)
    return level


def density(level, levels, pressure, mask):
    thickness = 1.0 + level.astype(jnp.float32) / levels
    return thickness * pressure[...] * mask[level].astype(jnp.float32)


def warm_kernel(levels, sizes, slots, tracer, pressure, mask, *refs):
    parts, (partial, salt) = refs[: len(sizes)], refs[len(sizes) :]
    slot = 0
    for size, part in zip(sizes, parts):
        for at in range(size):
            level = level_of_slot(slots, slot, levels)
            dense = density(level, levels, pressure, mask)
            warm = part[at]
            salt[level] = (HALINE + CABBELING * warm) * dense
            partial[level] = tracer[level] + (THERMAL + 2.0 * NONLINEAR * warm) * dense
            slot += 1


def salt_kernel(levels, sizes, slots, partial, pressure, mask, *refs):
    parts, result = refs[: len(sizes)], refs[len(sizes)]
    slot = 0
    for size, part in zip(sizes, parts):
        for at in range(size):
            level = level_of_slot(slots, slot, levels)
            dense = density(level, levels, pressure, mask)
            result[level] = partial[level] + CABBELING * part[at] * dense
            slot += 1


def shifted(value, axis, steps, around):
    count = lax.axis_size(axis)
    pairs = [(i, (i + steps) % count) for i in range(count) if around or 0 <= i + steps < count]
    return lax.ppermute(value, axis, pairs)


def shared(row):
    axes = ("gx", "gy")
    count = lax.axis_size("gx") * lax.axis_size("gy")
    rows = jnp.broadcast_to(row[None], (count,) + row.shape)
    return lax.all_to_all(rows, axes, 0, 0).reshape(count, LANES)


def body(
    temp_adjoint,
    height_adjoint,
    east_velocity,
    north_velocity,
    temp_store,
    salt_store,
    slot_map,
    land_mask,
    ocean_depth,
):
    levels, rows, columns = temp_adjoint.shape
    half_cycle = lax.axis_size("gx") // 2
    strip = 3 * RING + levels
    full = (rows + 2 * RING, columns + LANES)
    surface_args = (height_adjoint, land_mask, ocean_depth)

    def fetched(store, sizes):
        parts, start = [], 0
        for size in sizes:
            parts.append(shifted(lax.slice_in_dim(store, start, start + size), "gx", half_cycle, True))
            start += size
        return parts

    sizes = (levels // 2, levels - levels // 2)
    slots = shifted(slot_map, "gx", half_cycle, True).reshape(-1)
    warm_parts = fetched(temp_store, sizes)
    salt_parts = fetched(salt_store, sizes)

    to_east, to_west = call(
        functools.partial(pack_x_kernel, levels),
        [(strip, rows)] * 2,
        surface_args + (temp_adjoint, east_velocity),
        name="pack_x",
    )
    from_west = shifted(to_east, "gx", 1, True)
    from_east = shifted(to_west, "gx", -1, True)
    (tile_row,) = call(tile_basis_kernel, [(1, LANES)], surface_args, name="tile_basis")
    tiles = shared(tile_row)
    sides, tracer_sides, to_north, to_south = call(
        functools.partial(pack_y_kernel, levels),
        [(3, rows, LANES), (rows, LANES), (strip, full[1]), (strip, full[1])],
        surface_args + (temp_adjoint, north_velocity, from_west, from_east),
        name="pack_y",
    )
    from_south = shifted(to_north, "gy", 1, False)
    from_north = shifted(to_south, "gy", -1, False)
    basis, ground, products, steps = call(
        krylov_kernel,
        [(ITERS,) + full, (2,) + full, (1, LANES), (1, LANES)],
        surface_args + (sides, from_south, from_north, tiles),
        name="krylov",
    )
    gathered = shared(products)
    (tracer,) = call(
        functools.partial(tracer_kernel, levels),
        [temp_adjoint.shape],
        (temp_adjoint, east_velocity, north_velocity, land_mask, tracer_sides, from_south, from_north),
        name="tracer",
    )
    surface, pressure = call(
        solve_kernel,
        [(rows, columns)] * 2,
        (gathered, steps, basis, ground),
        name="solve",
    )
    partial, salt_back = call(
        functools.partial(warm_kernel, levels, sizes),
        [temp_adjoint.shape] * 2,
        (slots, tracer, pressure, land_mask, *warm_parts),
        specs=[SMEM] + [VMEM] * (3 + len(sizes)),
        name="warm",
    )
    (temp_back,) = call(
        functools.partial(salt_kernel, levels, sizes),
        [temp_adjoint.shape],
        (slots, partial, pressure, land_mask, *salt_parts),
        specs=[SMEM] + [VMEM] * (3 + len(sizes)),
        name="salt",
    )
    return (temp_back, salt_back, surface)


def solution(mesh):
    return jax.shard_map(
        body,
        mesh=mesh,
        in_specs=(
            P(None, "gy", "gx"),
            P("gy", "gx"),
            P(None, "gy", "gx"),
            P(None, "gy", "gx"),
            P(None, "gy", "gx"),
            P(None, "gy", "gx"),
            P("gx", "gy", None),
            P(None, "gy", "gx"),
            P("gy", "gx"),
        ),
        out_specs=(P(None, "gy", "gx"), P(None, "gy", "gx"), P("gy", "gx")),
        check_vma=False,
    )
```

```python
import functools

import jax
import jax.numpy as jnp
from jax import lax
from jax.experimental import pallas as pl
from jax.experimental.pallas import tpu as pltpu
from jax.sharding import PartitionSpec as P


ITERS = 6
RING = 8
KERNEL_VMEM = 16 * 1024 * 1024
LANES = 128

DIFFUSE = 0.2
TIMESTEP = 1.0
STIFFNESS = 8.0
GRAVITY = 4.0
THERMAL = 0.5
NONLINEAR = 0.4
CABBELING = 0.3
HALINE = 0.8


VMEM = pl.BlockSpec(memory_space=pltpu.VMEM)
SMEM = pl.BlockSpec(memory_space=pltpu.SMEM)
HBM = pl.BlockSpec(memory_space=pltpu.HBM)

OFF_AT, WEIGHT_AT = 16, 32
PAIRS = [(i, j) for i in range(ITERS + 1) for j in range(i, ITERS + 1)]


def call(kernel, outs, args, specs=None, keep=None, flops=4000000):
    specs = specs or [VMEM] * len(args)
    keep = keep or [True] * len(outs)
    args = [
        pltpu.with_memory_space_constraint(arg, pltpu.VMEM) if held else arg for arg, held in args
    ]
    shapes = [
        pltpu.VMEM(shape, jnp.float32) if kept else jax.ShapeDtypeStruct(shape, jnp.float32)
        for shape, kept in zip(outs, keep)
    ]
    return pl.pallas_call(
        kernel,
        out_shape=shapes,
        in_specs=specs,
        out_specs=[VMEM] * len(outs),
        compiler_params=pltpu.CompilerParams(vmem_limit_bytes=KERNEL_VMEM),
        cost_estimate=pl.CostEstimate(flops=flops, bytes_accessed=1000000, transcendentals=0),
    )(*args)


def held(*arrays):
    return tuple((array, True) for array in arrays)


def free(*arrays):
    return tuple((array, False) for array in arrays)


def total(value):
    return jnp.sum(jnp.sum(value, axis=0, keepdims=True), axis=1, keepdims=True)


def lane_index(shape):
    return lax.broadcasted_iota(jnp.int32, shape, 1)


def pack_x_kernel(levels, height, mask, depth, temp, east, to_east, to_west):
    wet = mask[0].astype(jnp.float32)
    fields = (wet * height[...], wet, depth[...])
    for at, field in enumerate(fields):
        flipped = jnp.transpose(field)
        to_west[at * RING : (at + 1) * RING, :] = flipped[:RING]
        to_east[at * RING : (at + 1) * RING, :] = flipped[-RING:]
    base = 3 * RING
    for level in range(levels):
        masked = mask[level].astype(jnp.float32) * temp[level]
        flux_east = (DIFFUSE - 0.5 * east[level]) * masked
        flux_west = (DIFFUSE + 0.5 * east[level]) * masked
        last = jnp.transpose(flux_east[:, -LANES:])
        first = jnp.transpose(flux_west[:, :LANES])
        to_east[base + level : base + level + 1, :] = last[-1:]
        to_west[base + level : base + level + 1, :] = first[:1]


def pack_y_kernel(
    levels, height, mask, depth, temp, north, from_west, from_east, sides, tracer_sides, to_north, to_south
):
    rows, columns = height.shape
    wet = mask[0].astype(jnp.float32)
    fields = (wet * height[...], wet, depth[...])
    for at, field in enumerate(fields):
        span = slice(at * RING, (at + 1) * RING)
        middle = jnp.zeros((LANES - 2 * RING, rows), jnp.float32)
        side = jnp.transpose(jnp.concatenate([from_east[span, :], middle, from_west[span, :]], axis=0))
        sides[at] = side
        to_north[span, :columns] = field[-RING:]
        to_north[span, columns:] = side[-RING:]
        to_south[span, :columns] = field[:RING]
        to_south[span, columns:] = side[:RING]
    base = 3 * RING
    span = slice(base, base + levels)
    middle = jnp.zeros((LANES - 2 * levels, rows), jnp.float32)
    tracer_sides[...] = jnp.transpose(
        jnp.concatenate([from_east[span, :], middle, from_west[span, :]], axis=0)
    )
    to_north[span, columns:] = jnp.zeros((levels, LANES), jnp.float32)
    to_south[span, columns:] = jnp.zeros((levels, LANES), jnp.float32)
    for level in range(levels):
        masked = mask[level].astype(jnp.float32) * temp[level]
        flux_north = (DIFFUSE - 0.5 * north[level]) * masked
        flux_south = (DIFFUSE + 0.5 * north[level]) * masked
        to_north[base + level : base + level + 1, :columns] = flux_north[-1:]
        to_south[base + level : base + level + 1, :columns] = flux_south[:1]


def tile_basis_kernel(height, mask, depth, row_out):
    rows, columns = height.shape
    wet = mask[0].astype(jnp.float32)
    deep = depth[...]
    row = lax.broadcasted_iota(jnp.int32, (rows, columns), 0)
    lane = lane_index((rows, columns))
    east_weight = (
        STIFFNESS * 0.5 * (deep + pltpu.roll(deep, columns - 1, 1)) * wet * pltpu.roll(wet, columns - 1, 1)
    )
    east_weight = jnp.where(lane == columns - 1, 0.0, east_weight)
    west_weight = pltpu.roll(east_weight, 1, 1)
    north_weight = STIFFNESS * 0.5 * (deep + pltpu.roll(deep, rows - 1, 0)) * wet * pltpu.roll(wet, rows - 1, 0)
    north_weight = jnp.where(row == rows - 1, 0.0, north_weight)
    south_weight = pltpu.roll(north_weight, 1, 0)

    def spread(field):
        out = west_weight * (field - pltpu.roll(field, 1, 1))
        out = out + east_weight * (field - pltpu.roll(field, columns - 1, 1))
        out = out + south_weight * (field - pltpu.roll(field, 1, 0))
        return out + north_weight * (field - pltpu.roll(field, rows - 1, 0))

    field = wet * height[...]
    square = total(field * field)
    weight = jnp.sqrt(square)
    vector = field * jnp.where(square > 0.0, lax.rsqrt(jnp.maximum(square, 1e-30)), 0.0)
    before, link = jnp.zeros_like(vector), jnp.zeros_like(square)
    at = lane_index((1, LANES))
    out = jnp.where(at == WEIGHT_AT, weight, 0.0)
    for step in range(ITERS):
        image = spread(vector) - link * before
        along, size = total(image * vector), total(image * image)
        out = jnp.where(at == step, along, out)
        if step + 1 < ITERS:
            left = size - along * along
            alive = left > 1e-6 * size
            scale = jnp.where(alive, lax.rsqrt(jnp.maximum(left, 1e-30)), 0.0)
            link = jnp.where(alive, jnp.sqrt(jnp.maximum(left, 0.0)), 0.0)
            before, vector = vector, (image - along * vector) * scale
            out = jnp.where(at == OFF_AT + step, link, out)
    row_out[...] = out


def merged_recurrence(tiles):
    at = lane_index(tiles.shape)
    diagonal = jnp.where(at < ITERS, tiles, 0.0)
    above = jnp.where(at < ITERS - 1, pltpu.roll(tiles, LANES - OFF_AT, 1), 0.0)
    below = pltpu.roll(above, 1, 1)
    vector = jnp.where(at == 0, pltpu.roll(tiles, LANES - WEIGHT_AT, 1), 0.0)
    square = total(vector * vector)
    vector = vector * jnp.where(square > 0.0, lax.rsqrt(jnp.maximum(square, 1e-30)), 0.0)
    before, link = jnp.zeros_like(vector), jnp.zeros_like(square)
    running = jnp.ones_like(square)
    steps = []
    for _ in range(ITERS):
        image = diagonal * vector - link * before
        image = image + above * pltpu.roll(vector, LANES - 1, 1) + below * pltpu.roll(vector, 1, 1)
        along, size = total(image * vector), total(image * image)
        left = size - along * along
        alive = left > 1e-6 * size
        middle = jnp.where(running > 0.0, along, 4.0 * STIFFNESS)
        back = link
        scale = jnp.where(alive, lax.rsqrt(jnp.maximum(left, 1e-30)), 0.0)
        link = jnp.where(alive, jnp.sqrt(jnp.maximum(left, 0.0)), 0.0)
        steps.append((middle, jnp.where(alive, link, 2.0 * STIFFNESS), back))
        running = jnp.where(alive, running, 0.0)
        before, vector = vector, (image - along * vector) * scale
    return steps


def krylov_kernel(
    height, mask, depth, sides, from_south, from_north, tiles, basis, ground, products, steps_out
):
    rows, columns = height.shape
    full_rows, full_columns = rows + 2 * RING, columns + LANES
    wet = mask[0].astype(jnp.float32)
    own = (wet * height[...], wet, depth[...])

    def widened(at):
        span = slice(at * RING, (at + 1) * RING)
        tile = jnp.concatenate([own[at], sides[at]], axis=1)
        return jnp.concatenate([tile, from_north[span, :], from_south[span, :]], axis=0)

    field, opening, deep = widened(0), widened(1), widened(2)
    ground[0] = opening
    ground[1] = deep
    west_weight = STIFFNESS * 0.5 * (deep + pltpu.roll(deep, 1, 1)) * opening * pltpu.roll(opening, 1, 1)
    east_weight = pltpu.roll(west_weight, full_columns - 1, 1)
    south_weight = STIFFNESS * 0.5 * (deep + pltpu.roll(deep, 1, 0)) * opening * pltpu.roll(opening, 1, 0)
    north_weight = pltpu.roll(south_weight, full_rows - 1, 0)

    def spread(value):
        out = west_weight * (value - pltpu.roll(value, 1, 1))
        out = out + east_weight * (value - pltpu.roll(value, full_columns - 1, 1))
        out = out + south_weight * (value - pltpu.roll(value, 1, 0))
        return out + north_weight * (value - pltpu.roll(value, full_rows - 1, 0))

    steps = merged_recurrence(tiles[...])
    at = lane_index((1, LANES))
    row = jnp.zeros((1, LANES), jnp.float32)
    for step, entries in enumerate(steps):
        for kind, entry in enumerate(entries):
            row = jnp.where(at == kind * OFF_AT + step, entry, row)
    steps_out[...] = row
    vectors = [field]
    before, value = None, field
    basis[0] = field
    for step, (middle, link, back) in enumerate(steps):
        image = spread(value) - middle * value
        if step:
            image = image - back * before
        before, value = value, image * (1.0 / link)
        if step + 1 < ITERS:
            basis[step + 1] = value
        vectors.append(value)
    cut = [vector[:rows, :columns] for vector in vectors]
    partial = [jnp.sum(cut[i] * cut[j], axis=0, keepdims=True) for i, j in PAIRS]
    partial = [sum(part[:, k : k + LANES] for k in range(0, columns, LANES)) for part in partial]
    partial = partial + [jnp.zeros((LANES - len(partial), LANES), jnp.float32)]
    table = jnp.transpose(jnp.concatenate(partial, axis=0))
    products[...] = jnp.sum(table, axis=0, keepdims=True)


def solve_kernel(gathered, steps_in, basis, ground, surface, pressure):
    rows, columns = surface.shape
    summed = jnp.sum(gathered[...], axis=0, keepdims=True)
    known = steps_in[...]
    at = lane_index((1, LANES))

    def entry(row, index):
        return jnp.sum(jnp.where(at == index, row, 0.0), axis=1, keepdims=True)

    gram = {}
    for index, (i, j) in enumerate(PAIRS):
        gram[i, j] = gram[j, i] = entry(summed, index)
    middle = [entry(known, step) for step in range(ITERS)]
    link = [entry(known, OFF_AT + step) for step in range(ITERS)]
    back = [entry(known, 2 * OFF_AT + step) for step in range(ITERS)]
    zero = jnp.zeros((1, 1), jnp.float32)

    def applied(vector):
        out = [zero] * (len(vector) + 1)
        for i, part in enumerate(vector):
            out[i] = out[i] + part + middle[i] * part
            out[i + 1] = out[i + 1] + link[i] * part
            if i:
                out[i - 1] = out[i - 1] + back[i] * part
        return out

    def inner(left, right):
        out = zero
        for i, a in enumerate(left):
            part = zero
            for j, b in enumerate(right):
                part = part + gram[i, j] * b
            out = out + a * part
        return out

    def scaled_add(left, scale, right):
        size = max(len(left), len(right))
        left = left + [zero] * (size - len(left))
        right = right + [zero] * (size - len(right))
        return [a + scale * b for a, b in zip(left, right)]

    residual = direction = [jnp.ones((1, 1), jnp.float32)]
    iterate = [zero]
    norm_now = gram[0, 0]
    for iteration in range(ITERS):
        image = applied(direction)
        product = inner(direction, image)
        step_size = jnp.where(product > 0.0, norm_now / product, 0.0)
        iterate = scaled_add(iterate, step_size, direction)
        if iteration + 1 < ITERS:
            residual = scaled_add(residual, -step_size, image)
            norm_next = inner(residual, residual)
            growth = jnp.where(norm_now > 0.0, norm_next / norm_now, 0.0)
            direction = scaled_add(residual, growth, direction)
            norm_now = norm_next
    value = iterate[0] * basis[0]
    for k in range(1, ITERS):
        value = value + iterate[k] * basis[k]
    surface[...] = value[:rows, :columns]
    opening = ground[0]
    load = ground[1] * value
    full_rows, full_columns = value.shape
    pull = jnp.zeros_like(load)
    for shift, axis in ((1, 1), (full_columns - 1, 1), (1, 0), (full_rows - 1, 0)):
        pull = pull + opening * pltpu.roll(opening, shift, axis) * (pltpu.roll(load, shift, axis) - load)
    pressure[...] = -GRAVITY * pull[:rows, :columns]


def tracer_kernel(levels, temp, east, north, mask, tracer_sides, from_south, from_north, tracer):
    rows, columns = temp.shape[1:]
    row = lax.broadcasted_iota(jnp.int32, (rows, columns), 0)
    lane = lane_index((rows, columns))
    base = 3 * RING
    for level in range(levels):
        masked = mask[level].astype(jnp.float32) * temp[level]
        east_coef = DIFFUSE - 0.5 * east[level]
        west_coef = DIFFUSE + 0.5 * east[level]
        north_coef = DIFFUSE - 0.5 * north[level]
        south_coef = DIFFUSE + 0.5 * north[level]
        side_west = tracer_sides[:, LANES - levels + level : LANES - levels + level + 1]
        side_east = tracer_sides[:, level : level + 1]
        side_south = from_south[base + level : base + level + 1, :columns]
        side_north = from_north[base + level : base + level + 1, :columns]
        inflow = jnp.where(lane == 0, side_west, pltpu.roll(east_coef * masked, 1, 1))
        inflow = inflow + jnp.where(
            lane == columns - 1, side_east, pltpu.roll(west_coef * masked, columns - 1, 1)
        )
        inflow = inflow + jnp.where(row == 0, side_south, pltpu.roll(north_coef * masked, 1, 0))
        inflow = inflow + jnp.where(
            row == rows - 1, side_north, pltpu.roll(south_coef * masked, rows - 1, 0)
        )
        tracer[level] = masked + TIMESTEP * (
            inflow - (east_coef + west_coef + north_coef + south_coef) * masked
        )


def level_of_slot(slots, slot, levels):
    level = jnp.int32(0)
    for k in range(1, levels):
        level = jnp.where(slots[k] == slot, jnp.int32(k), level)
    return level


def density(level, levels, pressure, mask):
    thickness = 1.0 + level.astype(jnp.float32) / levels
    return thickness * pressure[...] * mask[level].astype(jnp.float32)


def warm_kernel(levels, sizes, slots, tracer, pressure, mask, *refs):
    parts, (partial, salt) = refs[: len(sizes)], refs[len(sizes) :]
    slot = 0
    for size, part in zip(sizes, parts):
        for at in range(size):
            level = level_of_slot(slots, slot, levels)
            dense = density(level, levels, pressure, mask)
            warm = part[at]
            salt[level] = (HALINE + CABBELING * warm) * dense
            partial[level] = tracer[level] + (THERMAL + 2.0 * NONLINEAR * warm) * dense
            slot += 1


def salt_kernel(levels, first, slots, partial, pressure, mask, part, *refs):
    result, done, sems = refs[-3:]
    size = part.shape[0]
    copies = []
    for at in range(size):
        level = level_of_slot(slots, first + at, levels)
        dense = density(level, levels, pressure, mask)
        done[at] = partial[level] + CABBELING * part[at] * dense
        copies.append(pltpu.make_async_copy(done.at[at], result.at[level], sems.at[at]))
        copies[-1].start()
    for copy in copies:
        copy.wait()


def finish(levels, first, args, before):
    part = args[-1]
    shape = (levels,) + part.shape[1:]
    held_args = [pltpu.with_memory_space_constraint(arg, pltpu.VMEM) for arg in args[1:]]
    operands = [args[0]] + held_args + ([] if before is None else [before])
    return pl.pallas_call(
        functools.partial(salt_kernel, levels, first),
        out_shape=jax.ShapeDtypeStruct(shape, jnp.float32),
        in_specs=[SMEM] + [VMEM] * len(held_args) + ([] if before is None else [HBM]),
        out_specs=HBM,
        scratch_shapes=[
            pltpu.VMEM(part.shape, jnp.float32),
            pltpu.SemaphoreType.DMA((part.shape[0],)),
        ],
        input_output_aliases={} if before is None else {len(operands) - 1: 0},
        compiler_params=pltpu.CompilerParams(vmem_limit_bytes=KERNEL_VMEM),
        cost_estimate=pl.CostEstimate(flops=1000000, bytes_accessed=1000000, transcendentals=0),
    )(*operands)


def shifted(value, axis, steps, around):
    count = lax.axis_size(axis)
    pairs = [(i, (i + steps) % count) for i in range(count) if around or 0 <= i + steps < count]
    return lax.ppermute(value, axis, pairs)


def shared(row):
    axes = ("gx", "gy")
    count = lax.axis_size("gx") * lax.axis_size("gy")
    rows = jnp.broadcast_to(row[None], (count,) + row.shape)
    rows = lax.all_to_all(rows, axes, 0, 0)
    return rows.reshape(count, LANES)


def runs(levels):
    quarter, half = levels // 4, levels // 2
    return (quarter, quarter, levels - 2 * quarter), (half, levels - half)


def body(
    temp_adjoint,
    height_adjoint,
    east_velocity,
    north_velocity,
    temp_store,
    salt_store,
    slot_map,
    land_mask,
    ocean_depth,
):
    levels, rows, columns = temp_adjoint.shape
    half_cycle = lax.axis_size("gx") // 2
    strip = 3 * RING + levels
    full = (rows + 2 * RING, columns + LANES)
    surface_args = free(height_adjoint, land_mask, ocean_depth)

    def fetched(store, sizes):
        parts, start = [], 0
        for size in sizes:
            part = lax.slice_in_dim(store, start, start + size)
            parts.append(shifted(part, "gx", half_cycle, True))
            start += size
        return parts

    warm_sizes, salt_sizes = runs(levels)
    slots = shifted(slot_map, "gx", half_cycle, True).reshape(-1)
    warm_parts = fetched(temp_store, warm_sizes)
    salt_parts = fetched(salt_store, salt_sizes)

    to_east, to_west = call(
        functools.partial(pack_x_kernel, levels), [(strip, rows)] * 2, surface_args + free(temp_adjoint, east_velocity)
    )
    from_west = shifted(to_east, "gx", 1, True)
    from_east = shifted(to_west, "gx", -1, True)
    (tile_row,) = call(tile_basis_kernel, [(1, LANES)], surface_args)
    tiles = shared(tile_row)
    sides, tracer_sides, to_north, to_south = call(
        functools.partial(pack_y_kernel, levels),
        [(3, rows, LANES), (rows, LANES), (strip, full[1]), (strip, full[1])],
        surface_args + free(temp_adjoint, north_velocity) + held(from_west, from_east),
    )
    from_south = shifted(to_north, "gy", 1, False)
    from_north = shifted(to_south, "gy", -1, False)
    basis, ground, products, steps = call(
        krylov_kernel,
        [(ITERS,) + full, (2,) + full, (1, LANES), (1, LANES)],
        surface_args + held(sides, from_south, from_north, tiles),
    )
    gathered = shared(products)
    (tracer,) = call(
        functools.partial(tracer_kernel, levels),
        [temp_adjoint.shape],
        free(temp_adjoint, east_velocity, north_velocity, land_mask)
        + held(tracer_sides, from_south, from_north),
    )
    surface, pressure = call(
        solve_kernel, [(rows, columns)] * 2, held(gathered, steps, basis, ground), keep=[False, True]
    )
    partial, salt_back = call(
        functools.partial(warm_kernel, levels, warm_sizes),
        [temp_adjoint.shape] * 2,
        free(slots) + held(tracer, pressure, land_mask, *warm_parts),
        specs=[SMEM] + [VMEM] * (3 + len(warm_sizes)),
        keep=[True, False],
    )
    temp_back, first = None, 0
    for size, part in zip(salt_sizes, salt_parts):
        args = (slots, partial, pressure, land_mask, part)
        temp_back = finish(levels, first, args, temp_back)
        first += size
    return (temp_back, salt_back, surface)


def solution(mesh):
    return jax.shard_map(
        body,
        mesh=mesh,
        in_specs=(
            P(None, "gy", "gx"),
            P("gy", "gx"),
            P(None, "gy", "gx"),
            P(None, "gy", "gx"),
            P(None, "gy", "gx"),
            P(None, "gy", "gx"),
            P("gx", "gy", None),
            P(None, "gy", "gx"),
            P("gy", "gx"),
        ),
        out_specs=(P(None, "gy", "gx"), P(None, "gy", "gx"), P("gy", "gx")),
        check_vma=False,
    )
```

```python
import functools

import jax
import jax.numpy as jnp
from jax import lax
from jax.experimental import pallas as pl
from jax.experimental.pallas import tpu as pltpu
from jax.sharding import PartitionSpec as P


ITERS = 6
RING = 8
KERNEL_VMEM = 16 * 1024 * 1024
LANES = 128

DIFFUSE = 0.2
TIMESTEP = 1.0
STIFFNESS = 8.0
GRAVITY = 4.0
THERMAL = 0.5
NONLINEAR = 0.4
CABBELING = 0.3
HALINE = 0.8


VMEM = pl.BlockSpec(memory_space=pltpu.VMEM)
SMEM = pl.BlockSpec(memory_space=pltpu.SMEM)
HBM = pl.BlockSpec(memory_space=pltpu.HBM)

OFF_AT, WEIGHT_AT = 16, 32
PAIRS = [(i, j) for i in range(ITERS + 1) for j in range(i, ITERS + 1)]


def call(kernel, outs, args, specs=None, keep=None, grid=(), flops=4000000):
    specs = specs or [VMEM] * len(args)
    keep = keep or [True] * len(outs)
    args = [
        arg if space is None else pltpu.with_memory_space_constraint(arg, space) for arg, space in args
    ]
    shapes = [
        pltpu.VMEM(shape, jnp.float32) if kept else jax.ShapeDtypeStruct(shape, jnp.float32)
        for shape, kept in zip(outs, keep)
    ]
    return pl.pallas_call(
        kernel,
        out_shape=shapes,
        grid=grid,
        in_specs=specs,
        out_specs=[VMEM] * len(outs),
        compiler_params=pltpu.CompilerParams(vmem_limit_bytes=KERNEL_VMEM),
        cost_estimate=pl.CostEstimate(flops=flops, bytes_accessed=1000000, transcendentals=0),
    )(*args)


def held(*arrays):
    return tuple((array, pltpu.VMEM) for array in arrays)


def stored(*arrays):
    return tuple((array, pltpu.HBM) for array in arrays)


def free(*arrays):
    return tuple((array, None) for array in arrays)


def total(value):
    return jnp.sum(jnp.sum(value, axis=0, keepdims=True), axis=1, keepdims=True)


def lane_index(shape):
    return lax.broadcasted_iota(jnp.int32, shape, 1)


def pack_y_kernel(levels, height, mask, depth, temp, north, to_north, to_south):
    wet = mask[0].astype(jnp.float32)
    fields = (wet * height[...], wet, depth[...])
    for at, field in enumerate(fields):
        to_south[at * RING : (at + 1) * RING, :] = field[:RING]
        to_north[at * RING : (at + 1) * RING, :] = field[-RING:]
    base = 3 * RING
    for level in range(levels):
        first, last = slice(0, RING), slice(temp.shape[1] - RING, temp.shape[1])
        flux_south = (DIFFUSE + 0.5 * north[level, first]) * (
            mask[level, first].astype(jnp.float32) * temp[level, first]
        )
        flux_north = (DIFFUSE - 0.5 * north[level, last]) * (
            mask[level, last].astype(jnp.float32) * temp[level, last]
        )
        to_south[base + level : base + level + 1, :] = flux_south[:1]
        to_north[base + level : base + level + 1, :] = flux_north[-1:]


def pack_x_kernel(
    levels, height, mask, depth, temp, east, from_south, from_north, to_east, to_west
):
    rows = height.shape[0]
    wet = mask[0].astype(jnp.float32)
    fields = (wet * height[...], wet, depth[...])
    for at, field in enumerate(fields):
        span = slice(at * RING, (at + 1) * RING)
        beside = [from_north[span, :], from_south[span, :]]
        beside.append(jnp.zeros((LANES - 2 * RING, field.shape[1]), jnp.float32))
        flipped = jnp.transpose(jnp.concatenate([field] + beside, axis=0))
        to_west[span, :] = flipped[:RING]
        to_east[span, :] = flipped[-RING:]
    base = 3 * RING
    for level in range(levels):
        at = slice(base + level, base + level + 1)
        masked = mask[level].astype(jnp.float32) * temp[level]
        flux_east = (DIFFUSE - 0.5 * east[level]) * masked
        flux_west = (DIFFUSE + 0.5 * east[level]) * masked
        to_east[at, :rows] = jnp.transpose(flux_east[:, -LANES:])[-1:]
        to_west[at, :rows] = jnp.transpose(flux_west[:, :LANES])[:1]
    spare = slice(base, base + levels)
    to_east[spare, rows:] = jnp.zeros((levels, LANES), jnp.float32)
    to_west[spare, rows:] = jnp.zeros((levels, LANES), jnp.float32)


def beside_tile(from_west, from_east, start, size):
    span = slice(start, start + size)
    middle = jnp.zeros((LANES - 2 * size, from_west.shape[1]), jnp.float32)
    return jnp.transpose(jnp.concatenate([from_east[span, :], middle, from_west[span, :]], axis=0))


def tile_basis_kernel(height, mask, depth, row_out):
    rows, columns = height.shape
    wet = mask[0].astype(jnp.float32)
    deep = depth[...]
    row = lax.broadcasted_iota(jnp.int32, (rows, columns), 0)
    lane = lane_index((rows, columns))
    east_weight = (
        STIFFNESS * 0.5 * (deep + pltpu.roll(deep, columns - 1, 1)) * wet * pltpu.roll(wet, columns - 1, 1)
    )
    east_weight = jnp.where(lane == columns - 1, 0.0, east_weight)
    west_weight = pltpu.roll(east_weight, 1, 1)
    north_weight = STIFFNESS * 0.5 * (deep + pltpu.roll(deep, rows - 1, 0)) * wet * pltpu.roll(wet, rows - 1, 0)
    north_weight = jnp.where(row == rows - 1, 0.0, north_weight)
    south_weight = pltpu.roll(north_weight, 1, 0)

    def spread(field):
        out = west_weight * (field - pltpu.roll(field, 1, 1))
        out = out + east_weight * (field - pltpu.roll(field, columns - 1, 1))
        out = out + south_weight * (field - pltpu.roll(field, 1, 0))
        return out + north_weight * (field - pltpu.roll(field, rows - 1, 0))

    field = wet * height[...]
    square = total(field * field)
    weight = jnp.sqrt(square)
    vector = field * jnp.where(square > 0.0, lax.rsqrt(jnp.maximum(square, 1e-30)), 0.0)
    before, link = jnp.zeros_like(vector), jnp.zeros_like(square)
    at = lane_index((1, LANES))
    out = jnp.where(at == WEIGHT_AT, weight, 0.0)
    for step in range(ITERS):
        image = spread(vector) - link * before
        along, size = total(image * vector), total(image * image)
        out = jnp.where(at == step, along, out)
        if step + 1 < ITERS:
            left = size - along * along
            alive = left > 1e-6 * size
            scale = jnp.where(alive, lax.rsqrt(jnp.maximum(left, 1e-30)), 0.0)
            link = jnp.where(alive, jnp.sqrt(jnp.maximum(left, 0.0)), 0.0)
            before, vector = vector, (image - along * vector) * scale
            out = jnp.where(at == OFF_AT + step, link, out)
    row_out[...] = jnp.broadcast_to(out[None], row_out.shape)


def merged_recurrence(tiles):
    at = lane_index(tiles.shape)
    diagonal = jnp.where(at < ITERS, tiles, 0.0)
    above = jnp.where(at < ITERS - 1, pltpu.roll(tiles, LANES - OFF_AT, 1), 0.0)
    below = pltpu.roll(above, 1, 1)
    vector = jnp.where(at == 0, pltpu.roll(tiles, LANES - WEIGHT_AT, 1), 0.0)
    square = total(vector * vector)
    vector = vector * jnp.where(square > 0.0, lax.rsqrt(jnp.maximum(square, 1e-30)), 0.0)
    before, link = jnp.zeros_like(vector), jnp.zeros_like(square)
    running = jnp.ones_like(square)
    steps = []
    for _ in range(ITERS):
        image = diagonal * vector - link * before
        image = image + above * pltpu.roll(vector, LANES - 1, 1) + below * pltpu.roll(vector, 1, 1)
        along, size = total(image * vector), total(image * image)
        left = size - along * along
        alive = left > 1e-6 * size
        middle = jnp.where(running > 0.0, along, 4.0 * STIFFNESS)
        back = link
        scale = jnp.where(alive, lax.rsqrt(jnp.maximum(left, 1e-30)), 0.0)
        link = jnp.where(alive, jnp.sqrt(jnp.maximum(left, 0.0)), 0.0)
        steps.append((middle, jnp.where(alive, link, 2.0 * STIFFNESS), back))
        running = jnp.where(alive, running, 0.0)
        before, vector = vector, (image - along * vector) * scale
    return steps


def krylov_kernel(
    height, mask, depth, from_south, from_north, from_west, from_east, tiles, basis, products
):
    rows, columns = height.shape
    full_rows, full_columns = rows + 2 * RING, columns + LANES
    wet = mask[0].astype(jnp.float32)
    own = (wet * height[...], wet, depth[...])

    def widened(at):
        span = slice(at * RING, (at + 1) * RING)
        tile = jnp.concatenate([own[at], from_north[span, :], from_south[span, :]], axis=0)
        side = beside_tile(from_west, from_east, at * RING, RING)
        return jnp.concatenate([tile, side[:full_rows]], axis=1)

    field, opening, deep = widened(0), widened(1), widened(2)
    basis[ITERS] = opening
    basis[ITERS + 1] = deep
    west_weight = STIFFNESS * 0.5 * (deep + pltpu.roll(deep, 1, 1)) * opening * pltpu.roll(opening, 1, 1)
    east_weight = pltpu.roll(west_weight, full_columns - 1, 1)
    south_weight = STIFFNESS * 0.5 * (deep + pltpu.roll(deep, 1, 0)) * opening * pltpu.roll(opening, 1, 0)
    north_weight = pltpu.roll(south_weight, full_rows - 1, 0)

    def spread(value):
        out = west_weight * (value - pltpu.roll(value, 1, 1))
        out = out + east_weight * (value - pltpu.roll(value, full_columns - 1, 1))
        out = out + south_weight * (value - pltpu.roll(value, 1, 0))
        return out + north_weight * (value - pltpu.roll(value, full_rows - 1, 0))

    steps = merged_recurrence(tiles[...])
    at = lane_index((1, LANES))
    row = jnp.zeros((1, LANES), jnp.float32)
    for step, entries in enumerate(steps):
        for kind, entry in enumerate(entries):
            row = jnp.where(at == kind * OFF_AT + step, entry, row)
    basis[ITERS + 2, :1, :LANES] = row
    vectors = [field]
    before, value = None, field
    basis[0] = field
    for step, (middle, link, back) in enumerate(steps):
        image = spread(value) - middle * value
        if step:
            image = image - back * before
        before, value = value, image * (1.0 / link)
        if step + 1 < ITERS:
            basis[step + 1] = value
        vectors.append(value)
    cut = [vector[:rows, :columns] for vector in vectors]
    partial = [jnp.sum(cut[i] * cut[j], axis=0, keepdims=True) for i, j in PAIRS]
    partial = [sum(part[:, k : k + LANES] for k in range(0, columns, LANES)) for part in partial]
    partial = partial + [jnp.zeros((LANES - len(partial), LANES), jnp.float32)]
    table = jnp.transpose(jnp.concatenate(partial, axis=0))
    products[...] = jnp.broadcast_to(jnp.sum(table, axis=0, keepdims=True)[None], products.shape)


def solve_kernel(gathered, basis, surface, pressure):
    rows, columns = surface.shape
    summed = jnp.sum(gathered[...], axis=0, keepdims=True)
    known = basis[ITERS + 2, :1, :LANES]
    at = lane_index((1, LANES))

    def entry(row, index):
        return jnp.sum(jnp.where(at == index, row, 0.0), axis=1, keepdims=True)

    gram = {}
    for index, (i, j) in enumerate(PAIRS):
        gram[i, j] = gram[j, i] = entry(summed, index)
    middle = [entry(known, step) for step in range(ITERS)]
    link = [entry(known, OFF_AT + step) for step in range(ITERS)]
    back = [entry(known, 2 * OFF_AT + step) for step in range(ITERS)]
    zero = jnp.zeros((1, 1), jnp.float32)

    def applied(vector):
        out = [zero] * (len(vector) + 1)
        for i, part in enumerate(vector):
            out[i] = out[i] + part + middle[i] * part
            out[i + 1] = out[i + 1] + link[i] * part
            if i:
                out[i - 1] = out[i - 1] + back[i] * part
        return out

    def inner(left, right):
        out = zero
        for i, a in enumerate(left):
            part = zero
            for j, b in enumerate(right):
                part = part + gram[i, j] * b
            out = out + a * part
        return out

    def scaled_add(left, scale, right):
        size = max(len(left), len(right))
        left = left + [zero] * (size - len(left))
        right = right + [zero] * (size - len(right))
        return [a + scale * b for a, b in zip(left, right)]

    residual = direction = [jnp.ones((1, 1), jnp.float32)]
    iterate = [zero]
    norm_now = gram[0, 0]
    for iteration in range(ITERS):
        image = applied(direction)
        product = inner(direction, image)
        step_size = jnp.where(product > 0.0, norm_now / product, 0.0)
        iterate = scaled_add(iterate, step_size, direction)
        if iteration + 1 < ITERS:
            residual = scaled_add(residual, -step_size, image)
            norm_next = inner(residual, residual)
            growth = jnp.where(norm_now > 0.0, norm_next / norm_now, 0.0)
            direction = scaled_add(residual, growth, direction)
            norm_now = norm_next
    value = iterate[0] * basis[0]
    for k in range(1, ITERS):
        value = value + iterate[k] * basis[k]
    surface[...] = value[:rows, :columns]
    opening = basis[ITERS]
    load = basis[ITERS + 1] * value
    full_rows, full_columns = value.shape
    pull = jnp.zeros_like(load)
    for shift, axis in ((1, 1), (full_columns - 1, 1), (1, 0), (full_rows - 1, 0)):
        pull = pull + opening * pltpu.roll(opening, shift, axis) * (pltpu.roll(load, shift, axis) - load)
    pressure[...] = -GRAVITY * pull[:rows, :columns]


def tracer_kernel(
    levels, temp, east, north, mask, from_south, from_north, from_west, from_east, tracer
):
    rows, columns = temp.shape[1:]
    row = lax.broadcasted_iota(jnp.int32, (rows, columns), 0)
    lane = lane_index((rows, columns))
    base = 3 * RING
    tracer_sides = beside_tile(from_west, from_east, base, levels)[:rows]
    for level in range(levels):
        masked = mask[level].astype(jnp.float32) * temp[level]
        east_coef = DIFFUSE - 0.5 * east[level]
        west_coef = DIFFUSE + 0.5 * east[level]
        north_coef = DIFFUSE - 0.5 * north[level]
        south_coef = DIFFUSE + 0.5 * north[level]
        side_west = tracer_sides[:, LANES - levels + level : LANES - levels + level + 1]
        side_east = tracer_sides[:, level : level + 1]
        side_south = from_south[base + level : base + level + 1, :]
        side_north = from_north[base + level : base + level + 1, :]
        inflow = jnp.where(lane == 0, side_west, pltpu.roll(east_coef * masked, 1, 1))
        inflow = inflow + jnp.where(
            lane == columns - 1, side_east, pltpu.roll(west_coef * masked, columns - 1, 1)
        )
        inflow = inflow + jnp.where(row == 0, side_south, pltpu.roll(north_coef * masked, 1, 0))
        inflow = inflow + jnp.where(
            row == rows - 1, side_north, pltpu.roll(south_coef * masked, rows - 1, 0)
        )
        tracer[level] = masked + TIMESTEP * (
            inflow - (east_coef + west_coef + north_coef + south_coef) * masked
        )


def level_of_slot(slots, slot, levels):
    level = jnp.int32(0)
    for k in range(1, levels):
        level = jnp.where(slots[k] == slot, jnp.int32(k), level)
    return level


def density(level, levels, pressure, mask):
    thickness = 1.0 + level.astype(jnp.float32) / levels
    return thickness * pressure[...] * mask[level].astype(jnp.float32)


def warm_kernel(levels, sizes, slots, tracer, pressure, mask, *refs):
    parts, (partial, salt) = refs[: len(sizes)], refs[len(sizes) :]
    slot = 0
    for size, part in zip(sizes, parts):
        for at in range(size):
            level = level_of_slot(slots, slot, levels)
            dense = density(level, levels, pressure, mask)
            warm = part[at]
            salt[level] = (HALINE + CABBELING * warm) * dense
            partial[level] = tracer[level] + (THERMAL + 2.0 * NONLINEAR * warm) * dense
            slot += 1


def salt_kernel(levels, first, slots, partial, pressure, mask, part, *refs):
    result, done, sems = refs[-3:]
    size = part.shape[0]
    copies = []
    for at in range(size):
        level = level_of_slot(slots, first + at, levels)
        dense = density(level, levels, pressure, mask)
        done[at] = partial[level] + CABBELING * part[at] * dense
        copies.append(pltpu.make_async_copy(done.at[at], result.at[level], sems.at[at]))
        copies[-1].start()
    for copy in copies:
        copy.wait()


def finish(levels, first, args, before):
    part = args[-1]
    shape = (levels,) + part.shape[1:]
    held_args = [pltpu.with_memory_space_constraint(arg, pltpu.VMEM) for arg in args[1:]]
    operands = [args[0]] + held_args + ([] if before is None else [before])
    return pl.pallas_call(
        functools.partial(salt_kernel, levels, first),
        out_shape=jax.ShapeDtypeStruct(shape, jnp.float32),
        in_specs=[SMEM] + [VMEM] * len(held_args) + ([] if before is None else [HBM]),
        out_specs=HBM,
        scratch_shapes=[
            pltpu.VMEM(part.shape, jnp.float32),
            pltpu.SemaphoreType.DMA((part.shape[0],)),
        ],
        input_output_aliases={} if before is None else {len(operands) - 1: 0},
        compiler_params=pltpu.CompilerParams(vmem_limit_bytes=KERNEL_VMEM),
        cost_estimate=pl.CostEstimate(flops=1000000, bytes_accessed=1000000, transcendentals=0),
    )(*operands)


def shifted(value, axis, steps, around):
    count = lax.axis_size(axis)
    pairs = [(i, (i + steps) % count) for i in range(count) if around or 0 <= i + steps < count]
    return lax.ppermute(value, axis, pairs)


def shared(rows):
    rows = lax.all_to_all(rows, ("gx", "gy"), 0, 0)
    return rows.reshape(rows.shape[0], LANES)


def runs(levels):
    return (levels,), (levels // 2, levels - levels // 2)


def body(
    temp_adjoint,
    height_adjoint,
    east_velocity,
    north_velocity,
    temp_store,
    salt_store,
    slot_map,
    land_mask,
    ocean_depth,
):
    levels, rows, columns = temp_adjoint.shape
    half_cycle = lax.axis_size("gx") // 2
    devices = lax.axis_size("gx") * lax.axis_size("gy")
    strip = 3 * RING + levels
    full = (rows + 2 * RING, columns + LANES)
    surface_args = stored(height_adjoint, land_mask, ocean_depth)
    top = pl.BlockSpec((1, rows, columns), lambda _: (0, 0, 0))

    def fetched(store, sizes):
        parts, start = [], 0
        for size in sizes:
            part = store if size == levels else lax.slice_in_dim(store, start, start + size)
            parts.append(shifted(part, "gx", half_cycle, True))
            start += size
        return parts

    warm_sizes, salt_sizes = runs(levels)
    slots = shifted(slot_map, "gx", half_cycle, True).reshape(-1)
    warm_parts = fetched(temp_store, warm_sizes)
    salt_parts = fetched(salt_store, salt_sizes)

    to_north, to_south = call(
        functools.partial(pack_y_kernel, levels),
        [(strip, columns)] * 2,
        surface_args + stored(temp_adjoint, north_velocity),
    )
    from_south = shifted(to_north, "gy", 1, False)
    from_north = shifted(to_south, "gy", -1, False)
    (tile_rows,) = call(tile_basis_kernel, [(devices, 1, LANES)], surface_args, specs=[VMEM, top, VMEM], grid=(1,))
    to_east, to_west = call(
        functools.partial(pack_x_kernel, levels),
        [(strip, rows + LANES)] * 2,
        surface_args + stored(temp_adjoint, east_velocity) + held(from_south, from_north),
    )
    from_west = shifted(to_east, "gx", 1, True)
    from_east = shifted(to_west, "gx", -1, True)
    tiles = shared(tile_rows)
    beside = held(from_south, from_north, from_west, from_east)
    basis, products = call(
        krylov_kernel,
        [(ITERS + 3,) + full, (devices, 1, LANES)],
        surface_args + beside + held(tiles),
        specs=[VMEM, top] + [VMEM] * 6,
        grid=(1,),
    )
    gathered = shared(products)
    (tracer,) = call(
        functools.partial(tracer_kernel, levels),
        [temp_adjoint.shape],
        stored(temp_adjoint, east_velocity, north_velocity, land_mask) + beside,
    )
    surface, pressure = call(solve_kernel, [(rows, columns)] * 2, held(gathered, basis), keep=[False, True])
    partial, salt_back = call(
        functools.partial(warm_kernel, levels, warm_sizes),
        [temp_adjoint.shape] * 2,
        free(slots) + held(tracer, pressure) + free(land_mask, *warm_parts),
        specs=[SMEM] + [VMEM] * (3 + len(warm_sizes)),
        keep=[True, False],
    )
    temp_back, first = None, 0
    for size, part in zip(salt_sizes, salt_parts):
        args = (slots, partial, pressure, land_mask, part)
        temp_back = finish(levels, first, args, temp_back)
        first += size
    return (temp_back, salt_back, surface)


def solution(mesh):
    return jax.shard_map(
        body,
        mesh=mesh,
        in_specs=(
            P(None, "gy", "gx"),
            P("gy", "gx"),
            P(None, "gy", "gx"),
            P(None, "gy", "gx"),
            P(None, "gy", "gx"),
            P(None, "gy", "gx"),
            P("gx", "gy", None),
            P(None, "gy", "gx"),
            P("gy", "gx"),
        ),
        out_specs=(P(None, "gy", "gx"), P(None, "gy", "gx"), P("gy", "gx")),
        check_vma=False,
    )
```

```python
import functools

import jax
import jax.numpy as jnp
from jax import lax
from jax.experimental import pallas as pl
from jax.experimental.pallas import tpu as pltpu
from jax.sharding import PartitionSpec as P


ITERS = 6
RING = 8
KERNEL_VMEM = 16 * 1024 * 1024
LANES = 128

DIFFUSE = 0.2
TIMESTEP = 1.0
STIFFNESS = 8.0
GRAVITY = 4.0
THERMAL = 0.5
NONLINEAR = 0.4
CABBELING = 0.3
HALINE = 0.8


VMEM = pl.BlockSpec(memory_space=pltpu.VMEM)
SMEM = pl.BlockSpec(memory_space=pltpu.SMEM)
HBM = pl.BlockSpec(memory_space=pltpu.HBM)

OFF_AT, WEIGHT_AT = 16, 32
PAIRS = [(i, j) for i in range(ITERS + 1) for j in range(i, ITERS + 1)]


def call(kernel, outs, args, specs=None, keep=None, flops=4000000):
    specs = specs or [VMEM] * len(args)
    keep = keep or [True] * len(outs)
    args = [
        arg if space is None else pltpu.with_memory_space_constraint(arg, space) for arg, space in args
    ]
    shapes = [
        pltpu.VMEM(shape, jnp.float32) if kept else jax.ShapeDtypeStruct(shape, jnp.float32)
        for shape, kept in zip(outs, keep)
    ]
    return pl.pallas_call(
        kernel,
        out_shape=shapes,
        in_specs=specs,
        out_specs=[VMEM] * len(outs),
        compiler_params=pltpu.CompilerParams(vmem_limit_bytes=KERNEL_VMEM),
        cost_estimate=pl.CostEstimate(flops=flops, bytes_accessed=1000000, transcendentals=0),
    )(*args)


def held(*arrays):
    return tuple((array, pltpu.VMEM) for array in arrays)


def stored(*arrays):
    return tuple((array, pltpu.HBM) for array in arrays)


def free(*arrays):
    return tuple((array, None) for array in arrays)


def total(value):
    return jnp.sum(jnp.sum(value, axis=0, keepdims=True), axis=1, keepdims=True)


def lane_index(shape):
    return lax.broadcasted_iota(jnp.int32, shape, 1)


def pack_y_kernel(levels, height, mask, depth, temp, north, fields, *messages):
    wet = mask[0].astype(jnp.float32)
    fields[0] = wet * height[...]
    fields[1] = wet
    fields[2] = depth[...]
    first, last = slice(0, RING), slice(temp.shape[1] - RING, temp.shape[1])

    def send(span, to_north, to_south):
        if len(messages) == 1:
            messages[0][span, :] = jnp.where(lax.axis_index("gy") == 0, to_north, to_south)
        else:
            messages[0][span, :] = to_north
            messages[1][span, :] = to_south

    for at in range(3):
        field = fields[at]
        send(slice(at * RING, (at + 1) * RING), field[last], field[first])
    base = 3 * RING
    for level in range(levels):
        flux_south = (DIFFUSE + 0.5 * north[level, first]) * (
            mask[level, first].astype(jnp.float32) * temp[level, first]
        )
        flux_north = (DIFFUSE - 0.5 * north[level, last]) * (
            mask[level, last].astype(jnp.float32) * temp[level, last]
        )
        send(slice(base + level, base + level + 1), flux_north[-1:], flux_south[:1])


def pack_x_kernel(levels, received, fields, mask, temp, east, *refs):
    arrived, (from_south, from_north, to_east, to_west) = refs[:received], refs[received:]
    if received == 1:
        lower = lax.axis_index("gy") == 0
        from_south[...] = jnp.where(lower, 0.0, arrived[0][...])
        from_north[...] = jnp.where(lower, arrived[0][...], 0.0)
    else:
        from_south[...] = arrived[0][...]
        from_north[...] = arrived[1][...]
    rows = fields.shape[1]
    for at in range(3):
        span = slice(at * RING, (at + 1) * RING)
        beside = [from_north[span, :], from_south[span, :]]
        beside.append(jnp.zeros((LANES - 2 * RING, fields.shape[2]), jnp.float32))
        flipped = jnp.transpose(jnp.concatenate([fields[at]] + beside, axis=0))
        to_west[span, :] = flipped[:RING]
        to_east[span, :] = flipped[-RING:]
    base = 3 * RING
    for level in range(levels):
        at = slice(base + level, base + level + 1)
        masked = mask[level].astype(jnp.float32) * temp[level]
        flux_east = (DIFFUSE - 0.5 * east[level]) * masked
        flux_west = (DIFFUSE + 0.5 * east[level]) * masked
        to_east[at, :rows] = jnp.transpose(flux_east[:, -LANES:])[-1:]
        to_west[at, :rows] = jnp.transpose(flux_west[:, :LANES])[:1]
    spare = slice(base, base + levels)
    to_east[spare, rows:] = jnp.zeros((levels, LANES), jnp.float32)
    to_west[spare, rows:] = jnp.zeros((levels, LANES), jnp.float32)


def beside_tile(from_west, from_east, start, size):
    span = slice(start, start + size)
    middle = jnp.zeros((LANES - 2 * size, from_west.shape[1]), jnp.float32)
    return jnp.transpose(jnp.concatenate([from_east[span, :], middle, from_west[span, :]], axis=0))


def tile_basis_kernel(fields, row_out):
    rows, columns = fields.shape[1:]
    wet, deep = fields[1], fields[2]
    row = lax.broadcasted_iota(jnp.int32, (rows, columns), 0)
    lane = lane_index((rows, columns))
    east_weight = (
        STIFFNESS * 0.5 * (deep + pltpu.roll(deep, columns - 1, 1)) * wet * pltpu.roll(wet, columns - 1, 1)
    )
    east_weight = jnp.where(lane == columns - 1, 0.0, east_weight)
    west_weight = pltpu.roll(east_weight, 1, 1)
    north_weight = STIFFNESS * 0.5 * (deep + pltpu.roll(deep, rows - 1, 0)) * wet * pltpu.roll(wet, rows - 1, 0)
    north_weight = jnp.where(row == rows - 1, 0.0, north_weight)
    south_weight = pltpu.roll(north_weight, 1, 0)

    def spread(field):
        out = west_weight * (field - pltpu.roll(field, 1, 1))
        out = out + east_weight * (field - pltpu.roll(field, columns - 1, 1))
        out = out + south_weight * (field - pltpu.roll(field, 1, 0))
        return out + north_weight * (field - pltpu.roll(field, rows - 1, 0))

    field = fields[0]
    square = total(field * field)
    weight = jnp.sqrt(square)
    vector = field * jnp.where(square > 0.0, lax.rsqrt(jnp.maximum(square, 1e-30)), 0.0)
    before, link = jnp.zeros_like(vector), jnp.zeros_like(square)
    at = lane_index((1, LANES))
    out = jnp.where(at == WEIGHT_AT, weight, 0.0)
    for step in range(ITERS):
        image = spread(vector) - link * before
        along, size = total(image * vector), total(image * image)
        out = jnp.where(at == step, along, out)
        if step + 1 < ITERS:
            left = size - along * along
            alive = left > 1e-6 * size
            scale = jnp.where(alive, lax.rsqrt(jnp.maximum(left, 1e-30)), 0.0)
            link = jnp.where(alive, jnp.sqrt(jnp.maximum(left, 0.0)), 0.0)
            before, vector = vector, (image - along * vector) * scale
            out = jnp.where(at == OFF_AT + step, link, out)
    row_out[...] = jnp.broadcast_to(out[None], row_out.shape)


def merged_recurrence(tiles):
    at = lane_index(tiles.shape)
    diagonal = jnp.where(at < ITERS, tiles, 0.0)
    above = jnp.where(at < ITERS - 1, pltpu.roll(tiles, LANES - OFF_AT, 1), 0.0)
    below = pltpu.roll(above, 1, 1)
    vector = jnp.where(at == 0, pltpu.roll(tiles, LANES - WEIGHT_AT, 1), 0.0)
    square = total(vector * vector)
    vector = vector * jnp.where(square > 0.0, lax.rsqrt(jnp.maximum(square, 1e-30)), 0.0)
    before, link = jnp.zeros_like(vector), jnp.zeros_like(square)
    running = jnp.ones_like(square)
    steps = []
    for _ in range(ITERS):
        image = diagonal * vector - link * before
        image = image + above * pltpu.roll(vector, LANES - 1, 1) + below * pltpu.roll(vector, 1, 1)
        along, size = total(image * vector), total(image * image)
        left = size - along * along
        alive = left > 1e-6 * size
        middle = jnp.where(running > 0.0, along, 4.0 * STIFFNESS)
        back = link
        scale = jnp.where(alive, lax.rsqrt(jnp.maximum(left, 1e-30)), 0.0)
        link = jnp.where(alive, jnp.sqrt(jnp.maximum(left, 0.0)), 0.0)
        steps.append((middle, jnp.where(alive, link, 2.0 * STIFFNESS), back))
        running = jnp.where(alive, running, 0.0)
        before, vector = vector, (image - along * vector) * scale
    return steps


def krylov_kernel(fields, from_south, from_north, from_west, from_east, tiles, basis, products):
    rows, columns = fields.shape[1:]
    full_rows, full_columns = rows + 2 * RING, columns + LANES

    def widened(at):
        span = slice(at * RING, (at + 1) * RING)
        tile = jnp.concatenate([fields[at], from_north[span, :], from_south[span, :]], axis=0)
        side = beside_tile(from_west, from_east, at * RING, RING)
        return jnp.concatenate([tile, side[:full_rows]], axis=1)

    field, opening, deep = widened(0), widened(1), widened(2)
    basis[ITERS] = opening
    basis[ITERS + 1] = deep
    west_weight = STIFFNESS * 0.5 * (deep + pltpu.roll(deep, 1, 1)) * opening * pltpu.roll(opening, 1, 1)
    east_weight = pltpu.roll(west_weight, full_columns - 1, 1)
    south_weight = STIFFNESS * 0.5 * (deep + pltpu.roll(deep, 1, 0)) * opening * pltpu.roll(opening, 1, 0)
    north_weight = pltpu.roll(south_weight, full_rows - 1, 0)

    def spread(value):
        out = west_weight * (value - pltpu.roll(value, 1, 1))
        out = out + east_weight * (value - pltpu.roll(value, full_columns - 1, 1))
        out = out + south_weight * (value - pltpu.roll(value, 1, 0))
        return out + north_weight * (value - pltpu.roll(value, full_rows - 1, 0))

    steps = merged_recurrence(tiles[...])
    at = lane_index((1, LANES))
    row = jnp.zeros((1, LANES), jnp.float32)
    for step, entries in enumerate(steps):
        for kind, entry in enumerate(entries):
            row = jnp.where(at == kind * OFF_AT + step, entry, row)
    basis[ITERS + 2, :1, :LANES] = row
    vectors = [field]
    before, value = None, field
    basis[0] = field
    for step, (middle, link, back) in enumerate(steps):
        image = spread(value) - middle * value
        if step:
            image = image - back * before
        before, value = value, image * (1.0 / link)
        if step + 1 < ITERS:
            basis[step + 1] = value
        vectors.append(value)
    cut = [vector[:rows, :columns] for vector in vectors]
    partial = [jnp.sum(cut[i] * cut[j], axis=0, keepdims=True) for i, j in PAIRS]
    partial = [sum(part[:, k : k + LANES] for k in range(0, columns, LANES)) for part in partial]
    partial = partial + [jnp.zeros((LANES - len(partial), LANES), jnp.float32)]
    table = jnp.transpose(jnp.concatenate(partial, axis=0))
    products[...] = jnp.broadcast_to(jnp.sum(table, axis=0, keepdims=True)[None], products.shape)


def solve_kernel(gathered, basis, surface, pressure):
    rows, columns = surface.shape
    summed = jnp.sum(gathered[...], axis=0, keepdims=True)
    known = basis[ITERS + 2, :1, :LANES]
    at = lane_index((1, LANES))

    def entry(row, index):
        return jnp.sum(jnp.where(at == index, row, 0.0), axis=1, keepdims=True)

    gram = {}
    for index, (i, j) in enumerate(PAIRS):
        gram[i, j] = gram[j, i] = entry(summed, index)
    middle = [entry(known, step) for step in range(ITERS)]
    link = [entry(known, OFF_AT + step) for step in range(ITERS)]
    back = [entry(known, 2 * OFF_AT + step) for step in range(ITERS)]
    zero = jnp.zeros((1, 1), jnp.float32)

    def applied(vector):
        out = [zero] * (len(vector) + 1)
        for i, part in enumerate(vector):
            out[i] = out[i] + part + middle[i] * part
            out[i + 1] = out[i + 1] + link[i] * part
            if i:
                out[i - 1] = out[i - 1] + back[i] * part
        return out

    def inner(left, right):
        out = zero
        for i, a in enumerate(left):
            part = zero
            for j, b in enumerate(right):
                part = part + gram[i, j] * b
            out = out + a * part
        return out

    def scaled_add(left, scale, right):
        size = max(len(left), len(right))
        left = left + [zero] * (size - len(left))
        right = right + [zero] * (size - len(right))
        return [a + scale * b for a, b in zip(left, right)]

    residual = direction = [jnp.ones((1, 1), jnp.float32)]
    iterate = [zero]
    norm_now = gram[0, 0]
    for iteration in range(ITERS):
        image = applied(direction)
        product = inner(direction, image)
        step_size = jnp.where(product > 0.0, norm_now / product, 0.0)
        iterate = scaled_add(iterate, step_size, direction)
        if iteration + 1 < ITERS:
            residual = scaled_add(residual, -step_size, image)
            norm_next = inner(residual, residual)
            growth = jnp.where(norm_now > 0.0, norm_next / norm_now, 0.0)
            direction = scaled_add(residual, growth, direction)
            norm_now = norm_next
    value = iterate[0] * basis[0]
    for k in range(1, ITERS):
        value = value + iterate[k] * basis[k]
    surface[...] = value[:rows, :columns]
    opening = basis[ITERS]
    load = basis[ITERS + 1] * value
    full_rows, full_columns = value.shape
    pull = jnp.zeros_like(load)
    for shift, axis in ((1, 1), (full_columns - 1, 1), (1, 0), (full_rows - 1, 0)):
        pull = pull + opening * pltpu.roll(opening, shift, axis) * (pltpu.roll(load, shift, axis) - load)
    pressure[...] = -GRAVITY * pull[:rows, :columns]


def tracer_kernel(
    levels, temp, east, north, mask, from_south, from_north, from_west, from_east, tracer
):
    rows, columns = temp.shape[1:]
    row = lax.broadcasted_iota(jnp.int32, (rows, columns), 0)
    lane = lane_index((rows, columns))
    base = 3 * RING
    tracer_sides = beside_tile(from_west, from_east, base, levels)[:rows]
    for level in range(levels):
        masked = mask[level].astype(jnp.float32) * temp[level]
        east_coef = DIFFUSE - 0.5 * east[level]
        west_coef = DIFFUSE + 0.5 * east[level]
        north_coef = DIFFUSE - 0.5 * north[level]
        south_coef = DIFFUSE + 0.5 * north[level]
        side_west = tracer_sides[:, LANES - levels + level : LANES - levels + level + 1]
        side_east = tracer_sides[:, level : level + 1]
        side_south = from_south[base + level : base + level + 1, :]
        side_north = from_north[base + level : base + level + 1, :]
        inflow = jnp.where(lane == 0, side_west, pltpu.roll(east_coef * masked, 1, 1))
        inflow = inflow + jnp.where(
            lane == columns - 1, side_east, pltpu.roll(west_coef * masked, columns - 1, 1)
        )
        inflow = inflow + jnp.where(row == 0, side_south, pltpu.roll(north_coef * masked, 1, 0))
        inflow = inflow + jnp.where(
            row == rows - 1, side_north, pltpu.roll(south_coef * masked, rows - 1, 0)
        )
        tracer[level] = masked + TIMESTEP * (
            inflow - (east_coef + west_coef + north_coef + south_coef) * masked
        )


def level_of_slot(slots, slot, levels):
    level = jnp.int32(0)
    for k in range(1, levels):
        level = jnp.where(slots[k] == slot, jnp.int32(k), level)
    return level


def density(level, levels, pressure, mask):
    thickness = 1.0 + level.astype(jnp.float32) / levels
    return thickness * pressure[...] * mask[level].astype(jnp.float32)


def warm_kernel(levels, sizes, slots, tracer, pressure, mask, *refs):
    parts, (partial, salt) = refs[: len(sizes)], refs[len(sizes) :]
    slot = 0
    for size, part in zip(sizes, parts):
        for at in range(size):
            level = level_of_slot(slots, slot, levels)
            dense = density(level, levels, pressure, mask)
            warm = part[at]
            salt[level] = (HALINE + CABBELING * warm) * dense
            partial[level] = tracer[level] + (THERMAL + 2.0 * NONLINEAR * warm) * dense
            slot += 1


def salt_kernel(levels, first, slots, partial, pressure, mask, part, *refs):
    result, done, sems = refs[-3:]
    size = part.shape[0]
    copies = []
    for at in range(size):
        level = level_of_slot(slots, first + at, levels)
        dense = density(level, levels, pressure, mask)
        done[at] = partial[level] + CABBELING * part[at] * dense
        copies.append(pltpu.make_async_copy(done.at[at], result.at[level], sems.at[at]))
        copies[-1].start()
    for copy in copies:
        copy.wait()


def finish(levels, first, args, before):
    part = args[-1]
    shape = (levels,) + part.shape[1:]
    held_args = [pltpu.with_memory_space_constraint(arg, pltpu.VMEM) for arg in args[1:]]
    operands = [args[0]] + held_args + ([] if before is None else [before])
    return pl.pallas_call(
        functools.partial(salt_kernel, levels, first),
        out_shape=jax.ShapeDtypeStruct(shape, jnp.float32),
        in_specs=[SMEM] + [VMEM] * len(held_args) + ([] if before is None else [HBM]),
        out_specs=HBM,
        scratch_shapes=[
            pltpu.VMEM(part.shape, jnp.float32),
            pltpu.SemaphoreType.DMA((part.shape[0],)),
        ],
        input_output_aliases={} if before is None else {len(operands) - 1: 0},
        compiler_params=pltpu.CompilerParams(vmem_limit_bytes=KERNEL_VMEM),
        cost_estimate=pl.CostEstimate(flops=1000000, bytes_accessed=1000000, transcendentals=0),
    )(*operands)


def shifted(value, axis, steps, around):
    count = lax.axis_size(axis)
    pairs = [(i, (i + steps) % count) for i in range(count) if around or 0 <= i + steps < count]
    return lax.ppermute(value, axis, pairs)


def shared(rows):
    rows = lax.all_to_all(rows, ("gx", "gy"), 0, 0)
    return rows.reshape(rows.shape[0], LANES)


def runs(levels):
    most = 5 * levels // 8
    return (levels,), (most, levels - most)


def body(
    temp_adjoint,
    height_adjoint,
    east_velocity,
    north_velocity,
    temp_store,
    salt_store,
    slot_map,
    land_mask,
    ocean_depth,
):
    levels, rows, columns = temp_adjoint.shape
    half_cycle = lax.axis_size("gx") // 2
    devices = lax.axis_size("gx") * lax.axis_size("gy")
    strip = 3 * RING + levels
    full = (rows + 2 * RING, columns + LANES)

    warm_sizes, salt_sizes = runs(levels)
    slots = shifted(slot_map, "gx", half_cycle, True).reshape(-1)
    warm_parts = [shifted(temp_store, "gx", half_cycle, True)]

    swap = lax.axis_size("gy") == 2
    fields, *messages = call(
        functools.partial(pack_y_kernel, levels),
        [(3, rows, columns)] + [(strip, columns)] * (1 if swap else 2),
        stored(height_adjoint, land_mask, ocean_depth, temp_adjoint, north_velocity),
    )
    if swap:
        arrived = [shifted(messages[0], "gy", 1, True)]
    else:
        arrived = [shifted(messages[0], "gy", 1, False)]
        arrived += [shifted(messages[1], "gy", -1, False)]
    (tile_rows,) = call(tile_basis_kernel, [(devices, 1, LANES)], held(fields))
    from_south, from_north, to_east, to_west = call(
        functools.partial(pack_x_kernel, levels, len(arrived)),
        [(strip, columns)] * 2 + [(strip, rows + LANES)] * 2,
        held(fields) + stored(land_mask, temp_adjoint, east_velocity) + held(*arrived),
    )
    from_west = shifted(to_east, "gx", 1, True)
    from_east = shifted(to_west, "gx", -1, True)
    cuts, start = [], 0
    for size in salt_sizes:
        cuts.append(lax.slice_in_dim(salt_store, start, start + size))
        start += size
    *cuts, tile_rows = lax.optimization_barrier((*cuts, tile_rows))
    tiles = shared(tile_rows)
    salt_parts = [shifted(cut, "gx", half_cycle, True) for cut in cuts]
    beside = held(from_south, from_north, from_west, from_east)
    basis, products = call(
        krylov_kernel, [(ITERS + 3,) + full, (devices, 1, LANES)], held(fields) + beside + held(tiles)
    )
    gathered = shared(products)
    (tracer,) = call(
        functools.partial(tracer_kernel, levels),
        [temp_adjoint.shape],
        stored(temp_adjoint, east_velocity, north_velocity, land_mask) + beside,
    )
    surface, pressure = call(solve_kernel, [(rows, columns)] * 2, held(gathered, basis), keep=[False, True])
    partial, salt_back = call(
        functools.partial(warm_kernel, levels, warm_sizes),
        [temp_adjoint.shape] * 2,
        free(slots) + held(tracer, pressure) + free(land_mask, *warm_parts),
        specs=[SMEM] + [VMEM] * (3 + len(warm_sizes)),
        keep=[True, False],
    )
    temp_back, first = None, 0
    for size, part in zip(salt_sizes, salt_parts):
        args = (slots, partial, pressure, land_mask, part)
        temp_back = finish(levels, first, args, temp_back)
        first += size
    return (temp_back, salt_back, surface)


def solution(mesh):
    return jax.shard_map(
        body,
        mesh=mesh,
        in_specs=(
            P(None, "gy", "gx"),
            P("gy", "gx"),
            P(None, "gy", "gx"),
            P(None, "gy", "gx"),
            P(None, "gy", "gx"),
            P(None, "gy", "gx"),
            P("gx", "gy", None),
            P(None, "gy", "gx"),
            P("gy", "gx"),
        ),
        out_specs=(P(None, "gy", "gx"), P(None, "gy", "gx"), P("gy", "gx")),
        check_vma=False,
    )
```

```python
import functools

import jax
import jax.numpy as jnp
from jax import lax
from jax.experimental import pallas as pl
from jax.experimental.pallas import tpu as pltpu
from jax.sharding import PartitionSpec as P


ITERS = 6
RING = 8
KERNEL_VMEM = 16 * 1024 * 1024
LANES = 128

DIFFUSE = 0.2
TIMESTEP = 1.0
STIFFNESS = 8.0
GRAVITY = 4.0
THERMAL = 0.5
NONLINEAR = 0.4
CABBELING = 0.3
HALINE = 0.8


VMEM = pl.BlockSpec(memory_space=pltpu.VMEM)
SMEM = pl.BlockSpec(memory_space=pltpu.SMEM)
HBM = pl.BlockSpec(memory_space=pltpu.HBM)

OFF_AT, WEIGHT_AT = 16, 32
PAIRS = [(i, j) for i in range(ITERS + 1) for j in range(i, ITERS + 1)]


def call(kernel, outs, args, specs=None, keep=None, flops=4000000):
    specs = specs or [VMEM] * len(args)
    keep = keep or [True] * len(outs)
    args = [
        arg if space is None else pltpu.with_memory_space_constraint(arg, space) for arg, space in args
    ]
    shapes = [
        pltpu.VMEM(shape, jnp.float32) if kept else jax.ShapeDtypeStruct(shape, jnp.float32)
        for shape, kept in zip(outs, keep)
    ]
    return pl.pallas_call(
        kernel,
        out_shape=shapes,
        in_specs=specs,
        out_specs=[VMEM] * len(outs),
        compiler_params=pltpu.CompilerParams(vmem_limit_bytes=KERNEL_VMEM),
        cost_estimate=pl.CostEstimate(flops=flops, bytes_accessed=1000000, transcendentals=0),
    )(*args)


def held(*arrays):
    return tuple((array, pltpu.VMEM) for array in arrays)


def stored(*arrays):
    return tuple((array, pltpu.HBM) for array in arrays)


def free(*arrays):
    return tuple((array, None) for array in arrays)


def total(value):
    return jnp.sum(jnp.sum(value, axis=0, keepdims=True), axis=1, keepdims=True)


def lane_index(shape):
    return lax.broadcasted_iota(jnp.int32, shape, 1)


def pack_y_kernel(levels, height, mask, depth, temp, north, fields, *messages):
    wet = mask[0].astype(jnp.float32)
    fields[0] = wet * height[...]
    fields[1] = wet
    fields[2] = depth[...]
    first, last = slice(0, RING), slice(temp.shape[1] - RING, temp.shape[1])

    def send(span, to_north, to_south):
        if len(messages) == 1:
            messages[0][span, :] = jnp.where(lax.axis_index("gy") == 0, to_north, to_south)
        else:
            messages[0][span, :] = to_north
            messages[1][span, :] = to_south

    for at in range(3):
        field = fields[at]
        send(slice(at * RING, (at + 1) * RING), field[last], field[first])
    base = 3 * RING
    for level in range(levels):
        flux_south = (DIFFUSE + 0.5 * north[level, first]) * (
            mask[level, first].astype(jnp.float32) * temp[level, first]
        )
        flux_north = (DIFFUSE - 0.5 * north[level, last]) * (
            mask[level, last].astype(jnp.float32) * temp[level, last]
        )
        send(slice(base + level, base + level + 1), flux_north[-1:], flux_south[:1])


def pack_x_kernel(levels, received, fields, mask, temp, east, *refs):
    arrived, (from_south, from_north, to_east, to_west) = refs[:received], refs[received:]
    if received == 1:
        lower = lax.axis_index("gy") == 0
        from_south[...] = jnp.where(lower, 0.0, arrived[0][...])
        from_north[...] = jnp.where(lower, arrived[0][...], 0.0)
    else:
        from_south[...] = arrived[0][...]
        from_north[...] = arrived[1][...]
    rows = fields.shape[1]
    for at in range(3):
        span = slice(at * RING, (at + 1) * RING)
        beside = [from_north[span, :], from_south[span, :]]
        beside.append(jnp.zeros((LANES - 2 * RING, fields.shape[2]), jnp.float32))
        flipped = jnp.transpose(jnp.concatenate([fields[at]] + beside, axis=0))
        to_west[span, :] = flipped[:RING]
        to_east[span, :] = flipped[-RING:]
    base = 3 * RING
    for level in range(levels):
        at = slice(base + level, base + level + 1)
        masked = mask[level].astype(jnp.float32) * temp[level]
        flux_east = (DIFFUSE - 0.5 * east[level]) * masked
        flux_west = (DIFFUSE + 0.5 * east[level]) * masked
        to_east[at, :rows] = jnp.transpose(flux_east[:, -LANES:])[-1:]
        to_west[at, :rows] = jnp.transpose(flux_west[:, :LANES])[:1]
    spare = slice(base, base + levels)
    to_east[spare, rows:] = jnp.zeros((levels, LANES), jnp.float32)
    to_west[spare, rows:] = jnp.zeros((levels, LANES), jnp.float32)


def beside_tile(from_west, from_east, start, size):
    span = slice(start, start + size)
    middle = jnp.zeros((LANES - 2 * size, from_west.shape[1]), jnp.float32)
    return jnp.transpose(jnp.concatenate([from_east[span, :], middle, from_west[span, :]], axis=0))


def tile_basis_kernel(fields, row_out):
    rows, columns = fields.shape[1:]
    wet, deep = fields[1], fields[2]
    row = lax.broadcasted_iota(jnp.int32, (rows, columns), 0)
    lane = lane_index((rows, columns))
    east_weight = (
        STIFFNESS * 0.5 * (deep + pltpu.roll(deep, columns - 1, 1)) * wet * pltpu.roll(wet, columns - 1, 1)
    )
    east_weight = jnp.where(lane == columns - 1, 0.0, east_weight)
    west_weight = pltpu.roll(east_weight, 1, 1)
    north_weight = STIFFNESS * 0.5 * (deep + pltpu.roll(deep, rows - 1, 0)) * wet * pltpu.roll(wet, rows - 1, 0)
    north_weight = jnp.where(row == rows - 1, 0.0, north_weight)
    south_weight = pltpu.roll(north_weight, 1, 0)

    def spread(field):
        out = west_weight * (field - pltpu.roll(field, 1, 1))
        out = out + east_weight * (field - pltpu.roll(field, columns - 1, 1))
        out = out + south_weight * (field - pltpu.roll(field, 1, 0))
        return out + north_weight * (field - pltpu.roll(field, rows - 1, 0))

    field = fields[0]
    square = total(field * field)
    weight = jnp.sqrt(square)
    vector = field * jnp.where(square > 0.0, lax.rsqrt(jnp.maximum(square, 1e-30)), 0.0)
    before, link = jnp.zeros_like(vector), jnp.zeros_like(square)
    at = lane_index((1, LANES))
    out = jnp.where(at == WEIGHT_AT, weight, 0.0)
    for step in range(ITERS):
        image = spread(vector) - link * before
        along, size = total(image * vector), total(image * image)
        out = jnp.where(at == step, along, out)
        if step + 1 < ITERS:
            left = size - along * along
            alive = left > 1e-6 * size
            scale = jnp.where(alive, lax.rsqrt(jnp.maximum(left, 1e-30)), 0.0)
            link = jnp.where(alive, jnp.sqrt(jnp.maximum(left, 0.0)), 0.0)
            before, vector = vector, (image - along * vector) * scale
            out = jnp.where(at == OFF_AT + step, link, out)
    row_out[...] = jnp.broadcast_to(out[None], row_out.shape)


def merged_recurrence(tiles):
    at = lane_index(tiles.shape)
    diagonal = jnp.where(at < ITERS, tiles, 0.0)
    above = jnp.where(at < ITERS - 1, pltpu.roll(tiles, LANES - OFF_AT, 1), 0.0)
    below = pltpu.roll(above, 1, 1)
    vector = jnp.where(at == 0, pltpu.roll(tiles, LANES - WEIGHT_AT, 1), 0.0)
    square = total(vector * vector)
    vector = vector * jnp.where(square > 0.0, lax.rsqrt(jnp.maximum(square, 1e-30)), 0.0)
    before, link = jnp.zeros_like(vector), jnp.zeros_like(square)
    running = jnp.ones_like(square)
    steps = []
    for _ in range(ITERS):
        image = diagonal * vector - link * before
        image = image + above * pltpu.roll(vector, LANES - 1, 1) + below * pltpu.roll(vector, 1, 1)
        along, size = total(image * vector), total(image * image)
        left = size - along * along
        alive = left > 1e-6 * size
        middle = jnp.where(running > 0.0, along, 4.0 * STIFFNESS)
        back = link
        scale = jnp.where(alive, lax.rsqrt(jnp.maximum(left, 1e-30)), 0.0)
        link = jnp.where(alive, jnp.sqrt(jnp.maximum(left, 0.0)), 0.0)
        steps.append((middle, jnp.where(alive, link, 2.0 * STIFFNESS), back))
        running = jnp.where(alive, running, 0.0)
        before, vector = vector, (image - along * vector) * scale
    return steps


def krylov_kernel(fields, from_south, from_north, from_west, from_east, tiles, basis, products):
    rows, columns = fields.shape[1:]
    full_rows, full_columns = rows + 2 * RING, columns + LANES

    def widened(at):
        span = slice(at * RING, (at + 1) * RING)
        tile = jnp.concatenate([fields[at], from_north[span, :], from_south[span, :]], axis=0)
        side = beside_tile(from_west, from_east, at * RING, RING)
        return jnp.concatenate([tile, side[:full_rows]], axis=1)

    field, opening, deep = widened(0), widened(1), widened(2)
    basis[ITERS] = opening
    basis[ITERS + 1] = deep
    west_weight = STIFFNESS * 0.5 * (deep + pltpu.roll(deep, 1, 1)) * opening * pltpu.roll(opening, 1, 1)
    east_weight = pltpu.roll(west_weight, full_columns - 1, 1)
    south_weight = STIFFNESS * 0.5 * (deep + pltpu.roll(deep, 1, 0)) * opening * pltpu.roll(opening, 1, 0)
    north_weight = pltpu.roll(south_weight, full_rows - 1, 0)

    def spread(value):
        out = west_weight * (value - pltpu.roll(value, 1, 1))
        out = out + east_weight * (value - pltpu.roll(value, full_columns - 1, 1))
        out = out + south_weight * (value - pltpu.roll(value, 1, 0))
        return out + north_weight * (value - pltpu.roll(value, full_rows - 1, 0))

    steps = merged_recurrence(tiles[...])
    at = lane_index((1, LANES))
    row = jnp.zeros((1, LANES), jnp.float32)
    for step, entries in enumerate(steps):
        for kind, entry in enumerate(entries):
            row = jnp.where(at == kind * OFF_AT + step, entry, row)
    basis[ITERS + 2, :1, :LANES] = row
    vectors = [field]
    before, value = None, field
    basis[0] = field
    for step, (middle, link, back) in enumerate(steps):
        image = spread(value) - middle * value
        if step:
            image = image - back * before
        before, value = value, image * (1.0 / link)
        if step + 1 < ITERS:
            basis[step + 1] = value
        vectors.append(value)
    cut = [vector[:rows, :columns] for vector in vectors]
    partial = [jnp.sum(cut[i] * cut[j], axis=0, keepdims=True) for i, j in PAIRS]
    partial = [sum(part[:, k : k + LANES] for k in range(0, columns, LANES)) for part in partial]
    partial = partial + [jnp.zeros((LANES - len(partial), LANES), jnp.float32)]
    table = jnp.transpose(jnp.concatenate(partial, axis=0))
    products[...] = jnp.broadcast_to(jnp.sum(table, axis=0, keepdims=True)[None], products.shape)


def solve_kernel(gathered, basis, surface, pressure):
    rows, columns = surface.shape
    summed = jnp.sum(gathered[...], axis=0, keepdims=True)
    known = basis[ITERS + 2, :1, :LANES]
    at = lane_index((1, LANES))

    def entry(row, index):
        return jnp.sum(jnp.where(at == index, row, 0.0), axis=1, keepdims=True)

    gram = {}
    for index, (i, j) in enumerate(PAIRS):
        gram[i, j] = gram[j, i] = entry(summed, index)
    middle = [entry(known, step) for step in range(ITERS)]
    link = [entry(known, OFF_AT + step) for step in range(ITERS)]
    back = [entry(known, 2 * OFF_AT + step) for step in range(ITERS)]
    zero = jnp.zeros((1, 1), jnp.float32)

    def applied(vector):
        out = [zero] * (len(vector) + 1)
        for i, part in enumerate(vector):
            out[i] = out[i] + part + middle[i] * part
            out[i + 1] = out[i + 1] + link[i] * part
            if i:
                out[i - 1] = out[i - 1] + back[i] * part
        return out

    def inner(left, right):
        out = zero
        for i, a in enumerate(left):
            part = zero
            for j, b in enumerate(right):
                part = part + gram[i, j] * b
            out = out + a * part
        return out

    def scaled_add(left, scale, right):
        size = max(len(left), len(right))
        left = left + [zero] * (size - len(left))
        right = right + [zero] * (size - len(right))
        return [a + scale * b for a, b in zip(left, right)]

    residual = direction = [jnp.ones((1, 1), jnp.float32)]
    iterate = [zero]
    norm_now = gram[0, 0]
    for iteration in range(ITERS):
        image = applied(direction)
        product = inner(direction, image)
        step_size = jnp.where(product > 0.0, norm_now / product, 0.0)
        iterate = scaled_add(iterate, step_size, direction)
        if iteration + 1 < ITERS:
            residual = scaled_add(residual, -step_size, image)
            norm_next = inner(residual, residual)
            growth = jnp.where(norm_now > 0.0, norm_next / norm_now, 0.0)
            direction = scaled_add(residual, growth, direction)
            norm_now = norm_next
    value = iterate[0] * basis[0]
    for k in range(1, ITERS):
        value = value + iterate[k] * basis[k]
    surface[...] = value[:rows, :columns]
    opening = basis[ITERS]
    load = basis[ITERS + 1] * value
    full_rows, full_columns = value.shape
    pull = jnp.zeros_like(load)
    for shift, axis in ((1, 1), (full_columns - 1, 1), (1, 0), (full_rows - 1, 0)):
        pull = pull + opening * pltpu.roll(opening, shift, axis) * (pltpu.roll(load, shift, axis) - load)
    pressure[...] = -GRAVITY * pull[:rows, :columns]


def tracer_kernel(levels, temp, east, north, mask, from_south, from_north, tracer):
    rows, columns = temp.shape[1:]
    row = lax.broadcasted_iota(jnp.int32, (rows, columns), 0)
    lane = lane_index((rows, columns))
    base = 3 * RING
    for level in range(levels):
        masked = mask[level].astype(jnp.float32) * temp[level]
        east_coef = DIFFUSE - 0.5 * east[level]
        west_coef = DIFFUSE + 0.5 * east[level]
        north_coef = DIFFUSE - 0.5 * north[level]
        south_coef = DIFFUSE + 0.5 * north[level]
        side_south = from_south[base + level : base + level + 1, :]
        side_north = from_north[base + level : base + level + 1, :]
        inflow = jnp.where(lane == 0, 0.0, pltpu.roll(east_coef * masked, 1, 1))
        inflow = inflow + jnp.where(
            lane == columns - 1, 0.0, pltpu.roll(west_coef * masked, columns - 1, 1)
        )
        inflow = inflow + jnp.where(row == 0, side_south, pltpu.roll(north_coef * masked, 1, 0))
        inflow = inflow + jnp.where(
            row == rows - 1, side_north, pltpu.roll(south_coef * masked, rows - 1, 0)
        )
        tracer[level] = masked + TIMESTEP * (
            inflow - (east_coef + west_coef + north_coef + south_coef) * masked
        )


def level_of_slot(slots, slot, levels):
    level = jnp.int32(0)
    for k in range(1, levels):
        level = jnp.where(slots[k] == slot, jnp.int32(k), level)
    return level


def density(level, levels, pressure, mask):
    thickness = 1.0 + level.astype(jnp.float32) / levels
    return thickness * pressure[...] * mask[level].astype(jnp.float32)


def warm_kernel(levels, slots, tracer, pressure, from_west, from_east, mask, warm, partial, salt):
    rows, columns = pressure.shape
    lane = lane_index((rows, columns))
    sides = beside_tile(from_west, from_east, 3 * RING, levels)[:rows]
    for level in range(levels):
        side_west = sides[:, LANES - levels + level : LANES - levels + level + 1]
        side_east = sides[:, level : level + 1]
        edge = jnp.where(lane == 0, side_west, 0.0) + jnp.where(lane == columns - 1, side_east, 0.0)
        partial[level] = tracer[level] + TIMESTEP * edge
    for slot in range(levels):
        level = level_of_slot(slots, slot, levels)
        dense = density(level, levels, pressure, mask)
        value = warm[slot]
        salt[level] = (HALINE + CABBELING * value) * dense
        partial[level] = partial[level] + (THERMAL + 2.0 * NONLINEAR * value) * dense


def salt_kernel(levels, first, slots, partial, pressure, mask, part, *refs):
    result, done, sems = refs[-3:]
    size = part.shape[0]
    copies = []
    for at in range(size):
        level = level_of_slot(slots, first + at, levels)
        dense = density(level, levels, pressure, mask)
        done[at] = partial[level] + CABBELING * part[at] * dense
        copies.append(pltpu.make_async_copy(done.at[at], result.at[level], sems.at[at]))
        copies[-1].start()
    for copy in copies:
        copy.wait()


def finish(levels, first, args, before):
    part = args[-1]
    shape = (levels,) + part.shape[1:]
    held_args = [pltpu.with_memory_space_constraint(arg, pltpu.VMEM) for arg in args[1:]]
    operands = [args[0]] + held_args + ([] if before is None else [before])
    return pl.pallas_call(
        functools.partial(salt_kernel, levels, first),
        out_shape=jax.ShapeDtypeStruct(shape, jnp.float32),
        in_specs=[SMEM] + [VMEM] * len(held_args) + ([] if before is None else [HBM]),
        out_specs=HBM,
        scratch_shapes=[
            pltpu.VMEM(part.shape, jnp.float32),
            pltpu.SemaphoreType.DMA((part.shape[0],)),
        ],
        input_output_aliases={} if before is None else {len(operands) - 1: 0},
        compiler_params=pltpu.CompilerParams(vmem_limit_bytes=KERNEL_VMEM),
        cost_estimate=pl.CostEstimate(flops=1000000, bytes_accessed=1000000, transcendentals=0),
    )(*operands)


def shifted(value, axis, steps, around):
    count = lax.axis_size(axis)
    pairs = [(i, (i + steps) % count) for i in range(count) if around or 0 <= i + steps < count]
    return lax.ppermute(value, axis, pairs)


def shared(rows):
    rows = lax.all_to_all(rows, ("gx", "gy"), 0, 0)
    return rows.reshape(rows.shape[0], LANES)


def runs(levels):
    return levels // 2, levels - levels // 2


def body(
    temp_adjoint,
    height_adjoint,
    east_velocity,
    north_velocity,
    temp_store,
    salt_store,
    slot_map,
    land_mask,
    ocean_depth,
):
    levels, rows, columns = temp_adjoint.shape
    half_cycle = lax.axis_size("gx") // 2
    devices = lax.axis_size("gx") * lax.axis_size("gy")
    strip = 3 * RING + levels
    full = (rows + 2 * RING, columns + LANES)

    salt_sizes = runs(levels)
    slots = shifted(slot_map, "gx", half_cycle, True).reshape(-1)
    warm = shifted(temp_store, "gx", half_cycle, True)

    swap = lax.axis_size("gy") == 2
    fields, *messages = call(
        functools.partial(pack_y_kernel, levels),
        [(3, rows, columns)] + [(strip, columns)] * (1 if swap else 2),
        stored(height_adjoint, land_mask, ocean_depth, temp_adjoint, north_velocity),
    )
    if swap:
        arrived = [shifted(messages[0], "gy", 1, True)]
    else:
        arrived = [shifted(messages[0], "gy", 1, False)]
        arrived += [shifted(messages[1], "gy", -1, False)]
    (tile_rows,) = call(tile_basis_kernel, [(devices, 1, LANES)], held(fields))
    from_south, from_north, to_east, to_west = call(
        functools.partial(pack_x_kernel, levels, len(arrived)),
        [(strip, columns)] * 2 + [(strip, rows + LANES)] * 2,
        held(fields) + stored(land_mask, temp_adjoint, east_velocity) + held(*arrived),
    )
    from_west = shifted(to_east, "gx", 1, True)
    from_east = shifted(to_west, "gx", -1, True)
    (tracer,) = call(
        functools.partial(tracer_kernel, levels),
        [temp_adjoint.shape],
        stored(temp_adjoint, east_velocity, north_velocity, land_mask)
        + held(from_south, from_north),
        keep=[False],
    )
    cuts, start = [], 0
    for size in salt_sizes:
        cuts.append(lax.slice_in_dim(salt_store, start, start + size))
        start += size
    tiles = shared(tile_rows)
    salt_parts = [shifted(cut, "gx", half_cycle, True) for cut in cuts]
    beside = held(from_south, from_north, from_west, from_east)
    basis, products = call(
        krylov_kernel, [(ITERS + 3,) + full, (devices, 1, LANES)], held(fields) + beside + held(tiles)
    )
    gathered = shared(products)
    surface, pressure = call(solve_kernel, [(rows, columns)] * 2, held(gathered, basis), keep=[False, True])
    partial, salt_back = call(
        functools.partial(warm_kernel, levels),
        [temp_adjoint.shape] * 2,
        free(slots) + stored(tracer) + held(pressure, from_west, from_east) + free(land_mask, warm),
        specs=[SMEM] + [VMEM] * 6,
        keep=[True, False],
    )
    temp_back, first = None, 0
    for size, part in zip(salt_sizes, salt_parts):
        args = (slots, partial, pressure, land_mask, part)
        temp_back = finish(levels, first, args, temp_back)
        first += size
    return (temp_back, salt_back, surface)


def solution(mesh):
    return jax.shard_map(
        body,
        mesh=mesh,
        in_specs=(
            P(None, "gy", "gx"),
            P("gy", "gx"),
            P(None, "gy", "gx"),
            P(None, "gy", "gx"),
            P(None, "gy", "gx"),
            P(None, "gy", "gx"),
            P("gx", "gy", None),
            P(None, "gy", "gx"),
            P("gy", "gx"),
        ),
        out_specs=(P(None, "gy", "gx"), P(None, "gy", "gx"), P("gy", "gx")),
        check_vma=False,
    )
```

```python
import functools

import jax
import jax.numpy as jnp
from jax import lax
from jax.experimental import pallas as pl
from jax.experimental.pallas import tpu as pltpu
from jax.sharding import PartitionSpec as P


ITERS = 6
RING = 8
KERNEL_VMEM = 16 * 1024 * 1024
LANES = 128

DIFFUSE = 0.2
TIMESTEP = 1.0
STIFFNESS = 8.0
GRAVITY = 4.0
THERMAL = 0.5
NONLINEAR = 0.4
CABBELING = 0.3
HALINE = 0.8


VMEM = pl.BlockSpec(memory_space=pltpu.VMEM)
SMEM = pl.BlockSpec(memory_space=pltpu.SMEM)
HBM = pl.BlockSpec(memory_space=pltpu.HBM)

OFF_AT, WEIGHT_AT = 16, 32
PAIRS = [(i, j) for i in range(ITERS + 1) for j in range(i, ITERS + 1)]


def call(kernel, outs, args, specs=None, keep=None, flops=4000000):
    specs = specs or [VMEM] * len(args)
    keep = keep or [True] * len(outs)
    args = [
        arg if space is None else pltpu.with_memory_space_constraint(arg, space) for arg, space in args
    ]
    shapes = [
        pltpu.VMEM(shape, jnp.float32) if kept else jax.ShapeDtypeStruct(shape, jnp.float32)
        for shape, kept in zip(outs, keep)
    ]
    return pl.pallas_call(
        kernel,
        out_shape=shapes,
        in_specs=specs,
        out_specs=[VMEM] * len(outs),
        compiler_params=pltpu.CompilerParams(vmem_limit_bytes=KERNEL_VMEM),
        cost_estimate=pl.CostEstimate(flops=flops, bytes_accessed=1000000, transcendentals=0),
    )(*args)


def held(*arrays):
    return tuple((array, pltpu.VMEM) for array in arrays)


def stored(*arrays):
    return tuple((array, pltpu.HBM) for array in arrays)


def free(*arrays):
    return tuple((array, None) for array in arrays)


def total(value):
    return jnp.sum(jnp.sum(value, axis=0, keepdims=True), axis=1, keepdims=True)


def lane_index(shape):
    return lax.broadcasted_iota(jnp.int32, shape, 1)


def pack_y_kernel(levels, height, mask, depth, temp, north, fields, *messages):
    wet = mask[0].astype(jnp.float32)
    fields[0] = wet * height[...]
    fields[1] = wet
    fields[2] = depth[...]
    first, last = slice(0, RING), slice(temp.shape[1] - RING, temp.shape[1])

    def send(span, to_north, to_south):
        if len(messages) == 1:
            messages[0][span, :] = jnp.where(lax.axis_index("gy") == 0, to_north, to_south)
        else:
            messages[0][span, :] = to_north
            messages[1][span, :] = to_south

    for at in range(3):
        field = fields[at]
        send(slice(at * RING, (at + 1) * RING), field[last], field[first])
    base = 3 * RING
    for level in range(levels):
        flux_south = (DIFFUSE + 0.5 * north[level, first]) * (
            mask[level, first].astype(jnp.float32) * temp[level, first]
        )
        flux_north = (DIFFUSE - 0.5 * north[level, last]) * (
            mask[level, last].astype(jnp.float32) * temp[level, last]
        )
        send(slice(base + level, base + level + 1), flux_north[-1:], flux_south[:1])


def pack_x_kernel(levels, received, fields, mask, temp, east, *refs):
    arrived, (from_south, from_north, to_east, to_west) = refs[:received], refs[received:]
    if received == 1:
        lower = lax.axis_index("gy") == 0
        from_south[...] = jnp.where(lower, 0.0, arrived[0][...])
        from_north[...] = jnp.where(lower, arrived[0][...], 0.0)
    else:
        from_south[...] = arrived[0][...]
        from_north[...] = arrived[1][...]
    rows = fields.shape[1]
    for at in range(3):
        span = slice(at * RING, (at + 1) * RING)
        beside = [from_north[span, :], from_south[span, :]]
        beside.append(jnp.zeros((LANES - 2 * RING, fields.shape[2]), jnp.float32))
        flipped = jnp.transpose(jnp.concatenate([fields[at]] + beside, axis=0))
        to_west[span, :] = flipped[:RING]
        to_east[span, :] = flipped[-RING:]
    base = 3 * RING
    for level in range(levels):
        at = slice(base + level, base + level + 1)
        masked = mask[level].astype(jnp.float32) * temp[level]
        flux_east = (DIFFUSE - 0.5 * east[level]) * masked
        flux_west = (DIFFUSE + 0.5 * east[level]) * masked
        to_east[at, :rows] = jnp.transpose(flux_east[:, -LANES:])[-1:]
        to_west[at, :rows] = jnp.transpose(flux_west[:, :LANES])[:1]
    spare = slice(base, base + levels)
    to_east[spare, rows:] = jnp.zeros((levels, LANES), jnp.float32)
    to_west[spare, rows:] = jnp.zeros((levels, LANES), jnp.float32)


def beside_tile(from_west, from_east, start, size):
    span = slice(start, start + size)
    middle = jnp.zeros((LANES - 2 * size, from_west.shape[1]), jnp.float32)
    return jnp.transpose(jnp.concatenate([from_east[span, :], middle, from_west[span, :]], axis=0))


def tile_basis_kernel(fields, row_out):
    rows, columns = fields.shape[1:]
    wet, deep = fields[1], fields[2]
    row = lax.broadcasted_iota(jnp.int32, (rows, columns), 0)
    lane = lane_index((rows, columns))
    east_weight = (
        STIFFNESS * 0.5 * (deep + pltpu.roll(deep, columns - 1, 1)) * wet * pltpu.roll(wet, columns - 1, 1)
    )
    east_weight = jnp.where(lane == columns - 1, 0.0, east_weight)
    west_weight = pltpu.roll(east_weight, 1, 1)
    north_weight = STIFFNESS * 0.5 * (deep + pltpu.roll(deep, rows - 1, 0)) * wet * pltpu.roll(wet, rows - 1, 0)
    north_weight = jnp.where(row == rows - 1, 0.0, north_weight)
    south_weight = pltpu.roll(north_weight, 1, 0)

    def spread(field):
        out = west_weight * (field - pltpu.roll(field, 1, 1))
        out = out + east_weight * (field - pltpu.roll(field, columns - 1, 1))
        out = out + south_weight * (field - pltpu.roll(field, 1, 0))
        return out + north_weight * (field - pltpu.roll(field, rows - 1, 0))

    field = fields[0]
    square = total(field * field)
    weight = jnp.sqrt(square)
    vector = field * jnp.where(square > 0.0, lax.rsqrt(jnp.maximum(square, 1e-30)), 0.0)
    before, link = jnp.zeros_like(vector), jnp.zeros_like(square)
    at = lane_index((1, LANES))
    out = jnp.where(at == WEIGHT_AT, weight, 0.0)
    for step in range(ITERS):
        image = spread(vector) - link * before
        along, size = total(image * vector), total(image * image)
        out = jnp.where(at == step, along, out)
        if step + 1 < ITERS:
            left = size - along * along
            alive = left > 1e-6 * size
            scale = jnp.where(alive, lax.rsqrt(jnp.maximum(left, 1e-30)), 0.0)
            link = jnp.where(alive, jnp.sqrt(jnp.maximum(left, 0.0)), 0.0)
            before, vector = vector, (image - along * vector) * scale
            out = jnp.where(at == OFF_AT + step, link, out)
    place = lax.axis_index("gx") * lax.axis_size("gy") + lax.axis_index("gy")
    own = lax.broadcasted_iota(jnp.int32, row_out.shape, 0) == place
    row_out[...] = jnp.where(own, out, 0.0)


def merged_recurrence(tiles):
    at = lane_index(tiles.shape)
    diagonal = jnp.where(at < ITERS, tiles, 0.0)
    above = jnp.where(at < ITERS - 1, pltpu.roll(tiles, LANES - OFF_AT, 1), 0.0)
    below = pltpu.roll(above, 1, 1)
    vector = jnp.where(at == 0, pltpu.roll(tiles, LANES - WEIGHT_AT, 1), 0.0)
    square = total(vector * vector)
    vector = vector * jnp.where(square > 0.0, lax.rsqrt(jnp.maximum(square, 1e-30)), 0.0)
    before, link = jnp.zeros_like(vector), jnp.zeros_like(square)
    running = jnp.ones_like(square)
    steps = []
    for _ in range(ITERS):
        image = diagonal * vector - link * before
        image = image + above * pltpu.roll(vector, LANES - 1, 1) + below * pltpu.roll(vector, 1, 1)
        along, size = total(image * vector), total(image * image)
        left = size - along * along
        alive = left > 1e-6 * size
        middle = jnp.where(running > 0.0, along, 4.0 * STIFFNESS)
        back = link
        scale = jnp.where(alive, lax.rsqrt(jnp.maximum(left, 1e-30)), 0.0)
        link = jnp.where(alive, jnp.sqrt(jnp.maximum(left, 0.0)), 0.0)
        steps.append((middle, jnp.where(alive, link, 2.0 * STIFFNESS), back))
        running = jnp.where(alive, running, 0.0)
        before, vector = vector, (image - along * vector) * scale
    return steps


def krylov_kernel(fields, from_south, from_north, from_west, from_east, tiles, basis, products):
    rows, columns = fields.shape[1:]
    full_rows, full_columns = rows + 2 * RING, columns + LANES

    def widened(at):
        span = slice(at * RING, (at + 1) * RING)
        tile = jnp.concatenate([fields[at], from_north[span, :], from_south[span, :]], axis=0)
        side = beside_tile(from_west, from_east, at * RING, RING)
        return jnp.concatenate([tile, side[:full_rows]], axis=1)

    field, opening, deep = widened(0), widened(1), widened(2)
    basis[ITERS] = opening
    basis[ITERS + 1] = deep
    west_weight = STIFFNESS * 0.5 * (deep + pltpu.roll(deep, 1, 1)) * opening * pltpu.roll(opening, 1, 1)
    east_weight = pltpu.roll(west_weight, full_columns - 1, 1)
    south_weight = STIFFNESS * 0.5 * (deep + pltpu.roll(deep, 1, 0)) * opening * pltpu.roll(opening, 1, 0)
    north_weight = pltpu.roll(south_weight, full_rows - 1, 0)

    def spread(value):
        out = west_weight * (value - pltpu.roll(value, 1, 1))
        out = out + east_weight * (value - pltpu.roll(value, full_columns - 1, 1))
        out = out + south_weight * (value - pltpu.roll(value, 1, 0))
        return out + north_weight * (value - pltpu.roll(value, full_rows - 1, 0))

    steps = merged_recurrence(tiles[...])
    at = lane_index((1, LANES))
    row = jnp.zeros((1, LANES), jnp.float32)
    for step, entries in enumerate(steps):
        for kind, entry in enumerate(entries):
            row = jnp.where(at == kind * OFF_AT + step, entry, row)
    basis[ITERS + 2, :1, :LANES] = row
    vectors = [field]
    before, value = None, field
    basis[0] = field
    for step, (middle, link, back) in enumerate(steps):
        image = spread(value) - middle * value
        if step:
            image = image - back * before
        before, value = value, image * (1.0 / link)
        if step + 1 < ITERS:
            basis[step + 1] = value
        vectors.append(value)
    cut = [vector[:rows, :columns] for vector in vectors]
    partial = [jnp.sum(cut[i] * cut[j], axis=0, keepdims=True) for i, j in PAIRS]
    partial = [sum(part[:, k : k + LANES] for k in range(0, columns, LANES)) for part in partial]
    partial = partial + [jnp.zeros((LANES - len(partial), LANES), jnp.float32)]
    table = jnp.transpose(jnp.concatenate(partial, axis=0))
    products[...] = jnp.sum(table, axis=0, keepdims=True)


def solve_kernel(gathered, basis, surface, pressure):
    rows, columns = surface.shape
    summed = gathered[...]
    known = basis[ITERS + 2, :1, :LANES]
    at = lane_index((1, LANES))

    def entry(row, index):
        return jnp.sum(jnp.where(at == index, row, 0.0), axis=1, keepdims=True)

    gram = {}
    for index, (i, j) in enumerate(PAIRS):
        gram[i, j] = gram[j, i] = entry(summed, index)
    middle = [entry(known, step) for step in range(ITERS)]
    link = [entry(known, OFF_AT + step) for step in range(ITERS)]
    back = [entry(known, 2 * OFF_AT + step) for step in range(ITERS)]
    zero = jnp.zeros((1, 1), jnp.float32)

    def applied(vector):
        out = [zero] * (len(vector) + 1)
        for i, part in enumerate(vector):
            out[i] = out[i] + part + middle[i] * part
            out[i + 1] = out[i + 1] + link[i] * part
            if i:
                out[i - 1] = out[i - 1] + back[i] * part
        return out

    def inner(left, right):
        out = zero
        for i, a in enumerate(left):
            part = zero
            for j, b in enumerate(right):
                part = part + gram[i, j] * b
            out = out + a * part
        return out

    def scaled_add(left, scale, right):
        size = max(len(left), len(right))
        left = left + [zero] * (size - len(left))
        right = right + [zero] * (size - len(right))
        return [a + scale * b for a, b in zip(left, right)]

    residual = direction = [jnp.ones((1, 1), jnp.float32)]
    iterate = [zero]
    norm_now = gram[0, 0]
    for iteration in range(ITERS):
        image = applied(direction)
        product = inner(direction, image)
        step_size = jnp.where(product > 0.0, norm_now / product, 0.0)
        iterate = scaled_add(iterate, step_size, direction)
        if iteration + 1 < ITERS:
            residual = scaled_add(residual, -step_size, image)
            norm_next = inner(residual, residual)
            growth = jnp.where(norm_now > 0.0, norm_next / norm_now, 0.0)
            direction = scaled_add(residual, growth, direction)
            norm_now = norm_next
    value = iterate[0] * basis[0]
    for k in range(1, ITERS):
        value = value + iterate[k] * basis[k]
    surface[...] = value[:rows, :columns]
    opening = basis[ITERS]
    load = basis[ITERS + 1] * value
    full_rows, full_columns = value.shape
    pull = jnp.zeros_like(load)
    for shift, axis in ((1, 1), (full_columns - 1, 1), (1, 0), (full_rows - 1, 0)):
        pull = pull + opening * pltpu.roll(opening, shift, axis) * (pltpu.roll(load, shift, axis) - load)
    pressure[...] = -GRAVITY * pull[:rows, :columns]


def tracer_kernel(levels, temp, east, north, mask, from_south, from_north, tracer):
    rows, columns = temp.shape[1:]
    row = lax.broadcasted_iota(jnp.int32, (rows, columns), 0)
    lane = lane_index((rows, columns))
    base = 3 * RING
    for level in range(levels):
        masked = mask[level].astype(jnp.float32) * temp[level]
        east_coef = DIFFUSE - 0.5 * east[level]
        west_coef = DIFFUSE + 0.5 * east[level]
        north_coef = DIFFUSE - 0.5 * north[level]
        south_coef = DIFFUSE + 0.5 * north[level]
        side_south = from_south[base + level : base + level + 1, :]
        side_north = from_north[base + level : base + level + 1, :]
        inflow = jnp.where(lane == 0, 0.0, pltpu.roll(east_coef * masked, 1, 1))
        inflow = inflow + jnp.where(
            lane == columns - 1, 0.0, pltpu.roll(west_coef * masked, columns - 1, 1)
        )
        inflow = inflow + jnp.where(row == 0, side_south, pltpu.roll(north_coef * masked, 1, 0))
        inflow = inflow + jnp.where(
            row == rows - 1, side_north, pltpu.roll(south_coef * masked, rows - 1, 0)
        )
        tracer[level] = masked + TIMESTEP * (
            inflow - (east_coef + west_coef + north_coef + south_coef) * masked
        )


def level_of_slot(slots, slot, levels):
    level = jnp.int32(0)
    for k in range(1, levels):
        level = jnp.where(slots[k] == slot, jnp.int32(k), level)
    return level


def density(level, levels, pressure, mask):
    thickness = 1.0 + level.astype(jnp.float32) / levels
    return thickness * pressure[...] * mask[level].astype(jnp.float32)


def warm_kernel(levels, slots, tracer, pressure, from_west, from_east, mask, warm, partial, salt):
    rows, columns = pressure.shape
    lane = lane_index((rows, columns))
    sides = beside_tile(from_west, from_east, 3 * RING, levels)[:rows]
    for level in range(levels):
        side_west = sides[:, LANES - levels + level : LANES - levels + level + 1]
        side_east = sides[:, level : level + 1]
        edge = jnp.where(lane == 0, side_west, 0.0) + jnp.where(lane == columns - 1, side_east, 0.0)
        partial[level] = tracer[level] + TIMESTEP * edge
    for slot in range(levels):
        level = level_of_slot(slots, slot, levels)
        dense = density(level, levels, pressure, mask)
        value = warm[slot]
        salt[level] = (HALINE + CABBELING * value) * dense
        partial[level] = partial[level] + (THERMAL + 2.0 * NONLINEAR * value) * dense


def salt_kernel(levels, first, slots, partial, pressure, mask, part, *refs):
    result, done, sems = refs[-3:]
    size = part.shape[0]
    copies = []
    for at in range(size):
        level = level_of_slot(slots, first + at, levels)
        dense = density(level, levels, pressure, mask)
        done[at] = partial[level] + CABBELING * part[at] * dense
        copies.append(pltpu.make_async_copy(done.at[at], result.at[level], sems.at[at]))
        copies[-1].start()
    for copy in copies:
        copy.wait()


def finish(levels, first, args, before):
    part = args[-1]
    shape = (levels,) + part.shape[1:]
    held_args = [pltpu.with_memory_space_constraint(arg, pltpu.VMEM) for arg in args[1:]]
    operands = [args[0]] + held_args + ([] if before is None else [before])
    return pl.pallas_call(
        functools.partial(salt_kernel, levels, first),
        out_shape=jax.ShapeDtypeStruct(shape, jnp.float32),
        in_specs=[SMEM] + [VMEM] * len(held_args) + ([] if before is None else [HBM]),
        out_specs=HBM,
        scratch_shapes=[
            pltpu.VMEM(part.shape, jnp.float32),
            pltpu.SemaphoreType.DMA((part.shape[0],)),
        ],
        input_output_aliases={} if before is None else {len(operands) - 1: 0},
        compiler_params=pltpu.CompilerParams(vmem_limit_bytes=KERNEL_VMEM),
        cost_estimate=pl.CostEstimate(flops=1000000, bytes_accessed=1000000, transcendentals=0),
    )(*operands)


def shifted(value, axis, steps, around):
    count = lax.axis_size(axis)
    pairs = [(i, (i + steps) % count) for i in range(count) if around or 0 <= i + steps < count]
    return lax.ppermute(value, axis, pairs)


def swapped(value, axis, flip):
    pairs = [(i, i ^ flip) for i in range(lax.axis_size(axis))]
    return lax.ppermute(value, axis, pairs)


def shared(value):
    count_x, count_y = lax.axis_size("gx"), lax.axis_size("gy")
    inner = 4
    assert count_x & (count_x - 1) == 0 and count_y & (count_y - 1) == 0 and count_x >= inner
    flips = [("gy", 1 << bit) for bit in range(count_y.bit_length() - 1)] + [("gx", 2), ("gx", 1)]
    for axis, flip in flips:
        value = value + swapped(value, axis, flip)
    terms = [value] + [swapped(value, "gx", flip) for flip in range(inner, count_x, inner)]
    while len(terms) > 1:
        terms = [a + b for a, b in zip(terms[::2], terms[1::2])]
    return terms[0]


def runs(levels):
    most = 5 * levels // 8
    return most, levels - most


def body(
    temp_adjoint,
    height_adjoint,
    east_velocity,
    north_velocity,
    temp_store,
    salt_store,
    slot_map,
    land_mask,
    ocean_depth,
):
    levels, rows, columns = temp_adjoint.shape
    half_cycle = lax.axis_size("gx") // 2
    devices = lax.axis_size("gx") * lax.axis_size("gy")
    strip = 3 * RING + levels
    full = (rows + 2 * RING, columns + LANES)

    salt_sizes = runs(levels)
    slots = shifted(slot_map, "gx", half_cycle, True).reshape(-1)
    warm = shifted(temp_store, "gx", half_cycle, True)

    swap = lax.axis_size("gy") == 2
    fields, *messages = call(
        functools.partial(pack_y_kernel, levels),
        [(3, rows, columns)] + [(strip, columns)] * (1 if swap else 2),
        stored(height_adjoint, land_mask, ocean_depth, temp_adjoint, north_velocity),
    )
    if swap:
        arrived = [shifted(messages[0], "gy", 1, True)]
    else:
        arrived = [shifted(messages[0], "gy", 1, False)]
        arrived += [shifted(messages[1], "gy", -1, False)]
    (tile_rows,) = call(tile_basis_kernel, [(devices, LANES)], held(fields))
    from_south, from_north, to_east, to_west = call(
        functools.partial(pack_x_kernel, levels, len(arrived)),
        [(strip, columns)] * 2 + [(strip, rows + LANES)] * 2,
        held(fields) + stored(land_mask, temp_adjoint, east_velocity) + held(*arrived),
    )
    from_west = shifted(to_east, "gx", 1, True)
    from_east = shifted(to_west, "gx", -1, True)
    (tracer,) = call(
        functools.partial(tracer_kernel, levels),
        [temp_adjoint.shape],
        stored(temp_adjoint, east_velocity, north_velocity, land_mask)
        + held(from_south, from_north),
        keep=[False],
    )
    cuts, start = [], 0
    for size in salt_sizes:
        cuts.append(lax.slice_in_dim(salt_store, start, start + size))
        start += size
    tiles = shared(tile_rows)
    salt_parts = [shifted(cut, "gx", half_cycle, True) for cut in cuts]
    beside = held(from_south, from_north, from_west, from_east)
    basis, products = call(krylov_kernel, [(ITERS + 3,) + full, (1, LANES)], held(fields) + beside + held(tiles))
    gathered = shared(products)
    surface, pressure = call(solve_kernel, [(rows, columns)] * 2, held(gathered, basis), keep=[False, True])
    partial, salt_back = call(
        functools.partial(warm_kernel, levels),
        [temp_adjoint.shape] * 2,
        free(slots) + stored(tracer) + held(pressure, from_west, from_east) + free(land_mask, warm),
        specs=[SMEM] + [VMEM] * 6,
        keep=[True, False],
    )
    temp_back, first = None, 0
    for size, part in zip(salt_sizes, salt_parts):
        args = (slots, partial, pressure, land_mask, part)
        temp_back = finish(levels, first, args, temp_back)
        first += size
    return (temp_back, salt_back, surface)


def solution(mesh):
    return jax.shard_map(
        body,
        mesh=mesh,
        in_specs=(
            P(None, "gy", "gx"),
            P("gy", "gx"),
            P(None, "gy", "gx"),
            P(None, "gy", "gx"),
            P(None, "gy", "gx"),
            P(None, "gy", "gx"),
            P("gx", "gy", None),
            P(None, "gy", "gx"),
            P("gy", "gx"),
        ),
        out_specs=(P(None, "gy", "gx"), P(None, "gy", "gx"), P("gy", "gx")),
        check_vma=False,
    )
```

```python
import functools

import jax
import jax.numpy as jnp
from jax import lax
from jax.experimental import pallas as pl
from jax.experimental.pallas import tpu as pltpu
from jax.sharding import PartitionSpec as P


ITERS = 6
RING = 8
KERNEL_VMEM = 16 * 1024 * 1024
LANES = 128

DIFFUSE = 0.2
TIMESTEP = 1.0
STIFFNESS = 8.0
GRAVITY = 4.0
THERMAL = 0.5
NONLINEAR = 0.4
CABBELING = 0.3
HALINE = 0.8


VMEM = pl.BlockSpec(memory_space=pltpu.VMEM)
SMEM = pl.BlockSpec(memory_space=pltpu.SMEM)
HBM = pl.BlockSpec(memory_space=pltpu.HBM)

PAIRS = [(i, j) for i in range(ITERS + 1) for j in range(i, ITERS + 1)]
MIDDLE_AT, LINK_AT, BACK_AT, WEIGHT_AT = 32, 40, 48, 56


def call(kernel, outs, args, specs=None, keep=None, flops=4000000):
    specs = specs or [VMEM] * len(args)
    keep = keep or [True] * len(outs)
    args = [
        arg if space is None else pltpu.with_memory_space_constraint(arg, space) for arg, space in args
    ]
    shapes = [
        pltpu.VMEM(shape, jnp.float32) if kept else jax.ShapeDtypeStruct(shape, jnp.float32)
        for shape, kept in zip(outs, keep)
    ]
    return pl.pallas_call(
        kernel,
        out_shape=shapes,
        in_specs=specs,
        out_specs=[VMEM] * len(outs),
        compiler_params=pltpu.CompilerParams(vmem_limit_bytes=KERNEL_VMEM),
        cost_estimate=pl.CostEstimate(flops=flops, bytes_accessed=1000000, transcendentals=0),
    )(*args)


def held(*arrays):
    return tuple((array, pltpu.VMEM) for array in arrays)


def stored(*arrays):
    return tuple((array, pltpu.HBM) for array in arrays)


def free(*arrays):
    return tuple((array, None) for array in arrays)


def total(value):
    return jnp.sum(jnp.sum(value, axis=0, keepdims=True), axis=1, keepdims=True)


def lane_index(shape):
    return lax.broadcasted_iota(jnp.int32, shape, 1)


def pack_y_kernel(levels, height, mask, depth, temp, north, fields, *messages):
    wet = mask[0].astype(jnp.float32)
    fields[0] = wet * height[...]
    fields[1] = wet
    fields[2] = depth[...]
    first, last = slice(0, RING), slice(temp.shape[1] - RING, temp.shape[1])

    def send(span, to_north, to_south):
        if len(messages) == 1:
            messages[0][span, :] = jnp.where(lax.axis_index("gy") == 0, to_north, to_south)
        else:
            messages[0][span, :] = to_north
            messages[1][span, :] = to_south

    for at in range(3):
        field = fields[at]
        send(slice(at * RING, (at + 1) * RING), field[last], field[first])
    base = 3 * RING
    for level in range(levels):
        flux_south = (DIFFUSE + 0.5 * north[level, first]) * (
            mask[level, first].astype(jnp.float32) * temp[level, first]
        )
        flux_north = (DIFFUSE - 0.5 * north[level, last]) * (
            mask[level, last].astype(jnp.float32) * temp[level, last]
        )
        send(slice(base + level, base + level + 1), flux_north[-1:], flux_south[:1])


def pack_x_kernel(levels, received, fields, mask, temp, east, *refs):
    arrived, (from_south, from_north, to_east, to_west) = refs[:received], refs[received:]
    if received == 1:
        lower = lax.axis_index("gy") == 0
        from_south[...] = jnp.where(lower, 0.0, arrived[0][...])
        from_north[...] = jnp.where(lower, arrived[0][...], 0.0)
    else:
        from_south[...] = arrived[0][...]
        from_north[...] = arrived[1][...]
    rows = fields.shape[1]
    for at in range(3):
        span = slice(at * RING, (at + 1) * RING)
        beside = [from_north[span, :], from_south[span, :]]
        beside.append(jnp.zeros((LANES - 2 * RING, fields.shape[2]), jnp.float32))
        flipped = jnp.transpose(jnp.concatenate([fields[at]] + beside, axis=0))
        to_west[span, :] = flipped[:RING]
        to_east[span, :] = flipped[-RING:]
    base = 3 * RING
    for level in range(levels):
        at = slice(base + level, base + level + 1)
        masked = mask[level].astype(jnp.float32) * temp[level]
        flux_east = (DIFFUSE - 0.5 * east[level]) * masked
        flux_west = (DIFFUSE + 0.5 * east[level]) * masked
        to_east[at, :rows] = jnp.transpose(flux_east[:, -LANES:])[-1:]
        to_west[at, :rows] = jnp.transpose(flux_west[:, :LANES])[:1]
    spare = slice(base, base + levels)
    to_east[spare, rows:] = jnp.zeros((levels, LANES), jnp.float32)
    to_west[spare, rows:] = jnp.zeros((levels, LANES), jnp.float32)


def beside_tile(from_west, from_east, start, size):
    span = slice(start, start + size)
    middle = jnp.zeros((LANES - 2 * size, from_west.shape[1]), jnp.float32)
    return jnp.transpose(jnp.concatenate([from_east[span, :], middle, from_west[span, :]], axis=0))


def krylov_kernel(fields, from_south, from_north, from_west, from_east, basis, row_out):
    rows, columns = fields.shape[1:]
    full_rows, full_columns = rows + 2 * RING, columns + LANES

    def widened(at):
        span = slice(at * RING, (at + 1) * RING)
        tile = jnp.concatenate([fields[at], from_north[span, :], from_south[span, :]], axis=0)
        side = beside_tile(from_west, from_east, at * RING, RING)
        return jnp.concatenate([tile, side[:full_rows]], axis=1)

    field, opening, deep = widened(0), widened(1), widened(2)
    basis[ITERS] = opening
    basis[ITERS + 1] = deep
    west_weight = STIFFNESS * 0.5 * (deep + pltpu.roll(deep, 1, 1)) * opening * pltpu.roll(opening, 1, 1)
    east_weight = pltpu.roll(west_weight, full_columns - 1, 1)
    south_weight = STIFFNESS * 0.5 * (deep + pltpu.roll(deep, 1, 0)) * opening * pltpu.roll(opening, 1, 0)
    north_weight = pltpu.roll(south_weight, full_rows - 1, 0)

    def spread(value):
        out = west_weight * (value - pltpu.roll(value, 1, 1))
        out = out + east_weight * (value - pltpu.roll(value, full_columns - 1, 1))
        out = out + south_weight * (value - pltpu.roll(value, 1, 0))
        return out + north_weight * (value - pltpu.roll(value, full_rows - 1, 0))

    at = lane_index((1, LANES))
    square = total(field * field)
    row = jnp.where(at == WEIGHT_AT, jnp.sqrt(square), 0.0)
    value = field * jnp.where(square > 0.0, lax.rsqrt(jnp.maximum(square, 1e-30)), 0.0)
    running = jnp.where(square > 0.0, 1.0, 0.0)
    before, back = jnp.zeros_like(value), jnp.zeros_like(square)
    vectors = [value]
    basis[0] = value
    for step in range(ITERS):
        image = spread(value) - back * before
        along, size = total(image * value), total(image * image)
        middle, link, scale, alive = next_step(along, size, running)
        for start, entry in ((MIDDLE_AT, middle), (LINK_AT, link), (BACK_AT, back)):
            row = jnp.where(at == start + step, entry, row)
        before, value = value, (image - middle * value) * scale
        running, back = alive, link * alive
        vectors.append(value)
        if step + 1 < ITERS:
            basis[step + 1] = value
    cut = [vector[:rows, :columns] for vector in vectors]
    partial = [jnp.sum(cut[i] * cut[j], axis=0, keepdims=True) for i, j in PAIRS]
    partial = [sum(part[:, k : k + LANES] for k in range(0, columns, LANES)) for part in partial]
    partial = partial + [jnp.zeros((LANES - len(partial), LANES), jnp.float32)]
    table = jnp.transpose(jnp.concatenate(partial, axis=0))
    row = row + jnp.sum(table, axis=0, keepdims=True)
    row_out[...] = jnp.broadcast_to(row[None], row_out.shape)


def next_step(along, size, running):
    left = size - along * along
    alive = jnp.where((left > 1e-6 * size) & (running > 0.0), 1.0, 0.0)
    safe = jnp.maximum(left, 1e-30)
    middle = jnp.where(running > 0.0, along, 4.0 * STIFFNESS)
    link = jnp.where(alive > 0.0, jnp.sqrt(safe), 2.0 * STIFFNESS)
    scale = jnp.where(alive > 0.0, lax.rsqrt(safe), 1.0 / (2.0 * STIFFNESS))
    return middle, link, scale, alive


def merged_recurrence(tiles):
    at = lane_index(tiles.shape)
    diagonal = jnp.where(at < ITERS, pltpu.roll(tiles, LANES - MIDDLE_AT, 1), 0.0)
    above = jnp.where(at < ITERS - 1, pltpu.roll(tiles, LANES - BACK_AT - 1, 1), 0.0)
    below = pltpu.roll(above, 1, 1)
    vector = jnp.where(at == 0, pltpu.roll(tiles, LANES - WEIGHT_AT, 1), 0.0)
    square = total(vector * vector)
    vector = vector * jnp.where(square > 0.0, lax.rsqrt(jnp.maximum(square, 1e-30)), 0.0)
    before, back = jnp.zeros_like(vector), jnp.zeros_like(square)
    running = jnp.ones_like(square)
    steps = []
    for _ in range(ITERS):
        image = diagonal * vector - back * before
        image = image + above * pltpu.roll(vector, LANES - 1, 1) + below * pltpu.roll(vector, 1, 1)
        along, size = total(image * vector), total(image * image)
        middle, link, scale, alive = next_step(along, size, running)
        steps.append((middle, link, scale, back))
        before, vector = vector, (image - along * vector) * (scale * alive)
        running, back = alive, link * alive
    return steps


def solve_kernel(gathered, basis, surface, pressure):
    rows, columns = surface.shape
    place = lax.axis_index("gx") * lax.axis_size("gy") + lax.axis_index("gy")
    tiles = gathered[...]
    steps = merged_recurrence(tiles)
    spare = -tiles.shape[0] % LANES
    if spare:
        tiles = jnp.concatenate([tiles, jnp.zeros((spare, LANES), jnp.float32)], axis=0)
    table = jnp.transpose(tiles)

    def known(index):
        return table[index : index + 1, :]

    products = {}
    for index, (i, j) in enumerate(PAIRS):
        products[i, j] = products[j, i] = known(index)
    change = [[known(WEIGHT_AT)]]
    for step, (middle, _, scale, back) in enumerate(steps):
        last = change[step]
        out = [None] * (step + 2)

        def add(at, term):
            out[at] = term if out[at] is None else out[at] + term

        for j, part in enumerate(last):
            add(j, (known(MIDDLE_AT + j) - middle) * part)
            add(j + 1, known(LINK_AT + j) * part)
            if j:
                add(j - 1, known(BACK_AT + j) * part)
        if step:
            for j, part in enumerate(change[step - 1]):
                add(j, -back * part)
        change.append([scale * term for term in out])
    gram = {}
    for k in range(ITERS + 1):
        half = [
            sum(change[k][i] * products[i, j] for i in range(k + 1)) for j in range(ITERS + 1)
        ]
        for m in range(k, ITERS + 1):
            both = sum(half[j] * change[m][j] for j in range(m + 1))
            gram[k, m] = gram[m, k] = jnp.sum(both, axis=1, keepdims=True)
    zero = jnp.zeros((1, 1), jnp.float32)

    def applied(vector):
        out = [zero] * (len(vector) + 1)
        for i, part in enumerate(vector):
            middle, link, _, back = steps[i]
            out[i] = out[i] + part + middle * part
            out[i + 1] = out[i + 1] + link * part
            if i:
                out[i - 1] = out[i - 1] + back * part
        return out

    def inner(left, right):
        out = zero
        for i, a in enumerate(left):
            part = zero
            for j, b in enumerate(right):
                part = part + gram[i, j] * b
            out = out + a * part
        return out

    def scaled_add(left, scale, right):
        size = max(len(left), len(right))
        left = left + [zero] * (size - len(left))
        right = right + [zero] * (size - len(right))
        return [a + scale * b for a, b in zip(left, right)]

    residual = direction = [jnp.ones((1, 1), jnp.float32)]
    iterate = [zero]
    norm_now = gram[0, 0]
    for iteration in range(ITERS):
        image = applied(direction)
        product = inner(direction, image)
        step_size = jnp.where(product > 0.0, norm_now / product, 0.0)
        iterate = scaled_add(iterate, step_size, direction)
        if iteration + 1 < ITERS:
            residual = scaled_add(residual, -step_size, image)
            norm_next = inner(residual, residual)
            growth = jnp.where(norm_now > 0.0, norm_next / norm_now, 0.0)
            direction = scaled_add(residual, growth, direction)
            norm_now = norm_next
    mine = lane_index((1, table.shape[1])) == place
    value = None
    for j in range(ITERS):
        weight = sum(iterate[k] * change[k][j] for k in range(j, ITERS))
        weight = jnp.sum(jnp.where(mine, weight, 0.0), axis=1, keepdims=True)
        value = weight * basis[j] if value is None else value + weight * basis[j]
    surface[...] = value[:rows, :columns]
    opening = basis[ITERS]
    load = basis[ITERS + 1] * value
    full_rows, full_columns = value.shape
    pull = jnp.zeros_like(load)
    for shift, axis in ((1, 1), (full_columns - 1, 1), (1, 0), (full_rows - 1, 0)):
        pull = pull + opening * pltpu.roll(opening, shift, axis) * (pltpu.roll(load, shift, axis) - load)
    pressure[...] = -GRAVITY * pull[:rows, :columns]


def tracer_kernel(levels, temp, east, north, mask, from_south, from_north, tracer):
    rows, columns = temp.shape[1:]
    row = lax.broadcasted_iota(jnp.int32, (rows, columns), 0)
    lane = lane_index((rows, columns))
    base = 3 * RING
    for level in range(levels):
        masked = mask[level].astype(jnp.float32) * temp[level]
        east_coef = DIFFUSE - 0.5 * east[level]
        west_coef = DIFFUSE + 0.5 * east[level]
        north_coef = DIFFUSE - 0.5 * north[level]
        south_coef = DIFFUSE + 0.5 * north[level]
        side_south = from_south[base + level : base + level + 1, :]
        side_north = from_north[base + level : base + level + 1, :]
        inflow = jnp.where(lane == 0, 0.0, pltpu.roll(east_coef * masked, 1, 1))
        inflow = inflow + jnp.where(
            lane == columns - 1, 0.0, pltpu.roll(west_coef * masked, columns - 1, 1)
        )
        inflow = inflow + jnp.where(row == 0, side_south, pltpu.roll(north_coef * masked, 1, 0))
        inflow = inflow + jnp.where(
            row == rows - 1, side_north, pltpu.roll(south_coef * masked, rows - 1, 0)
        )
        tracer[level] = masked + TIMESTEP * (
            inflow - (east_coef + west_coef + north_coef + south_coef) * masked
        )


def level_of_slot(slots, slot, levels):
    level = jnp.int32(0)
    for k in range(1, levels):
        level = jnp.where(slots[k] == slot, jnp.int32(k), level)
    return level


def density(level, levels, pressure, mask):
    thickness = 1.0 + level.astype(jnp.float32) / levels
    return thickness * pressure[...] * mask[level].astype(jnp.float32)


def warm_kernel(levels, slots, tracer, pressure, from_west, from_east, mask, outer, inner, partial, salt):
    rows, columns = pressure.shape
    lane = lane_index((rows, columns))
    sides = beside_tile(from_west, from_east, 3 * RING, levels)[:rows]
    for level in range(levels):
        side_west = sides[:, LANES - levels + level : LANES - levels + level + 1]
        side_east = sides[:, level : level + 1]
        edge = jnp.where(lane == 0, side_west, 0.0) + jnp.where(lane == columns - 1, side_east, 0.0)
        partial[level] = tracer[level] + TIMESTEP * edge
    for slot in range(levels):
        level = level_of_slot(slots, slot, levels)
        dense = density(level, levels, pressure, mask)
        value = jnp.where(from_outer(), outer[slot], inner[slot])
        salt[level] = (HALINE + CABBELING * value) * dense
        partial[level] = partial[level] + (THERMAL + 2.0 * NONLINEAR * value) * dense


def salt_kernel(levels, first, slots, partial, pressure, mask, inner, part, *refs):
    result, done, sems = refs[-3:]
    size = part.shape[0]
    copies = []
    for at in range(size):
        level = level_of_slot(slots, first + at, levels)
        dense = density(level, levels, pressure, mask)
        done[at] = partial[level] + CABBELING * jnp.where(from_outer(), part[at], inner[first + at]) * dense
        copies.append(pltpu.make_async_copy(done.at[at], result.at[level], sems.at[at]))
        copies[-1].start()
    for copy in copies:
        copy.wait()


def finish(levels, first, args, before):
    part = args[-1]
    shape = (levels,) + part.shape[1:]
    held_args = [pltpu.with_memory_space_constraint(arg, pltpu.VMEM) for arg in args[1:]]
    operands = [args[0]] + held_args + ([] if before is None else [before])
    return pl.pallas_call(
        functools.partial(salt_kernel, levels, first),
        out_shape=jax.ShapeDtypeStruct(shape, jnp.float32),
        in_specs=[SMEM] + [VMEM] * len(held_args) + ([] if before is None else [HBM]),
        out_specs=HBM,
        scratch_shapes=[
            pltpu.VMEM(part.shape, jnp.float32),
            pltpu.SemaphoreType.DMA((part.shape[0],)),
        ],
        input_output_aliases={} if before is None else {len(operands) - 1: 0},
        compiler_params=pltpu.CompilerParams(vmem_limit_bytes=KERNEL_VMEM),
        cost_estimate=pl.CostEstimate(flops=1000000, bytes_accessed=1000000, transcendentals=0),
    )(*operands)


def shifted(value, axis, steps, around):
    count = lax.axis_size(axis)
    pairs = [(i, (i + steps) % count) for i in range(count) if around or 0 <= i + steps < count]
    return lax.ppermute(value, axis, pairs)


def shared(rows):
    rows = lax.all_to_all(rows, ("gx", "gy"), 0, 0)
    return rows.reshape(rows.shape[0], LANES)


QUARTERS = {"a": (2, 0, 3, 1), "b": (1, 3, 0, 2)}


def fetched(value, kind):
    quarter = lax.axis_size("gx") // 4
    pairs = [
        (source * quarter + i, target * quarter + i)
        for source, target in enumerate(QUARTERS[kind])
        for i in range(quarter)
    ]
    return lax.ppermute(value, "gx", pairs)


def from_outer():
    place, count = lax.axis_index("gx"), lax.axis_size("gx")
    return (place >= count // 4) & (place < count - count // 4)


def runs(levels):
    return levels // 2, levels - levels // 2


def body(
    temp_adjoint,
    height_adjoint,
    east_velocity,
    north_velocity,
    temp_store,
    salt_store,
    slot_map,
    land_mask,
    ocean_depth,
):
    levels, rows, columns = temp_adjoint.shape
    half_cycle = lax.axis_size("gx") // 2
    devices = lax.axis_size("gx") * lax.axis_size("gy")
    strip = 3 * RING + levels
    full = (rows + 2 * RING, columns + LANES)

    salt_sizes = runs(levels)
    slots = shifted(slot_map, "gx", half_cycle, True).reshape(-1)
    warm_a, warm_b = (fetched(temp_store, kind) for kind in QUARTERS)
    salt_b = fetched(salt_store, "b")

    swap = lax.axis_size("gy") == 2
    fields, *messages = call(
        functools.partial(pack_y_kernel, levels),
        [(3, rows, columns)] + [(strip, columns)] * (1 if swap else 2),
        stored(height_adjoint, land_mask, ocean_depth, temp_adjoint, north_velocity),
    )
    if swap:
        arrived = [shifted(messages[0], "gy", 1, True)]
    else:
        arrived = [shifted(messages[0], "gy", 1, False)]
        arrived += [shifted(messages[1], "gy", -1, False)]
    from_south, from_north, to_east, to_west = call(
        functools.partial(pack_x_kernel, levels, len(arrived)),
        [(strip, columns)] * 2 + [(strip, rows + LANES)] * 2,
        held(fields) + stored(land_mask, temp_adjoint, east_velocity) + held(*arrived),
    )
    from_west = shifted(to_east, "gx", 1, True)
    from_east = shifted(to_west, "gx", -1, True)
    (tracer,) = call(
        functools.partial(tracer_kernel, levels),
        [temp_adjoint.shape],
        stored(temp_adjoint, east_velocity, north_velocity, land_mask)
        + held(from_south, from_north),
        keep=[False],
    )
    cuts, start = [], 0
    for size in salt_sizes:
        cuts.append(lax.slice_in_dim(salt_store, start, start + size))
        start += size
    salt_parts = [fetched(cut, "a") for cut in cuts]
    beside = held(from_south, from_north, from_west, from_east)
    basis, tile_rows = call(krylov_kernel, [(ITERS + 2,) + full, (devices, 1, LANES)], held(fields) + beside)
    gathered = shared(tile_rows)
    surface, pressure = call(solve_kernel, [(rows, columns)] * 2, held(gathered, basis), keep=[False, True])
    partial, salt_back = call(
        functools.partial(warm_kernel, levels),
        [temp_adjoint.shape] * 2,
        free(slots) + stored(tracer) + held(pressure, from_west, from_east) + free(land_mask, warm_a, warm_b),
        specs=[SMEM] + [VMEM] * 7,
        keep=[True, False],
    )
    temp_back, first = None, 0
    for size, part in zip(salt_sizes, salt_parts):
        args = (slots, partial, pressure, land_mask, salt_b, part)
        temp_back = finish(levels, first, args, temp_back)
        first += size
    return (temp_back, salt_back, surface)


def solution(mesh):
    return jax.shard_map(
        body,
        mesh=mesh,
        in_specs=(
            P(None, "gy", "gx"),
            P("gy", "gx"),
            P(None, "gy", "gx"),
            P(None, "gy", "gx"),
            P(None, "gy", "gx"),
            P(None, "gy", "gx"),
            P("gx", "gy", None),
            P(None, "gy", "gx"),
            P("gy", "gx"),
        ),
        out_specs=(P(None, "gy", "gx"), P(None, "gy", "gx"), P("gy", "gx")),
        check_vma=False,
    )
```

```python
import functools

import jax
import jax.numpy as jnp
from jax import lax
from jax.experimental import pallas as pl
from jax.experimental.pallas import tpu as pltpu
from jax.sharding import PartitionSpec as P


ITERS = 6
RING = 8
KERNEL_VMEM = 16 * 1024 * 1024
LANES = 128

DIFFUSE = 0.2
TIMESTEP = 1.0
STIFFNESS = 8.0
GRAVITY = 4.0
THERMAL = 0.5
NONLINEAR = 0.4
CABBELING = 0.3
HALINE = 0.8


VMEM = pl.BlockSpec(memory_space=pltpu.VMEM)
SMEM = pl.BlockSpec(memory_space=pltpu.SMEM)
HBM = pl.BlockSpec(memory_space=pltpu.HBM)

PAIRS = [(i, j) for i in range(ITERS + 1) for j in range(i, ITERS + 1)]
MIDDLE_AT, LINK_AT, BACK_AT, WEIGHT_AT = 32, 40, 48, 56


def call(kernel, outs, args, specs=None, keep=None, flops=4000000):
    specs = specs or [VMEM] * len(args)
    keep = keep or [True] * len(outs)
    args = [
        arg if space is None else pltpu.with_memory_space_constraint(arg, space) for arg, space in args
    ]
    shapes = [
        pltpu.VMEM(shape, jnp.float32) if kept else jax.ShapeDtypeStruct(shape, jnp.float32)
        for shape, kept in zip(outs, keep)
    ]
    return pl.pallas_call(
        kernel,
        out_shape=shapes,
        in_specs=specs,
        out_specs=[VMEM] * len(outs),
        compiler_params=pltpu.CompilerParams(vmem_limit_bytes=KERNEL_VMEM),
        cost_estimate=pl.CostEstimate(flops=flops, bytes_accessed=1000000, transcendentals=0),
    )(*args)


def held(*arrays):
    return tuple((array, pltpu.VMEM) for array in arrays)


def stored(*arrays):
    return tuple((array, pltpu.HBM) for array in arrays)


def free(*arrays):
    return tuple((array, None) for array in arrays)


def total(value):
    return jnp.sum(jnp.sum(value, axis=0, keepdims=True), axis=1, keepdims=True)


def lane_index(shape):
    return lax.broadcasted_iota(jnp.int32, shape, 1)


def pack_y_kernel(levels, height, mask, depth, temp, north, fields, *messages):
    wet = mask[0].astype(jnp.float32)
    fields[0] = wet * height[...]
    fields[1] = wet
    fields[2] = depth[...]
    first, last = slice(0, RING), slice(temp.shape[1] - RING, temp.shape[1])

    def send(span, to_north, to_south):
        if len(messages) == 1:
            messages[0][span, :] = jnp.where(lax.axis_index("gy") == 0, to_north, to_south)
        else:
            messages[0][span, :] = to_north
            messages[1][span, :] = to_south

    for at in range(3):
        field = fields[at]
        send(slice(at * RING, (at + 1) * RING), field[last], field[first])
    base = 3 * RING
    for level in range(levels):
        flux_south = (DIFFUSE + 0.5 * north[level, first]) * (
            mask[level, first].astype(jnp.float32) * temp[level, first]
        )
        flux_north = (DIFFUSE - 0.5 * north[level, last]) * (
            mask[level, last].astype(jnp.float32) * temp[level, last]
        )
        send(slice(base + level, base + level + 1), flux_north[-1:], flux_south[:1])


def pack_t_kernel(levels, mask, temp, east, to_east, to_west):
    for level in range(levels):
        at = slice(level, level + 1)
        masked = mask[level].astype(jnp.float32) * temp[level]
        flux_east = (DIFFUSE - 0.5 * east[level]) * masked
        flux_west = (DIFFUSE + 0.5 * east[level]) * masked
        to_east[at, :] = jnp.transpose(flux_east[:, -LANES:])[-1:]
        to_west[at, :] = jnp.transpose(flux_west[:, :LANES])[:1]


def pack_x_kernel(levels, received, fields, tracer_east, tracer_west, *refs):
    arrived, (from_south, from_north, to_east, to_west) = refs[:received], refs[received:]
    if received == 1:
        lower = lax.axis_index("gy") == 0
        from_south[...] = jnp.where(lower, 0.0, arrived[0][...])
        from_north[...] = jnp.where(lower, arrived[0][...], 0.0)
    else:
        from_south[...] = arrived[0][...]
        from_north[...] = arrived[1][...]
    rows = fields.shape[1]
    for at in range(3):
        span = slice(at * RING, (at + 1) * RING)
        beside = [from_north[span, :], from_south[span, :]]
        beside.append(jnp.zeros((LANES - 2 * RING, fields.shape[2]), jnp.float32))
        flipped = jnp.transpose(jnp.concatenate([fields[at]] + beside, axis=0))
        to_west[span, :] = flipped[:RING]
        to_east[span, :] = flipped[-RING:]
    span = slice(3 * RING, 3 * RING + levels)
    to_east[span, :rows] = tracer_east[...]
    to_west[span, :rows] = tracer_west[...]
    to_east[span, rows:] = jnp.zeros((levels, LANES), jnp.float32)
    to_west[span, rows:] = jnp.zeros((levels, LANES), jnp.float32)


def beside_tile(from_west, from_east, start, size):
    span = slice(start, start + size)
    middle = jnp.zeros((LANES - 2 * size, from_west.shape[1]), jnp.float32)
    return jnp.transpose(jnp.concatenate([from_east[span, :], middle, from_west[span, :]], axis=0))


def krylov_kernel(fields, from_south, from_north, from_west, from_east, basis, row_out):
    rows, columns = fields.shape[1:]
    full_rows, full_columns = rows + 2 * RING, columns + LANES

    def widened(at):
        span = slice(at * RING, (at + 1) * RING)
        tile = jnp.concatenate([fields[at], from_north[span, :], from_south[span, :]], axis=0)
        side = beside_tile(from_west, from_east, at * RING, RING)
        return jnp.concatenate([tile, side[:full_rows]], axis=1)

    field, opening, deep = widened(0), widened(1), widened(2)
    basis[ITERS] = opening
    basis[ITERS + 1] = deep
    west_weight = STIFFNESS * 0.5 * (deep + pltpu.roll(deep, 1, 1)) * opening * pltpu.roll(opening, 1, 1)
    east_weight = pltpu.roll(west_weight, full_columns - 1, 1)
    south_weight = STIFFNESS * 0.5 * (deep + pltpu.roll(deep, 1, 0)) * opening * pltpu.roll(opening, 1, 0)
    north_weight = pltpu.roll(south_weight, full_rows - 1, 0)

    def spread(value):
        out = west_weight * (value - pltpu.roll(value, 1, 1))
        out = out + east_weight * (value - pltpu.roll(value, full_columns - 1, 1))
        out = out + south_weight * (value - pltpu.roll(value, 1, 0))
        return out + north_weight * (value - pltpu.roll(value, full_rows - 1, 0))

    at = lane_index((1, LANES))
    square = total(field * field)
    row = jnp.where(at == WEIGHT_AT, jnp.sqrt(square), 0.0)
    value = field * jnp.where(square > 0.0, lax.rsqrt(jnp.maximum(square, 1e-30)), 0.0)
    running = jnp.where(square > 0.0, 1.0, 0.0)
    before, back = jnp.zeros_like(value), jnp.zeros_like(square)
    vectors = [value]
    basis[0] = value
    for step in range(ITERS):
        image = spread(value) - back * before
        along, size = total(image * value), total(image * image)
        middle, link, scale, alive = next_step(along, size, running)
        for start, entry in ((MIDDLE_AT, middle), (LINK_AT, link), (BACK_AT, back)):
            row = jnp.where(at == start + step, entry, row)
        before, value = value, (image - middle * value) * scale
        running, back = alive, link * alive
        vectors.append(value)
        if step + 1 < ITERS:
            basis[step + 1] = value
    cut = [vector[:rows, :columns] for vector in vectors]
    partial = [jnp.sum(cut[i] * cut[j], axis=0, keepdims=True) for i, j in PAIRS]
    partial = [sum(part[:, k : k + LANES] for k in range(0, columns, LANES)) for part in partial]
    partial = partial + [jnp.zeros((LANES - len(partial), LANES), jnp.float32)]
    table = jnp.transpose(jnp.concatenate(partial, axis=0))
    row = row + jnp.sum(table, axis=0, keepdims=True)
    row_out[...] = jnp.broadcast_to(row[None], row_out.shape)


def next_step(along, size, running):
    left = size - along * along
    alive = jnp.where((left > 1e-6 * size) & (running > 0.0), 1.0, 0.0)
    safe = jnp.maximum(left, 1e-30)
    middle = jnp.where(running > 0.0, along, 4.0 * STIFFNESS)
    link = jnp.where(alive > 0.0, jnp.sqrt(safe), 2.0 * STIFFNESS)
    scale = jnp.where(alive > 0.0, lax.rsqrt(safe), 1.0 / (2.0 * STIFFNESS))
    return middle, link, scale, alive


def merged_recurrence(tiles):
    at = lane_index(tiles.shape)
    diagonal = jnp.where(at < ITERS, pltpu.roll(tiles, LANES - MIDDLE_AT, 1), 0.0)
    above = jnp.where(at < ITERS - 1, pltpu.roll(tiles, LANES - BACK_AT - 1, 1), 0.0)
    below = pltpu.roll(above, 1, 1)
    vector = jnp.where(at == 0, pltpu.roll(tiles, LANES - WEIGHT_AT, 1), 0.0)
    square = total(vector * vector)
    vector = vector * jnp.where(square > 0.0, lax.rsqrt(jnp.maximum(square, 1e-30)), 0.0)
    before, back = jnp.zeros_like(vector), jnp.zeros_like(square)
    running = jnp.ones_like(square)
    steps = []
    for _ in range(ITERS):
        image = diagonal * vector - back * before
        image = image + above * pltpu.roll(vector, LANES - 1, 1) + below * pltpu.roll(vector, 1, 1)
        along, size = total(image * vector), total(image * image)
        middle, link, scale, alive = next_step(along, size, running)
        steps.append((middle, link, scale, back))
        before, vector = vector, (image - along * vector) * (scale * alive)
        running, back = alive, link * alive
    return steps


def solve_kernel(gathered, basis, surface, pressure):
    rows, columns = surface.shape
    place = lax.axis_index("gx") * lax.axis_size("gy") + lax.axis_index("gy")
    tiles = gathered[...]
    steps = merged_recurrence(tiles)
    spare = -tiles.shape[0] % LANES
    if spare:
        tiles = jnp.concatenate([tiles, jnp.zeros((spare, LANES), jnp.float32)], axis=0)
    table = jnp.transpose(tiles)

    def known(index):
        return table[index : index + 1, :]

    products = {}
    for index, (i, j) in enumerate(PAIRS):
        products[i, j] = products[j, i] = known(index)
    change = [[known(WEIGHT_AT)]]
    for step, (middle, _, scale, back) in enumerate(steps):
        last = change[step]
        out = [None] * (step + 2)

        def add(at, term):
            out[at] = term if out[at] is None else out[at] + term

        for j, part in enumerate(last):
            add(j, (known(MIDDLE_AT + j) - middle) * part)
            add(j + 1, known(LINK_AT + j) * part)
            if j:
                add(j - 1, known(BACK_AT + j) * part)
        if step:
            for j, part in enumerate(change[step - 1]):
                add(j, -back * part)
        change.append([scale * term for term in out])
    gram = {}
    for k in range(ITERS + 1):
        half = [
            sum(change[k][i] * products[i, j] for i in range(k + 1)) for j in range(ITERS + 1)
        ]
        for m in range(k, ITERS + 1):
            both = sum(half[j] * change[m][j] for j in range(m + 1))
            gram[k, m] = gram[m, k] = jnp.sum(both, axis=1, keepdims=True)
    zero = jnp.zeros((1, 1), jnp.float32)

    def applied(vector):
        out = [zero] * (len(vector) + 1)
        for i, part in enumerate(vector):
            middle, link, _, back = steps[i]
            out[i] = out[i] + part + middle * part
            out[i + 1] = out[i + 1] + link * part
            if i:
                out[i - 1] = out[i - 1] + back * part
        return out

    def inner(left, right):
        out = zero
        for i, a in enumerate(left):
            part = zero
            for j, b in enumerate(right):
                part = part + gram[i, j] * b
            out = out + a * part
        return out

    def scaled_add(left, scale, right):
        size = max(len(left), len(right))
        left = left + [zero] * (size - len(left))
        right = right + [zero] * (size - len(right))
        return [a + scale * b for a, b in zip(left, right)]

    residual = direction = [jnp.ones((1, 1), jnp.float32)]
    iterate = [zero]
    norm_now = gram[0, 0]
    for iteration in range(ITERS):
        image = applied(direction)
        product = inner(direction, image)
        step_size = jnp.where(product > 0.0, norm_now / product, 0.0)
        iterate = scaled_add(iterate, step_size, direction)
        if iteration + 1 < ITERS:
            residual = scaled_add(residual, -step_size, image)
            norm_next = inner(residual, residual)
            growth = jnp.where(norm_now > 0.0, norm_next / norm_now, 0.0)
            direction = scaled_add(residual, growth, direction)
            norm_now = norm_next
    mine = lane_index((1, table.shape[1])) == place
    value = None
    for j in range(ITERS):
        weight = sum(iterate[k] * change[k][j] for k in range(j, ITERS))
        weight = jnp.sum(jnp.where(mine, weight, 0.0), axis=1, keepdims=True)
        value = weight * basis[j] if value is None else value + weight * basis[j]
    surface[...] = value[:rows, :columns]
    opening = basis[ITERS]
    load = basis[ITERS + 1] * value
    full_rows, full_columns = value.shape
    pull = jnp.zeros_like(load)
    for shift, axis in ((1, 1), (full_columns - 1, 1), (1, 0), (full_rows - 1, 0)):
        pull = pull + opening * pltpu.roll(opening, shift, axis) * (pltpu.roll(load, shift, axis) - load)
    pressure[...] = -GRAVITY * pull[:rows, :columns]


def tracer_kernel(levels, temp, east, north, mask, from_south, from_north, tracer):
    rows, columns = temp.shape[1:]
    row = lax.broadcasted_iota(jnp.int32, (rows, columns), 0)
    lane = lane_index((rows, columns))
    base = 3 * RING
    for level in range(levels):
        masked = mask[level].astype(jnp.float32) * temp[level]
        east_coef = DIFFUSE - 0.5 * east[level]
        west_coef = DIFFUSE + 0.5 * east[level]
        north_coef = DIFFUSE - 0.5 * north[level]
        south_coef = DIFFUSE + 0.5 * north[level]
        side_south = from_south[base + level : base + level + 1, :]
        side_north = from_north[base + level : base + level + 1, :]
        inflow = jnp.where(lane == 0, 0.0, pltpu.roll(east_coef * masked, 1, 1))
        inflow = inflow + jnp.where(
            lane == columns - 1, 0.0, pltpu.roll(west_coef * masked, columns - 1, 1)
        )
        inflow = inflow + jnp.where(row == 0, side_south, pltpu.roll(north_coef * masked, 1, 0))
        inflow = inflow + jnp.where(
            row == rows - 1, side_north, pltpu.roll(south_coef * masked, rows - 1, 0)
        )
        tracer[level] = masked + TIMESTEP * (
            inflow - (east_coef + west_coef + north_coef + south_coef) * masked
        )


def level_of_slot(slots, slot, levels):
    level = jnp.int32(0)
    for k in range(1, levels):
        level = jnp.where(slots[k] == slot, jnp.int32(k), level)
    return level


def density(level, levels, pressure, mask):
    thickness = 1.0 + level.astype(jnp.float32) / levels
    return thickness * pressure[...] * mask[level].astype(jnp.float32)


def warm_kernel(levels, slots, tracer, pressure, from_west, from_east, mask, outer, inner, partial, salt):
    rows, columns = pressure.shape
    lane = lane_index((rows, columns))
    sides = beside_tile(from_west, from_east, 3 * RING, levels)[:rows]
    for level in range(levels):
        side_west = sides[:, LANES - levels + level : LANES - levels + level + 1]
        side_east = sides[:, level : level + 1]
        edge = jnp.where(lane == 0, side_west, 0.0) + jnp.where(lane == columns - 1, side_east, 0.0)
        partial[level] = tracer[level] + TIMESTEP * edge
    for slot in range(levels):
        level = level_of_slot(slots, slot, levels)
        dense = density(level, levels, pressure, mask)
        value = jnp.where(from_outer(), outer[slot], inner[slot])
        salt[level] = (HALINE + CABBELING * value) * dense
        partial[level] = partial[level] + (THERMAL + 2.0 * NONLINEAR * value) * dense


def salt_kernel(levels, first, slots, partial, pressure, mask, inner, part, *refs):
    result, done, sems = refs[-3:]

    def finished(values, start):
        copies = []
        for at in range(values.shape[0]):
            level = level_of_slot(slots, start + at, levels)
            dense = density(level, levels, pressure, mask)
            done[at] = partial[level] + CABBELING * values[at] * dense
            copies.append(pltpu.make_async_copy(done.at[at], result.at[level], sems.at[at]))
            copies[-1].start()
        for copy in copies:
            copy.wait()

    @pl.when(from_outer())
    def _():
        finished(part, first)

    if first == 0:

        @pl.when(jnp.logical_not(from_outer()))
        def _():
            finished(inner, 0)


def finish(levels, first, args, before):
    part = args[-1]
    shape = (levels,) + part.shape[1:]
    held_args = [pltpu.with_memory_space_constraint(arg, pltpu.VMEM) for arg in args[1:]]
    operands = [args[0]] + held_args + ([] if before is None else [before])
    return pl.pallas_call(
        functools.partial(salt_kernel, levels, first),
        out_shape=jax.ShapeDtypeStruct(shape, jnp.float32),
        in_specs=[SMEM] + [VMEM] * len(held_args) + ([] if before is None else [HBM]),
        out_specs=HBM,
        scratch_shapes=[
            pltpu.VMEM(shape, jnp.float32),
            pltpu.SemaphoreType.DMA((levels,)),
        ],
        input_output_aliases={} if before is None else {len(operands) - 1: 0},
        compiler_params=pltpu.CompilerParams(vmem_limit_bytes=KERNEL_VMEM),
        cost_estimate=pl.CostEstimate(flops=1000000, bytes_accessed=1000000, transcendentals=0),
    )(*operands)


def shifted(value, axis, steps, around):
    count = lax.axis_size(axis)
    pairs = [(i, (i + steps) % count) for i in range(count) if around or 0 <= i + steps < count]
    return lax.ppermute(value, axis, pairs)


def shared(rows):
    rows = lax.all_to_all(rows, ("gx", "gy"), 0, 0)
    return rows.reshape(rows.shape[0], LANES)


QUARTERS = {"a": (2, 0, 3, 1), "b": (1, 3, 0, 2)}


def fetched(value, kind):
    quarter = lax.axis_size("gx") // 4
    pairs = [
        (source * quarter + i, target * quarter + i)
        for source, target in enumerate(QUARTERS[kind])
        for i in range(quarter)
    ]
    return lax.ppermute(value, "gx", pairs)


def from_outer():
    place, count = lax.axis_index("gx"), lax.axis_size("gx")
    return (place >= count // 4) & (place < count - count // 4)


def runs(levels):
    most = 5 * levels // 8
    return most, levels - most


def body(
    temp_adjoint,
    height_adjoint,
    east_velocity,
    north_velocity,
    temp_store,
    salt_store,
    slot_map,
    land_mask,
    ocean_depth,
):
    levels, rows, columns = temp_adjoint.shape
    half_cycle = lax.axis_size("gx") // 2
    devices = lax.axis_size("gx") * lax.axis_size("gy")
    strip = 3 * RING + levels
    full = (rows + 2 * RING, columns + LANES)

    salt_sizes = runs(levels)
    slots = shifted(slot_map, "gx", half_cycle, True).reshape(-1)
    warm_a, warm_b = (fetched(temp_store, kind) for kind in QUARTERS)
    salt_b = fetched(salt_store, "b")

    swap = lax.axis_size("gy") == 2
    fields, *messages = call(
        functools.partial(pack_y_kernel, levels),
        [(3, rows, columns)] + [(strip, columns)] * (1 if swap else 2),
        stored(height_adjoint, land_mask, ocean_depth, temp_adjoint, north_velocity),
    )
    if swap:
        arrived = [shifted(messages[0], "gy", 1, True)]
    else:
        arrived = [shifted(messages[0], "gy", 1, False)]
        arrived += [shifted(messages[1], "gy", -1, False)]
    tracer_east, tracer_west = call(
        functools.partial(pack_t_kernel, levels), [(levels, rows)] * 2, stored(land_mask, temp_adjoint, east_velocity)
    )
    from_south, from_north, to_east, to_west = call(
        functools.partial(pack_x_kernel, levels, len(arrived)),
        [(strip, columns)] * 2 + [(strip, rows + LANES)] * 2,
        held(fields, tracer_east, tracer_west, *arrived),
    )
    from_west = shifted(to_east, "gx", 1, True)
    from_east = shifted(to_west, "gx", -1, True)
    (tracer,) = call(
        functools.partial(tracer_kernel, levels),
        [temp_adjoint.shape],
        stored(temp_adjoint, east_velocity, north_velocity, land_mask)
        + held(from_south, from_north),
        keep=[False],
    )
    cuts, start = [], 0
    for size in salt_sizes:
        cuts.append(lax.slice_in_dim(salt_store, start, start + size))
        start += size
    salt_parts = [fetched(cut, "a") for cut in cuts]
    beside = held(from_south, from_north, from_west, from_east)
    basis, tile_rows = call(krylov_kernel, [(ITERS + 2,) + full, (devices, 1, LANES)], held(fields) + beside)
    gathered = shared(tile_rows)
    surface, pressure = call(solve_kernel, [(rows, columns)] * 2, held(gathered, basis), keep=[False, True])
    partial, salt_back = call(
        functools.partial(warm_kernel, levels),
        [temp_adjoint.shape] * 2,
        free(slots) + stored(tracer) + held(pressure, from_west, from_east) + free(land_mask, warm_a, warm_b),
        specs=[SMEM] + [VMEM] * 7,
        keep=[True, False],
    )
    temp_back, first = None, 0
    for size, part in zip(salt_sizes, salt_parts):
        args = (slots, partial, pressure, land_mask, salt_b, part)
        temp_back = finish(levels, first, args, temp_back)
        first += size
    return (temp_back, salt_back, surface)


def solution(mesh):
    return jax.shard_map(
        body,
        mesh=mesh,
        in_specs=(
            P(None, "gy", "gx"),
            P("gy", "gx"),
            P(None, "gy", "gx"),
            P(None, "gy", "gx"),
            P(None, "gy", "gx"),
            P(None, "gy", "gx"),
            P("gx", "gy", None),
            P(None, "gy", "gx"),
            P("gy", "gx"),
        ),
        out_specs=(P(None, "gy", "gx"), P(None, "gy", "gx"), P("gy", "gx")),
        check_vma=False,
    )
```

```python
import functools

import jax
import jax.numpy as jnp
from jax import lax
from jax.experimental import pallas as pl
from jax.experimental.pallas import tpu as pltpu
from jax.sharding import PartitionSpec as P


ITERS = 6
RING = 8
KERNEL_VMEM = 16 * 1024 * 1024
LANES = 128

DIFFUSE = 0.2
TIMESTEP = 1.0
STIFFNESS = 8.0
GRAVITY = 4.0
THERMAL = 0.5
NONLINEAR = 0.4
CABBELING = 0.3
HALINE = 0.8


VMEM = pl.BlockSpec(memory_space=pltpu.VMEM)
SMEM = pl.BlockSpec(memory_space=pltpu.SMEM)
HBM = pl.BlockSpec(memory_space=pltpu.HBM)

PAIRS = [(i, j) for i in range(ITERS + 1) for j in range(i, ITERS + 1)]
MIDDLE_AT, LINK_AT, BACK_AT, WEIGHT_AT = 32, 40, 48, 56


def call(kernel, outs, args, specs=None, keep=None, flops=4000000):
    specs = specs or [VMEM] * len(args)
    keep = keep or [True] * len(outs)
    args = [
        arg if space is None else pltpu.with_memory_space_constraint(arg, space) for arg, space in args
    ]
    shapes = [
        pltpu.VMEM(shape, jnp.float32) if kept else jax.ShapeDtypeStruct(shape, jnp.float32)
        for shape, kept in zip(outs, keep)
    ]
    return pl.pallas_call(
        kernel,
        out_shape=shapes,
        in_specs=specs,
        out_specs=[VMEM] * len(outs),
        compiler_params=pltpu.CompilerParams(vmem_limit_bytes=KERNEL_VMEM),
        cost_estimate=pl.CostEstimate(flops=flops, bytes_accessed=1000000, transcendentals=0),
    )(*args)


def held(*arrays):
    return tuple((array, pltpu.VMEM) for array in arrays)


def stored(*arrays):
    return tuple((array, pltpu.HBM) for array in arrays)


def free(*arrays):
    return tuple((array, None) for array in arrays)


def total(value):
    return jnp.sum(jnp.sum(value, axis=0, keepdims=True), axis=1, keepdims=True)


def lane_index(shape):
    return lax.broadcasted_iota(jnp.int32, shape, 1)


def pack_y_kernel(levels, height, mask, depth, temp, north, fields, *messages):
    wet = mask[0].astype(jnp.float32)
    fields[0] = wet * height[...]
    fields[1] = wet
    fields[2] = depth[...]
    first, last = slice(0, RING), slice(temp.shape[1] - RING, temp.shape[1])

    def send(span, to_north, to_south):
        if len(messages) == 1:
            messages[0][span, :] = jnp.where(lax.axis_index("gy") == 0, to_north, to_south)
        else:
            messages[0][span, :] = to_north
            messages[1][span, :] = to_south

    for at in range(3):
        field = fields[at]
        send(slice(at * RING, (at + 1) * RING), field[last], field[first])
    base = 3 * RING
    for level in range(levels):
        flux_south = (DIFFUSE + 0.5 * north[level, first]) * (
            mask[level, first].astype(jnp.float32) * temp[level, first]
        )
        flux_north = (DIFFUSE - 0.5 * north[level, last]) * (
            mask[level, last].astype(jnp.float32) * temp[level, last]
        )
        send(slice(base + level, base + level + 1), flux_north[-1:], flux_south[:1])


def pack_t_kernel(levels, mask, temp, east, to_east, to_west):
    for level in range(levels):
        at = slice(level, level + 1)
        masked = mask[level].astype(jnp.float32) * temp[level]
        flux_east = (DIFFUSE - 0.5 * east[level]) * masked
        flux_west = (DIFFUSE + 0.5 * east[level]) * masked
        to_east[at, :] = jnp.transpose(flux_east[:, -LANES:])[-1:]
        to_west[at, :] = jnp.transpose(flux_west[:, :LANES])[:1]


def pack_x_kernel(levels, received, fields, tracer_east, tracer_west, *refs):
    arrived, (from_south, from_north, to_east, to_west) = refs[:received], refs[received:]
    if received == 1:
        lower = lax.axis_index("gy") == 0
        from_south[...] = jnp.where(lower, 0.0, arrived[0][...])
        from_north[...] = jnp.where(lower, arrived[0][...], 0.0)
    else:
        from_south[...] = arrived[0][...]
        from_north[...] = arrived[1][...]
    rows = fields.shape[1]
    for at in range(3):
        span = slice(at * RING, (at + 1) * RING)
        beside = [from_north[span, :], from_south[span, :]]
        beside.append(jnp.zeros((LANES - 2 * RING, fields.shape[2]), jnp.float32))
        flipped = jnp.transpose(jnp.concatenate([fields[at]] + beside, axis=0))
        to_west[span, :] = flipped[:RING]
        to_east[span, :] = flipped[-RING:]
    span = slice(3 * RING, 3 * RING + levels)
    to_east[span, :rows] = tracer_east[...]
    to_west[span, :rows] = tracer_west[...]
    to_east[span, rows:] = jnp.zeros((levels, LANES), jnp.float32)
    to_west[span, rows:] = jnp.zeros((levels, LANES), jnp.float32)


def beside_tile(from_west, from_east, start, size):
    span = slice(start, start + size)
    middle = jnp.zeros((LANES - 2 * size, from_west.shape[1]), jnp.float32)
    return jnp.transpose(jnp.concatenate([from_east[span, :], middle, from_west[span, :]], axis=0))


def krylov_kernel(fields, from_south, from_north, from_west, from_east, basis, row_out):
    rows, columns = fields.shape[1:]
    full_rows, full_columns = rows + 2 * RING, columns + LANES

    def widened(at):
        span = slice(at * RING, (at + 1) * RING)
        tile = jnp.concatenate([fields[at], from_north[span, :], from_south[span, :]], axis=0)
        side = beside_tile(from_west, from_east, at * RING, RING)
        return jnp.concatenate([tile, side[:full_rows]], axis=1)

    field, opening, deep = widened(0), widened(1), widened(2)
    basis[ITERS] = opening
    basis[ITERS + 1] = deep
    west_weight = STIFFNESS * 0.5 * (deep + pltpu.roll(deep, 1, 1)) * opening * pltpu.roll(opening, 1, 1)
    east_weight = pltpu.roll(west_weight, full_columns - 1, 1)
    south_weight = STIFFNESS * 0.5 * (deep + pltpu.roll(deep, 1, 0)) * opening * pltpu.roll(opening, 1, 0)
    north_weight = pltpu.roll(south_weight, full_rows - 1, 0)

    def spread(value):
        out = west_weight * (value - pltpu.roll(value, 1, 1))
        out = out + east_weight * (value - pltpu.roll(value, full_columns - 1, 1))
        out = out + south_weight * (value - pltpu.roll(value, 1, 0))
        return out + north_weight * (value - pltpu.roll(value, full_rows - 1, 0))

    at = lane_index((1, LANES))
    square = total(field * field)
    row = jnp.where(at == WEIGHT_AT, jnp.sqrt(square), 0.0)
    value = field * jnp.where(square > 0.0, lax.rsqrt(jnp.maximum(square, 1e-30)), 0.0)
    running = jnp.where(square > 0.0, 1.0, 0.0)
    before, back = jnp.zeros_like(value), jnp.zeros_like(square)
    vectors = [value]
    basis[0] = value
    for step in range(ITERS):
        image = spread(value) - back * before
        along, size = total(image * value), total(image * image)
        middle, link, scale, alive = next_step(along, size, running)
        for start, entry in ((MIDDLE_AT, middle), (LINK_AT, link), (BACK_AT, back)):
            row = jnp.where(at == start + step, entry, row)
        before, value = value, (image - middle * value) * scale
        running, back = alive, link * alive
        vectors.append(value)
        if step + 1 < ITERS:
            basis[step + 1] = value
    cut = [vector[:rows, :columns] for vector in vectors]
    partial = [jnp.sum(cut[i] * cut[j], axis=0, keepdims=True) for i, j in PAIRS]
    partial = [sum(part[:, k : k + LANES] for k in range(0, columns, LANES)) for part in partial]
    partial = partial + [jnp.zeros((LANES - len(partial), LANES), jnp.float32)]
    table = jnp.transpose(jnp.concatenate(partial, axis=0))
    row = row + jnp.sum(table, axis=0, keepdims=True)
    row_out[...] = jnp.broadcast_to(row[None], row_out.shape)


def next_step(along, size, running):
    left = size - along * along
    alive = jnp.where((left > 1e-6 * size) & (running > 0.0), 1.0, 0.0)
    safe = jnp.maximum(left, 1e-30)
    middle = jnp.where(running > 0.0, along, 4.0 * STIFFNESS)
    link = jnp.where(alive > 0.0, jnp.sqrt(safe), 2.0 * STIFFNESS)
    scale = jnp.where(alive > 0.0, lax.rsqrt(safe), 1.0 / (2.0 * STIFFNESS))
    return middle, link, scale, alive


def merged_recurrence(tiles):
    at = lane_index(tiles.shape)
    diagonal = jnp.where(at < ITERS, pltpu.roll(tiles, LANES - MIDDLE_AT, 1), 0.0)
    above = jnp.where(at < ITERS - 1, pltpu.roll(tiles, LANES - BACK_AT - 1, 1), 0.0)
    below = pltpu.roll(above, 1, 1)
    vector = jnp.where(at == 0, pltpu.roll(tiles, LANES - WEIGHT_AT, 1), 0.0)
    square = total(vector * vector)
    vector = vector * jnp.where(square > 0.0, lax.rsqrt(jnp.maximum(square, 1e-30)), 0.0)
    before, back = jnp.zeros_like(vector), jnp.zeros_like(square)
    running = jnp.ones_like(square)
    steps = []
    for _ in range(ITERS):
        image = diagonal * vector - back * before
        image = image + above * pltpu.roll(vector, LANES - 1, 1) + below * pltpu.roll(vector, 1, 1)
        along, size = total(image * vector), total(image * image)
        middle, link, scale, alive = next_step(along, size, running)
        steps.append((middle, link, scale, back))
        before, vector = vector, (image - along * vector) * (scale * alive)
        running, back = alive, link * alive
    return steps


def solve_kernel(gathered, basis, surface, pressure):
    rows, columns = surface.shape
    place = lax.axis_index("gx") * lax.axis_size("gy") + lax.axis_index("gy")
    tiles = gathered[...]
    steps = merged_recurrence(tiles)
    spare = -tiles.shape[0] % LANES
    if spare:
        tiles = jnp.concatenate([tiles, jnp.zeros((spare, LANES), jnp.float32)], axis=0)
    table = jnp.transpose(tiles)

    def known(index):
        return table[index : index + 1, :]

    products = {}
    for index, (i, j) in enumerate(PAIRS):
        products[i, j] = products[j, i] = known(index)
    change = [[known(WEIGHT_AT)]]
    for step, (middle, _, scale, back) in enumerate(steps):
        last = change[step]
        out = [None] * (step + 2)

        def add(at, term):
            out[at] = term if out[at] is None else out[at] + term

        for j, part in enumerate(last):
            add(j, (known(MIDDLE_AT + j) - middle) * part)
            add(j + 1, known(LINK_AT + j) * part)
            if j:
                add(j - 1, known(BACK_AT + j) * part)
        if step:
            for j, part in enumerate(change[step - 1]):
                add(j, -back * part)
        change.append([scale * term for term in out])
    gram = {}
    for k in range(ITERS + 1):
        half = [
            sum(change[k][i] * products[i, j] for i in range(k + 1)) for j in range(ITERS + 1)
        ]
        for m in range(k, ITERS + 1):
            both = sum(half[j] * change[m][j] for j in range(m + 1))
            gram[k, m] = gram[m, k] = jnp.sum(both, axis=1, keepdims=True)
    zero = jnp.zeros((1, 1), jnp.float32)

    def applied(vector):
        out = [zero] * (len(vector) + 1)
        for i, part in enumerate(vector):
            middle, link, _, back = steps[i]
            out[i] = out[i] + part + middle * part
            out[i + 1] = out[i + 1] + link * part
            if i:
                out[i - 1] = out[i - 1] + back * part
        return out

    def inner(left, right):
        out = zero
        for i, a in enumerate(left):
            part = zero
            for j, b in enumerate(right):
                part = part + gram[i, j] * b
            out = out + a * part
        return out

    def scaled_add(left, scale, right):
        size = max(len(left), len(right))
        left = left + [zero] * (size - len(left))
        right = right + [zero] * (size - len(right))
        return [a + scale * b for a, b in zip(left, right)]

    residual = direction = [jnp.ones((1, 1), jnp.float32)]
    iterate = [zero]
    norm_now = gram[0, 0]
    for iteration in range(ITERS):
        image = applied(direction)
        product = inner(direction, image)
        step_size = jnp.where(product > 0.0, norm_now / product, 0.0)
        iterate = scaled_add(iterate, step_size, direction)
        if iteration + 1 < ITERS:
            residual = scaled_add(residual, -step_size, image)
            norm_next = inner(residual, residual)
            growth = jnp.where(norm_now > 0.0, norm_next / norm_now, 0.0)
            direction = scaled_add(residual, growth, direction)
            norm_now = norm_next
    mine = lane_index((1, table.shape[1])) == place
    value = None
    for j in range(ITERS):
        weight = sum(iterate[k] * change[k][j] for k in range(j, ITERS))
        weight = jnp.sum(jnp.where(mine, weight, 0.0), axis=1, keepdims=True)
        value = weight * basis[j] if value is None else value + weight * basis[j]
    surface[...] = value[:rows, :columns]
    opening = basis[ITERS]
    load = basis[ITERS + 1] * value
    full_rows, full_columns = value.shape
    pull = jnp.zeros_like(load)
    for shift, axis in ((1, 1), (full_columns - 1, 1), (1, 0), (full_rows - 1, 0)):
        pull = pull + opening * pltpu.roll(opening, shift, axis) * (pltpu.roll(load, shift, axis) - load)
    pressure[...] = -GRAVITY * pull[:rows, :columns]


def tracer_kernel(levels, temp, east, north, mask, from_south, from_north, tracer):
    rows, columns = temp.shape[1:]
    row = lax.broadcasted_iota(jnp.int32, (rows, columns), 0)
    lane = lane_index((rows, columns))
    base = 3 * RING
    for level in range(levels):
        masked = mask[level].astype(jnp.float32) * temp[level]
        east_coef = DIFFUSE - 0.5 * east[level]
        west_coef = DIFFUSE + 0.5 * east[level]
        north_coef = DIFFUSE - 0.5 * north[level]
        south_coef = DIFFUSE + 0.5 * north[level]
        side_south = from_south[base + level : base + level + 1, :]
        side_north = from_north[base + level : base + level + 1, :]
        inflow = jnp.where(lane == 0, 0.0, pltpu.roll(east_coef * masked, 1, 1))
        inflow = inflow + jnp.where(
            lane == columns - 1, 0.0, pltpu.roll(west_coef * masked, columns - 1, 1)
        )
        inflow = inflow + jnp.where(row == 0, side_south, pltpu.roll(north_coef * masked, 1, 0))
        inflow = inflow + jnp.where(
            row == rows - 1, side_north, pltpu.roll(south_coef * masked, rows - 1, 0)
        )
        tracer[level] = masked + TIMESTEP * (
            inflow - (east_coef + west_coef + north_coef + south_coef) * masked
        )


def level_of_slot(slots, slot, levels):
    level = jnp.int32(0)
    for k in range(1, levels):
        level = jnp.where(slots[k] == slot, jnp.int32(k), level)
    return level


def density(level, levels, pressure, mask):
    thickness = 1.0 + level.astype(jnp.float32) / levels
    return thickness * pressure[...] * mask[level].astype(jnp.float32)


def warm_kernel(levels, slots, tracer, pressure, from_west, from_east, mask, outer, inner, partial, salt):
    rows, columns = pressure.shape
    lane = lane_index((rows, columns))
    sides = beside_tile(from_west, from_east, 3 * RING, levels)[:rows]
    for level in range(levels):
        side_west = sides[:, LANES - levels + level : LANES - levels + level + 1]
        side_east = sides[:, level : level + 1]
        edge = jnp.where(lane == 0, side_west, 0.0) + jnp.where(lane == columns - 1, side_east, 0.0)
        partial[level] = tracer[level] + TIMESTEP * edge
    for slot in range(levels):
        level = level_of_slot(slots, slot, levels)
        dense = density(level, levels, pressure, mask)
        value = jnp.where(from_outer(), outer[slot], inner[slot])
        salt[level] = (HALINE + CABBELING * value) * dense
        partial[level] = partial[level] + (THERMAL + 2.0 * NONLINEAR * value) * dense


def sort_kernel(sizes, slots, store, *parts):
    level = 0
    for size, part in zip(sizes, parts):
        for at in range(size):
            part[at] = store[slots[level]]
            level += 1


def salt_kernel(levels, first, partial, pressure, mask, part, *refs):
    result, done, sems = refs[-3:]

    def finished(values, place):
        copies = []
        for at in range(values.shape[0]):
            level = place(at)
            dense = density(level, levels, pressure, mask)
            done[at] = partial[level] + CABBELING * values[at] * dense
            copies.append(pltpu.make_async_copy(done.at[at], result.at[level], sems.at[at]))
            copies[-1].start()
        for copy in copies:
            copy.wait()

    @pl.when(from_outer())
    def _():
        finished(part, lambda at: jnp.int32(first + at))

    if first == 0:
        inner, slots = refs[:2]

        @pl.when(jnp.logical_not(from_outer()))
        def _():
            finished(inner, lambda at: level_of_slot(slots, at, levels))


def finish(levels, first, args, whole, before):
    part = args[-1]
    shape = (levels,) + part.shape[1:]
    operands = [pltpu.with_memory_space_constraint(arg, pltpu.VMEM) for arg in args]
    specs = [VMEM] * len(operands)
    if first == 0:
        operands += [pltpu.with_memory_space_constraint(whole[0], pltpu.VMEM), whole[1]]
        specs += [VMEM, SMEM]
    else:
        operands.append(before)
        specs.append(HBM)
    return pl.pallas_call(
        functools.partial(salt_kernel, levels, first),
        out_shape=jax.ShapeDtypeStruct(shape, jnp.float32),
        in_specs=specs,
        out_specs=HBM,
        scratch_shapes=[
            pltpu.VMEM(shape, jnp.float32),
            pltpu.SemaphoreType.DMA((levels,)),
        ],
        input_output_aliases={len(operands) - 1: 0} if first else {},
        compiler_params=pltpu.CompilerParams(vmem_limit_bytes=KERNEL_VMEM),
        cost_estimate=pl.CostEstimate(flops=1000000, bytes_accessed=1000000, transcendentals=0),
    )(*operands)


def shifted(value, axis, steps, around):
    count = lax.axis_size(axis)
    pairs = [(i, (i + steps) % count) for i in range(count) if around or 0 <= i + steps < count]
    return lax.ppermute(value, axis, pairs)


def shared(rows):
    rows = lax.all_to_all(rows, ("gx", "gy"), 0, 0)
    return rows.reshape(rows.shape[0], LANES)


QUARTERS = {"a": (2, 0, 3, 1), "b": (1, 3, 0, 2)}


def fetched(value, kind):
    quarter = lax.axis_size("gx") // 4
    pairs = [
        (source * quarter + i, target * quarter + i)
        for source, target in enumerate(QUARTERS[kind])
        for i in range(quarter)
    ]
    return lax.ppermute(value, "gx", pairs)


def from_outer():
    place, count = lax.axis_index("gx"), lax.axis_size("gx")
    return (place >= count // 4) & (place < count - count // 4)


def runs(levels):
    most = 5 * levels // 8
    return most, levels - most


def body(
    temp_adjoint,
    height_adjoint,
    east_velocity,
    north_velocity,
    temp_store,
    salt_store,
    slot_map,
    land_mask,
    ocean_depth,
):
    levels, rows, columns = temp_adjoint.shape
    half_cycle = lax.axis_size("gx") // 2
    devices = lax.axis_size("gx") * lax.axis_size("gy")
    strip = 3 * RING + levels
    full = (rows + 2 * RING, columns + LANES)

    salt_sizes = runs(levels)
    slots = shifted(slot_map, "gx", half_cycle, True).reshape(-1)
    warm_a, warm_b = (fetched(temp_store, kind) for kind in QUARTERS)
    salt_b = fetched(salt_store, "b")

    swap = lax.axis_size("gy") == 2
    fields, *messages = call(
        functools.partial(pack_y_kernel, levels),
        [(3, rows, columns)] + [(strip, columns)] * (1 if swap else 2),
        stored(height_adjoint, land_mask, ocean_depth, temp_adjoint, north_velocity),
    )
    if swap:
        arrived = [shifted(messages[0], "gy", 1, True)]
    else:
        arrived = [shifted(messages[0], "gy", 1, False)]
        arrived += [shifted(messages[1], "gy", -1, False)]
    tracer_east, tracer_west = call(
        functools.partial(pack_t_kernel, levels), [(levels, rows)] * 2, stored(land_mask, temp_adjoint, east_velocity)
    )
    from_south, from_north, to_east, to_west = call(
        functools.partial(pack_x_kernel, levels, len(arrived)),
        [(strip, columns)] * 2 + [(strip, rows + LANES)] * 2,
        held(fields, tracer_east, tracer_west, *arrived),
    )
    from_west = shifted(to_east, "gx", 1, True)
    from_east = shifted(to_west, "gx", -1, True)
    (tracer,) = call(
        functools.partial(tracer_kernel, levels),
        [temp_adjoint.shape],
        stored(temp_adjoint, east_velocity, north_velocity, land_mask)
        + held(from_south, from_north),
        keep=[False],
    )
    cuts = call(
        functools.partial(sort_kernel, salt_sizes),
        [(size, rows, columns) for size in salt_sizes],
        free(slot_map.reshape(-1)) + stored(salt_store),
        specs=[SMEM, VMEM],
        keep=[False] * len(salt_sizes),
    )
    salt_parts = [fetched(cut, "a") for cut in cuts]
    beside = held(from_south, from_north, from_west, from_east)
    basis, tile_rows = call(krylov_kernel, [(ITERS + 2,) + full, (devices, 1, LANES)], held(fields) + beside)
    gathered = shared(tile_rows)
    surface, pressure = call(solve_kernel, [(rows, columns)] * 2, held(gathered, basis), keep=[False, True])
    partial, salt_back = call(
        functools.partial(warm_kernel, levels),
        [temp_adjoint.shape] * 2,
        free(slots) + stored(tracer) + held(pressure, from_west, from_east) + free(land_mask, warm_a, warm_b),
        specs=[SMEM] + [VMEM] * 7,
        keep=[True, False],
    )
    temp_back, first = None, 0
    for size, part in zip(salt_sizes, salt_parts):
        args = (partial, pressure, land_mask, part)
        temp_back = finish(levels, first, args, (salt_b, slots), temp_back)
        first += size
    return (temp_back, salt_back, surface)


def solution(mesh):
    return jax.shard_map(
        body,
        mesh=mesh,
        in_specs=(
            P(None, "gy", "gx"),
            P("gy", "gx"),
            P(None, "gy", "gx"),
            P(None, "gy", "gx"),
            P(None, "gy", "gx"),
            P(None, "gy", "gx"),
            P("gx", "gy", None),
            P(None, "gy", "gx"),
            P("gy", "gx"),
        ),
        out_specs=(P(None, "gy", "gx"), P(None, "gy", "gx"), P("gy", "gx")),
        check_vma=False,
    )
```

```python
import functools

import jax
import jax.numpy as jnp
from jax import lax
from jax.experimental import pallas as pl
from jax.experimental.pallas import tpu as pltpu
from jax.sharding import PartitionSpec as P


ITERS = 6
RING = 8
KERNEL_VMEM = 16 * 1024 * 1024
LANES = 128

DIFFUSE = 0.2
TIMESTEP = 1.0
STIFFNESS = 8.0
GRAVITY = 4.0
THERMAL = 0.5
NONLINEAR = 0.4
CABBELING = 0.3
HALINE = 0.8


VMEM = pl.BlockSpec(memory_space=pltpu.VMEM)
SMEM = pl.BlockSpec(memory_space=pltpu.SMEM)
HBM = pl.BlockSpec(memory_space=pltpu.HBM)

PAIRS = [(i, j) for i in range(ITERS + 1) for j in range(i, ITERS + 1)]
MIDDLE_AT, LINK_AT, BACK_AT, WEIGHT_AT = 32, 40, 48, 56


def call(kernel, outs, args, specs=None, keep=None, flops=4000000):
    specs = specs or [VMEM] * len(args)
    keep = keep or [True] * len(outs)
    args = [
        arg if space is None else pltpu.with_memory_space_constraint(arg, space) for arg, space in args
    ]
    shapes = [
        pltpu.VMEM(shape, jnp.float32) if kept else jax.ShapeDtypeStruct(shape, jnp.float32)
        for shape, kept in zip(outs, keep)
    ]
    return pl.pallas_call(
        kernel,
        out_shape=shapes,
        in_specs=specs,
        out_specs=[VMEM] * len(outs),
        compiler_params=pltpu.CompilerParams(vmem_limit_bytes=KERNEL_VMEM),
        cost_estimate=pl.CostEstimate(flops=flops, bytes_accessed=1000000, transcendentals=0),
    )(*args)


def held(*arrays):
    return tuple((array, pltpu.VMEM) for array in arrays)


def stored(*arrays):
    return tuple((array, pltpu.HBM) for array in arrays)


def free(*arrays):
    return tuple((array, None) for array in arrays)


def total(value):
    return jnp.sum(jnp.sum(value, axis=0, keepdims=True), axis=1, keepdims=True)


def lane_index(shape):
    return lax.broadcasted_iota(jnp.int32, shape, 1)


def pack_y_kernel(levels, height, mask, depth, temp, north, fields, *messages):
    wet = mask[0].astype(jnp.float32)
    fields[0] = wet * height[...]
    fields[1] = wet
    fields[2] = depth[...]
    first, last = slice(0, RING), slice(temp.shape[1] - RING, temp.shape[1])

    def send(span, to_north, to_south):
        if len(messages) == 1:
            messages[0][span, :] = jnp.where(lax.axis_index("gy") == 0, to_north, to_south)
        else:
            messages[0][span, :] = to_north
            messages[1][span, :] = to_south

    for at in range(3):
        field = fields[at]
        send(slice(at * RING, (at + 1) * RING), field[last], field[first])
    base = 3 * RING
    for level in range(levels):
        flux_south = (DIFFUSE + 0.5 * north[level, first]) * (
            mask[level, first].astype(jnp.float32) * temp[level, first]
        )
        flux_north = (DIFFUSE - 0.5 * north[level, last]) * (
            mask[level, last].astype(jnp.float32) * temp[level, last]
        )
        send(slice(base + level, base + level + 1), flux_north[-1:], flux_south[:1])


def pack_t_kernel(levels, mask, temp, east, to_east, to_west):
    for level in range(levels):
        at = slice(level, level + 1)
        masked = mask[level].astype(jnp.float32) * temp[level]
        flux_east = (DIFFUSE - 0.5 * east[level]) * masked
        flux_west = (DIFFUSE + 0.5 * east[level]) * masked
        to_east[at, :] = jnp.transpose(flux_east[:, -LANES:])[-1:]
        to_west[at, :] = jnp.transpose(flux_west[:, :LANES])[:1]


def pack_x_kernel(levels, received, fields, tracer_east, tracer_west, *refs):
    arrived, (from_south, from_north, to_east, to_west) = refs[:received], refs[received:]
    if received == 1:
        lower = lax.axis_index("gy") == 0
        from_south[...] = jnp.where(lower, 0.0, arrived[0][...])
        from_north[...] = jnp.where(lower, arrived[0][...], 0.0)
    else:
        from_south[...] = arrived[0][...]
        from_north[...] = arrived[1][...]
    rows = fields.shape[1]
    for at in range(3):
        span = slice(at * RING, (at + 1) * RING)
        beside = [from_north[span, :], from_south[span, :]]
        beside.append(jnp.zeros((LANES - 2 * RING, fields.shape[2]), jnp.float32))
        flipped = jnp.transpose(jnp.concatenate([fields[at]] + beside, axis=0))
        to_west[span, :] = flipped[:RING]
        to_east[span, :] = flipped[-RING:]
    span = slice(3 * RING, 3 * RING + levels)
    to_east[span, :rows] = tracer_east[...]
    to_west[span, :rows] = tracer_west[...]
    to_east[span, rows:] = jnp.zeros((levels, LANES), jnp.float32)
    to_west[span, rows:] = jnp.zeros((levels, LANES), jnp.float32)


def beside_tile(from_west, from_east, start, size):
    span = slice(start, start + size)
    middle = jnp.zeros((LANES - 2 * size, from_west.shape[1]), jnp.float32)
    return jnp.transpose(jnp.concatenate([from_east[span, :], middle, from_west[span, :]], axis=0))


def krylov_kernel(fields, from_south, from_north, from_west, from_east, basis, row_out):
    rows, columns = fields.shape[1:]
    full_rows, full_columns = rows + 2 * RING, columns + LANES

    def widened(at):
        span = slice(at * RING, (at + 1) * RING)
        tile = jnp.concatenate([fields[at], from_north[span, :], from_south[span, :]], axis=0)
        side = beside_tile(from_west, from_east, at * RING, RING)
        return jnp.concatenate([tile, side[:full_rows]], axis=1)

    field, opening, deep = widened(0), widened(1), widened(2)
    basis[ITERS] = opening
    basis[ITERS + 1] = deep
    west_weight = STIFFNESS * 0.5 * (deep + pltpu.roll(deep, 1, 1)) * opening * pltpu.roll(opening, 1, 1)
    east_weight = pltpu.roll(west_weight, full_columns - 1, 1)
    south_weight = STIFFNESS * 0.5 * (deep + pltpu.roll(deep, 1, 0)) * opening * pltpu.roll(opening, 1, 0)
    north_weight = pltpu.roll(south_weight, full_rows - 1, 0)

    def spread(value):
        out = west_weight * (value - pltpu.roll(value, 1, 1))
        out = out + east_weight * (value - pltpu.roll(value, full_columns - 1, 1))
        out = out + south_weight * (value - pltpu.roll(value, 1, 0))
        return out + north_weight * (value - pltpu.roll(value, full_rows - 1, 0))

    at = lane_index((1, LANES))
    square = total(field * field)
    row = jnp.where(at == WEIGHT_AT, jnp.sqrt(square), 0.0)
    value = field * jnp.where(square > 0.0, lax.rsqrt(jnp.maximum(square, 1e-30)), 0.0)
    running = jnp.where(square > 0.0, 1.0, 0.0)
    before, back = jnp.zeros_like(value), jnp.zeros_like(square)
    vectors = [value]
    basis[0] = value
    for step in range(ITERS):
        image = spread(value) - back * before
        along, size = total(image * value), total(image * image)
        middle, link, scale, alive = next_step(along, size, running)
        for start, entry in ((MIDDLE_AT, middle), (LINK_AT, link), (BACK_AT, back)):
            row = jnp.where(at == start + step, entry, row)
        before, value = value, (image - middle * value) * scale
        running, back = alive, link * alive
        vectors.append(value)
        if step + 1 < ITERS:
            basis[step + 1] = value
    cut = [vector[:rows, :columns] for vector in vectors]
    partial = [jnp.sum(cut[i] * cut[j], axis=0, keepdims=True) for i, j in PAIRS]
    partial = [sum(part[:, k : k + LANES] for k in range(0, columns, LANES)) for part in partial]
    partial = partial + [jnp.zeros((LANES - len(partial), LANES), jnp.float32)]
    table = jnp.transpose(jnp.concatenate(partial, axis=0))
    row = row + jnp.sum(table, axis=0, keepdims=True)
    row_out[...] = jnp.broadcast_to(row[None], row_out.shape)


def next_step(along, size, running):
    left = size - along * along
    alive = jnp.where((left > 1e-6 * size) & (running > 0.0), 1.0, 0.0)
    safe = jnp.maximum(left, 1e-30)
    middle = jnp.where(running > 0.0, along, 4.0 * STIFFNESS)
    link = jnp.where(alive > 0.0, jnp.sqrt(safe), 2.0 * STIFFNESS)
    scale = jnp.where(alive > 0.0, lax.rsqrt(safe), 1.0 / (2.0 * STIFFNESS))
    return middle, link, scale, alive


def merged_recurrence(tiles):
    at = lane_index(tiles.shape)
    diagonal = jnp.where(at < ITERS, pltpu.roll(tiles, LANES - MIDDLE_AT, 1), 0.0)
    above = jnp.where(at < ITERS - 1, pltpu.roll(tiles, LANES - BACK_AT - 1, 1), 0.0)
    below = pltpu.roll(above, 1, 1)
    vector = jnp.where(at == 0, pltpu.roll(tiles, LANES - WEIGHT_AT, 1), 0.0)
    square = total(vector * vector)
    vector = vector * jnp.where(square > 0.0, lax.rsqrt(jnp.maximum(square, 1e-30)), 0.0)
    before, back = jnp.zeros_like(vector), jnp.zeros_like(square)
    running = jnp.ones_like(square)
    steps = []
    for _ in range(ITERS):
        image = diagonal * vector - back * before
        image = image + above * pltpu.roll(vector, LANES - 1, 1) + below * pltpu.roll(vector, 1, 1)
        along, size = total(image * vector), total(image * image)
        middle, link, scale, alive = next_step(along, size, running)
        steps.append((middle, link, scale, back))
        before, vector = vector, (image - along * vector) * (scale * alive)
        running, back = alive, link * alive
    return steps


def solve_kernel(gathered, basis, surface, pressure):
    rows, columns = surface.shape
    place = lax.axis_index("gx") * lax.axis_size("gy") + lax.axis_index("gy")
    tiles = gathered[...]
    steps = merged_recurrence(tiles)
    spare = -tiles.shape[0] % LANES
    if spare:
        tiles = jnp.concatenate([tiles, jnp.zeros((spare, LANES), jnp.float32)], axis=0)
    table = jnp.transpose(tiles)

    def known(index):
        return table[index : index + 1, :]

    products = {}
    for index, (i, j) in enumerate(PAIRS):
        products[i, j] = products[j, i] = known(index)
    change = [[known(WEIGHT_AT)]]
    for step, (middle, _, scale, back) in enumerate(steps):
        last = change[step]
        out = [None] * (step + 2)

        def add(at, term):
            out[at] = term if out[at] is None else out[at] + term

        for j, part in enumerate(last):
            add(j, (known(MIDDLE_AT + j) - middle) * part)
            add(j + 1, known(LINK_AT + j) * part)
            if j:
                add(j - 1, known(BACK_AT + j) * part)
        if step:
            for j, part in enumerate(change[step - 1]):
                add(j, -back * part)
        change.append([scale * term for term in out])
    gram = {}
    for k in range(ITERS + 1):
        half = [
            sum(change[k][i] * products[i, j] for i in range(k + 1)) for j in range(ITERS + 1)
        ]
        for m in range(k, ITERS + 1):
            both = sum(half[j] * change[m][j] for j in range(m + 1))
            gram[k, m] = gram[m, k] = jnp.sum(both, axis=1, keepdims=True)
    zero = jnp.zeros((1, 1), jnp.float32)

    def applied(vector):
        out = [zero] * (len(vector) + 1)
        for i, part in enumerate(vector):
            middle, link, _, back = steps[i]
            out[i] = out[i] + part + middle * part
            out[i + 1] = out[i + 1] + link * part
            if i:
                out[i - 1] = out[i - 1] + back * part
        return out

    def inner(left, right):
        out = zero
        for i, a in enumerate(left):
            part = zero
            for j, b in enumerate(right):
                part = part + gram[i, j] * b
            out = out + a * part
        return out

    def scaled_add(left, scale, right):
        size = max(len(left), len(right))
        left = left + [zero] * (size - len(left))
        right = right + [zero] * (size - len(right))
        return [a + scale * b for a, b in zip(left, right)]

    residual = direction = [jnp.ones((1, 1), jnp.float32)]
    iterate = [zero]
    norm_now = gram[0, 0]
    for iteration in range(ITERS):
        image = applied(direction)
        product = inner(direction, image)
        step_size = jnp.where(product > 0.0, norm_now / product, 0.0)
        iterate = scaled_add(iterate, step_size, direction)
        if iteration + 1 < ITERS:
            residual = scaled_add(residual, -step_size, image)
            norm_next = inner(residual, residual)
            growth = jnp.where(norm_now > 0.0, norm_next / norm_now, 0.0)
            direction = scaled_add(residual, growth, direction)
            norm_now = norm_next
    mine = lane_index((1, table.shape[1])) == place
    value = None
    for j in range(ITERS):
        weight = sum(iterate[k] * change[k][j] for k in range(j, ITERS))
        weight = jnp.sum(jnp.where(mine, weight, 0.0), axis=1, keepdims=True)
        value = weight * basis[j] if value is None else value + weight * basis[j]
    surface[...] = value[:rows, :columns]
    opening = basis[ITERS]
    load = basis[ITERS + 1] * value
    full_rows, full_columns = value.shape
    pull = jnp.zeros_like(load)
    for shift, axis in ((1, 1), (full_columns - 1, 1), (1, 0), (full_rows - 1, 0)):
        pull = pull + opening * pltpu.roll(opening, shift, axis) * (pltpu.roll(load, shift, axis) - load)
    pressure[...] = -GRAVITY * pull[:rows, :columns]


def tracer_kernel(levels, temp, east, north, mask, from_south, from_north, tracer):
    rows, columns = temp.shape[1:]
    row = lax.broadcasted_iota(jnp.int32, (rows, columns), 0)
    lane = lane_index((rows, columns))
    base = 3 * RING
    for level in range(levels):
        masked = mask[level].astype(jnp.float32) * temp[level]
        east_coef = DIFFUSE - 0.5 * east[level]
        west_coef = DIFFUSE + 0.5 * east[level]
        north_coef = DIFFUSE - 0.5 * north[level]
        south_coef = DIFFUSE + 0.5 * north[level]
        side_south = from_south[base + level : base + level + 1, :]
        side_north = from_north[base + level : base + level + 1, :]
        inflow = jnp.where(lane == 0, 0.0, pltpu.roll(east_coef * masked, 1, 1))
        inflow = inflow + jnp.where(
            lane == columns - 1, 0.0, pltpu.roll(west_coef * masked, columns - 1, 1)
        )
        inflow = inflow + jnp.where(row == 0, side_south, pltpu.roll(north_coef * masked, 1, 0))
        inflow = inflow + jnp.where(
            row == rows - 1, side_north, pltpu.roll(south_coef * masked, rows - 1, 0)
        )
        tracer[level] = masked + TIMESTEP * (
            inflow - (east_coef + west_coef + north_coef + south_coef) * masked
        )


def level_of_slot(slots, slot, levels):
    level = jnp.int32(0)
    for k in range(1, levels):
        level = jnp.where(slots[k] == slot, jnp.int32(k), level)
    return level


def density(level, levels, pressure, mask):
    thickness = 1.0 + level.astype(jnp.float32) / levels
    return thickness * pressure[...] * mask[level].astype(jnp.float32)


def warm_kernel(levels, slots, tracer, pressure, from_west, from_east, mask, outer, inner, partial, salt):
    rows, columns = pressure.shape
    lane = lane_index((rows, columns))
    sides = beside_tile(from_west, from_east, 3 * RING, levels)[:rows]
    for level in range(levels):
        side_west = sides[:, LANES - levels + level : LANES - levels + level + 1]
        side_east = sides[:, level : level + 1]
        edge = jnp.where(lane == 0, side_west, 0.0) + jnp.where(lane == columns - 1, side_east, 0.0)
        partial[level] = tracer[level] + TIMESTEP * edge
    for slot in range(levels):
        level = level_of_slot(slots, slot, levels)
        dense = density(level, levels, pressure, mask)
        value = jnp.where(from_outer(), outer[slot], inner[slot])
        salt[level] = (HALINE + CABBELING * value) * dense
        partial[level] = partial[level] + (THERMAL + 2.0 * NONLINEAR * value) * dense


def sort_kernel(sizes, slots, store, *parts):
    level = 0
    for size, part in zip(sizes, parts):
        for at in range(size):
            part[at] = store[slots[level]]
            level += 1


def finish_levels(levels, partial, pressure, mask, values, place, result, done, sems):
    copies = []
    for at in range(values.shape[0]):
        level = place(at)
        dense = density(level, levels, pressure, mask)
        done[at] = partial[level] + CABBELING * values[at] * dense
        copies.append(pltpu.make_async_copy(done.at[at], result.at[level], sems.at[at]))
        copies[-1].start()
    for copy in copies:
        copy.wait()


def inner_kernel(levels, partial, pressure, mask, values, slots, *refs):
    @pl.when(jnp.logical_not(from_outer()))
    def _():
        place = lambda at: level_of_slot(slots, at, levels)
        finish_levels(levels, partial, pressure, mask, values, place, *refs)


def outer_kernel(levels, first, partial, pressure, mask, values, before, *refs):
    @pl.when(from_outer())
    def _():
        place = lambda at: jnp.int32(first + at)
        finish_levels(levels, partial, pressure, mask, values, place, *refs)


def finish(kernel, levels, args, extra):
    part = args[-1]
    operands = [pltpu.with_memory_space_constraint(arg, pltpu.VMEM) for arg in args] + [extra]
    begins = extra.ndim == 1
    return pl.pallas_call(
        kernel,
        out_shape=jax.ShapeDtypeStruct((levels,) + part.shape[1:], jnp.float32),
        in_specs=[VMEM] * len(args) + [SMEM if begins else HBM],
        out_specs=HBM,
        scratch_shapes=[
            pltpu.VMEM(part.shape, jnp.float32),
            pltpu.SemaphoreType.DMA((part.shape[0],)),
        ],
        input_output_aliases={} if begins else {len(args): 0},
        compiler_params=pltpu.CompilerParams(vmem_limit_bytes=KERNEL_VMEM),
        cost_estimate=pl.CostEstimate(flops=1000000, bytes_accessed=1000000, transcendentals=0),
    )(*operands)


def shifted(value, axis, steps, around):
    count = lax.axis_size(axis)
    pairs = [(i, (i + steps) % count) for i in range(count) if around or 0 <= i + steps < count]
    return lax.ppermute(value, axis, pairs)


def shared(rows):
    rows = lax.all_to_all(rows, ("gx", "gy"), 0, 0)
    return rows.reshape(rows.shape[0], LANES)


QUARTERS = {"a": (2, 0, 3, 1), "b": (1, 3, 0, 2)}


def fetched(value, kind):
    quarter = lax.axis_size("gx") // 4
    pairs = [
        (source * quarter + i, target * quarter + i)
        for source, target in enumerate(QUARTERS[kind])
        for i in range(quarter)
    ]
    return lax.ppermute(value, "gx", pairs)


def from_outer():
    place, count = lax.axis_index("gx"), lax.axis_size("gx")
    return (place >= count // 4) & (place < count - count // 4)


def runs(levels):
    most = 6 * levels // 8
    return most, levels - most


def body(
    temp_adjoint,
    height_adjoint,
    east_velocity,
    north_velocity,
    temp_store,
    salt_store,
    slot_map,
    land_mask,
    ocean_depth,
):
    levels, rows, columns = temp_adjoint.shape
    half_cycle = lax.axis_size("gx") // 2
    devices = lax.axis_size("gx") * lax.axis_size("gy")
    strip = 3 * RING + levels
    full = (rows + 2 * RING, columns + LANES)

    salt_sizes = runs(levels)
    slots = shifted(slot_map, "gx", half_cycle, True).reshape(-1)
    warm_a, warm_b = (fetched(temp_store, kind) for kind in QUARTERS)
    salt_b = fetched(salt_store, "b")

    swap = lax.axis_size("gy") == 2
    fields, *messages = call(
        functools.partial(pack_y_kernel, levels),
        [(3, rows, columns)] + [(strip, columns)] * (1 if swap else 2),
        stored(height_adjoint, land_mask, ocean_depth, temp_adjoint, north_velocity),
    )
    if swap:
        arrived = [shifted(messages[0], "gy", 1, True)]
    else:
        arrived = [shifted(messages[0], "gy", 1, False)]
        arrived += [shifted(messages[1], "gy", -1, False)]
    tracer_east, tracer_west = call(
        functools.partial(pack_t_kernel, levels), [(levels, rows)] * 2, stored(land_mask, temp_adjoint, east_velocity)
    )
    from_south, from_north, to_east, to_west = call(
        functools.partial(pack_x_kernel, levels, len(arrived)),
        [(strip, columns)] * 2 + [(strip, rows + LANES)] * 2,
        held(fields, tracer_east, tracer_west, *arrived),
    )
    from_west = shifted(to_east, "gx", 1, True)
    from_east = shifted(to_west, "gx", -1, True)
    (tracer,) = call(
        functools.partial(tracer_kernel, levels),
        [temp_adjoint.shape],
        stored(temp_adjoint, east_velocity, north_velocity, land_mask)
        + held(from_south, from_north),
        keep=[False],
    )
    cuts = call(
        functools.partial(sort_kernel, salt_sizes),
        [(size, rows, columns) for size in salt_sizes],
        free(slot_map.reshape(-1)) + stored(salt_store),
        specs=[SMEM, VMEM],
        keep=[False] * len(salt_sizes),
    )
    salt_parts = [fetched(cut, "a") for cut in cuts]
    beside = held(from_south, from_north, from_west, from_east)
    basis, tile_rows = call(krylov_kernel, [(ITERS + 2,) + full, (devices, 1, LANES)], held(fields) + beside)
    gathered = shared(tile_rows)
    surface, pressure = call(solve_kernel, [(rows, columns)] * 2, held(gathered, basis), keep=[False, True])
    partial, salt_back = call(
        functools.partial(warm_kernel, levels),
        [temp_adjoint.shape] * 2,
        free(slots) + stored(tracer) + held(pressure, from_west, from_east) + free(land_mask, warm_a, warm_b),
        specs=[SMEM] + [VMEM] * 7,
        keep=[True, False],
    )
    common = (partial, pressure, land_mask)
    inner = functools.partial(inner_kernel, levels)
    temp_back, first = finish(inner, levels, (*common, salt_b), slots), 0
    for size, part in zip(salt_sizes, salt_parts):
        outer = functools.partial(outer_kernel, levels, first)
        temp_back = finish(outer, levels, (*common, part), temp_back)
        first += size
    return (temp_back, salt_back, surface)


def solution(mesh):
    return jax.shard_map(
        body,
        mesh=mesh,
        in_specs=(
            P(None, "gy", "gx"),
            P("gy", "gx"),
            P(None, "gy", "gx"),
            P(None, "gy", "gx"),
            P(None, "gy", "gx"),
            P(None, "gy", "gx"),
            P("gx", "gy", None),
            P(None, "gy", "gx"),
            P("gy", "gx"),
        ),
        out_specs=(P(None, "gy", "gx"), P(None, "gy", "gx"), P("gy", "gx")),
        check_vma=False,
    )
```
